32 devices in a mesh: dp: 2 (over x), tp: 4 (over z), sp: 4 (over y, core).
Axes of the slice: x: 2, y: 2, z: 4, core: 2. Of those that a mesh axis runs over, the one named last changes fastest.
Arguments:
- tokens: bfloat16 [32768, 1024], P(('dp', 'sp')), parts along dimension 0
- glob_pos: int32 [2048], P('dp'), parts along dimension 0
- w_query: bfloat16 [1024, 16, 64], P(None, 'tp')
- w_key: bfloat16 [1024, 16, 64], P(None, 'tp')
- w_value: bfloat16 [1024, 16, 64], P(None, 'tp')
- w_out: bfloat16 [16, 64, 1024], P('tp')
- w_up: bfloat16 [1024, 2624], P(None, 'tp')
- w_down: bfloat16 [2624, 1024], P('tp')
Outputs:
- output: bfloat16 [32768, 1024], P(('dp', 'sp')), parts along dimension 0
There are 2 independent parts. The reference program is written for one: setup_inputs(seed, part) draws one part's arguments, and reference() takes and returns one part's arrays. A program takes and returns all parts, laid end to end along the dimension named above; an argument that names none is the same for every part.
All inputs are finite; a program needn't handle non-finite values.
Results may differ from the reference program's by a relative error of at most 0.00794781.
Values are sent between devices in bfloat16 or wider.
A program may use at most 1 GiB of HBM per device.

```python
import jax
import jax.numpy as jnp
from jax import lax
import math

D = 1024
HEADS = 16
FF = 2624
WIN = 256
SEQ = 16384
GLOB = 1024

HEAD = D // HEADS


def setup_inputs(seed: int = 0, part: int = 0) -> dict:
    root_key = jax.random.key(seed)
    weight_root, part_root = jax.random.split(root_key, 2)
    part_key = jax.random.fold_in(part_root, part)
    tok_key, pos_key = jax.random.split(part_key, 2)
    tokens = jax.random.normal(tok_key, (SEQ, D), jnp.float32).astype(jnp.bfloat16)
    inner_pos = jax.random.permutation(pos_key, SEQ - 2)[: GLOB - 2] + 1
    glob_pos = jnp.sort(jnp.concatenate([jnp.array([0, SEQ - 1], jnp.int32), inner_pos.astype(jnp.int32)]))
    w_keys = jax.random.split(weight_root, 7)
    qk_std = (2.0 / D) ** 0.5
    out_std = max(1.0, ((2 * WIN + GLOB) / 50.0) ** 0.5) / math.sqrt(D)
    w_query = (jax.random.normal(w_keys[0], (D, HEADS, HEAD), jnp.float32) * qk_std).astype(jnp.bfloat16)
    w_key = (jax.random.normal(w_keys[1], (D, HEADS, HEAD), jnp.float32) * qk_std).astype(jnp.bfloat16)
    w_value = (jax.random.normal(w_keys[2], (D, HEADS, HEAD), jnp.float32) / math.sqrt(D)).astype(jnp.bfloat16)
    w_out = (jax.random.normal(w_keys[3], (HEADS, HEAD, D), jnp.float32) * out_std).astype(jnp.bfloat16)
    w_up = (jax.random.normal(w_keys[4], (D, FF), jnp.float32) / math.sqrt(D)).astype(jnp.bfloat16)
    w_down = (jax.random.normal(w_keys[5], (FF, D), jnp.float32) / math.sqrt(FF)).astype(jnp.bfloat16)
    return {'tokens': tokens, 'glob_pos': glob_pos, 'w_query': w_query, 'w_key': w_key, 'w_value': w_value, 'w_out': w_out, 'w_up': w_up, 'w_down': w_down}


def reference(tokens, glob_pos, w_query, w_key, w_value, w_out, w_up, w_down):
    scale = 1.0 / math.sqrt(HEAD)
    q_rows = jnp.dot(tokens, w_query.reshape(D, D), preferred_element_type=jnp.float32).astype(jnp.bfloat16).reshape(SEQ, HEADS, HEAD)
    k_rows = jnp.dot(tokens, w_key.reshape(D, D), preferred_element_type=jnp.float32).astype(jnp.bfloat16).reshape(SEQ, HEADS, HEAD)
    v_rows = jnp.dot(tokens, w_value.reshape(D, D), preferred_element_type=jnp.float32).astype(jnp.bfloat16).reshape(SEQ, HEADS, HEAD)
    glob_flag = jnp.zeros((SEQ,), jnp.int32).at[glob_pos].set(1)
    pad_cfg = ((WIN, WIN), (0, 0), (0, 0))
    k_pad = jnp.pad(k_rows, pad_cfg)
    v_pad = jnp.pad(v_rows, pad_cfg)
    flag_pad = jnp.pad(glob_flag, (WIN, WIN))
    k_glob = k_rows[glob_pos].astype(jnp.float32)
    v_glob = v_rows[glob_pos].astype(jnp.float32)
    q_block = 128
    key_span = q_block + 2 * WIN

    def window_block(blk_index):
        start = blk_index * q_block
        q_blk = lax.dynamic_slice_in_dim(q_rows, start, q_block).astype(jnp.float32)
        k_blk = lax.dynamic_slice_in_dim(k_pad, start, key_span).astype(jnp.float32)
        v_blk = lax.dynamic_slice_in_dim(v_pad, start, key_span).astype(jnp.float32)
        f_blk = lax.dynamic_slice_in_dim(flag_pad, start, key_span)
        q_pos = start + jnp.arange(q_block)
        k_pos = start - WIN + jnp.arange(key_span)
        k_ok = (k_pos >= 0) & (k_pos < SEQ) & (f_blk == 0)
        allowed = (jnp.abs(q_pos[:, None] - k_pos[None, :]) <= WIN) & k_ok[None, :]
        s_win = jnp.einsum('qhe,khe->hqk', q_blk, k_blk) * scale
        s_win = jnp.where(allowed[None], s_win, -jnp.inf)
        s_glob = jnp.einsum('qhe,ghe->hqg', q_blk, k_glob) * scale
        prob_rows = jax.nn.softmax(jnp.concatenate([s_win, s_glob], axis=2), axis=2)
        prob_rows = prob_rows.astype(jnp.bfloat16).astype(jnp.float32)
        v_all = jnp.concatenate([v_blk, v_glob], axis=0)
        return jnp.einsum('hqk,khe->qhe', prob_rows, v_all).astype(jnp.bfloat16)

    o_rows = lax.map(window_block, jnp.arange(SEQ // q_block)).reshape(SEQ, HEADS, HEAD)
    q_heads = jnp.transpose(q_rows[glob_pos], (1, 0, 2))
    k_heads = jnp.transpose(k_rows, (1, 0, 2))
    v_heads = jnp.transpose(v_rows, (1, 0, 2))

    def glob_head(head_parts):
        q_head, k_head, v_head = head_parts
        scores = jnp.dot(q_head, k_head.T, preferred_element_type=jnp.float32) * scale
        prob_rows = jax.nn.softmax(scores, axis=1).astype(jnp.bfloat16)
        return jnp.dot(prob_rows, v_head, preferred_element_type=jnp.float32).astype(jnp.bfloat16)

    glob_out = jnp.transpose(lax.map(glob_head, (q_heads, k_heads, v_heads)), (1, 0, 2))
    o_rows = o_rows.at[glob_pos].set(glob_out)
    mixed = jnp.dot(o_rows.reshape(SEQ, D), w_out.reshape(D, D), preferred_element_type=jnp.float32)
    hidden = (tokens.astype(jnp.float32) + mixed).astype(jnp.bfloat16)
    gelu_rows = jax.nn.gelu(jnp.dot(hidden, w_up, preferred_element_type=jnp.float32), approximate=True).astype(jnp.bfloat16)
    down_sum = jnp.dot(gelu_rows, w_down, preferred_element_type=jnp.float32)
    return (hidden.astype(jnp.float32) + down_sum).astype(jnp.bfloat16)
```

```python
import functools
import math

import jax
import jax.numpy as jnp
from jax import lax
from jax.experimental import pallas as pl
from jax.experimental.pallas import tpu as pltpu
from jax.sharding import PartitionSpec as P

WIN = 256
QB = 256
FLOOR = -3.0e38
F32 = jnp.float32
BF16 = jnp.bfloat16
NT = (((1,), (1,)), ((), ()))


def dot_nt(a, b):
    return lax.dot_general(a, b, NT, preferred_element_type=F32)


def dot_nn(a, b):
    return jnp.dot(a, b, preferred_element_type=F32)


def params(n_axes, vmem_mib=48):
    return pltpu.CompilerParams(
        dimension_semantics=("arbitrary",) * n_axes, vmem_limit_bytes=vmem_mib << 20)


def cost(flops, bytes_accessed, exps=0):
    return pl.CostEstimate(flops=int(flops), bytes_accessed=int(bytes_accessed), transcendentals=int(exps))


def stack_pair(q_pair):
    low = lax.broadcasted_iota(jnp.int32, q_pair.shape, 1) < 64
    zero = jnp.zeros_like(q_pair)
    return jnp.concatenate([jnp.where(low, q_pair, zero), jnp.where(low, zero, q_pair)], axis=0)


def merge_pair(rows):
    half = rows.shape[0] // 2
    low = lax.broadcasted_iota(jnp.int32, (half, 128), 1) < 64
    return jnp.where(low, jnp.broadcast_to(rows[:half], (half, 128)), jnp.broadcast_to(rows[half:], (half, 128)))


def pick_kernel(pos_ref, idx_ref, qkv_ref, out_ref, acc_ref):
    n_rows = qkv_ref.shape[0]
    n_pick = out_ref.shape[0]
    g0 = pl.program_id(0) * n_pick
    first, last = pos_ref[g0], pos_ref[g0 + n_pick - 1]
    acc_ref[...] = jnp.zeros_like(acc_ref)
    idx = idx_ref[...]

    @pl.loop(0, n_rows // QB)
    def _(r):
        lo = r * QB

        @pl.when((first < lo + QB) & (last >= lo))
        def _():
            hit = idx == lo + lax.broadcasted_iota(jnp.int32, (n_pick, QB), 1)
            acc_ref[...] += dot_nn(hit.astype(F32).astype(BF16), qkv_ref[pl.ds(pl.multiple_of(lo, QB), QB), :])

    out_ref[...] = acc_ref[...].astype(out_ref.dtype)


def pick_rows(qkv, local_idx):
    n_glob = local_idx.shape[0]
    n_rows, width = qkv.shape
    block = 128
    return pl.pallas_call(
        pick_kernel,
        grid_spec=pltpu.PrefetchScalarGridSpec(
            num_scalar_prefetch=1, grid=(n_glob // block,),
            in_specs=[pl.BlockSpec((block, 1), lambda i, p: (i, 0)),
                      pl.BlockSpec((n_rows, width), lambda i, p: (0, 0))],
            out_specs=pl.BlockSpec((block, width), lambda i, p: (i, 0)),
            scratch_shapes=[pltpu.VMEM((block, width), F32)]),
        out_shape=jax.ShapeDtypeStruct((n_glob, width), BF16),
        compiler_params=params(1), cost_estimate=cost(2e9, 8e6), name="pick",
    )(local_idx, local_idx[:, None], qkv)


def window_kernel(q_ref, kl_ref, kc_ref, kr_ref, vl_ref, vc_ref, vr_ref, hl_ref, hr_ref,
                  bl_ref, bc_ref, br_ref, acc_ref, m_ref, l_ref, tri_ref):
    i = pl.program_id(0)

    @pl.when(i == 0)
    def _():
        r_i = lax.broadcasted_iota(jnp.int32, (QB, QB), 0)
        c_i = lax.broadcasted_iota(jnp.int32, (QB, QB), 1)
        for half in range(2):
            tri_ref[0, half * QB:(half + 1) * QB] = jnp.where(c_i >= r_i, 0.0, -jnp.inf)
            tri_ref[1, half * QB:(half + 1) * QB] = jnp.where(c_i <= r_i, 0.0, -jnp.inf)

    is_first = i == 0
    is_last = i == pl.num_programs(0) - 1
    for pr in range(2):
        cols = slice(pr * 128, pr * 128 + 128)
        vcols = slice(256 + pr * 128, 256 + pr * 128 + 128)
        q2 = stack_pair(q_ref[:, cols])
        kl = jnp.where(is_first, hl_ref[:, cols], kl_ref[:, cols])
        kr = jnp.where(is_last, hr_ref[:, cols], kr_ref[:, cols])
        vl = jnp.where(is_first, hl_ref[:, vcols], vl_ref[:, cols])
        vr = jnp.where(is_last, hr_ref[:, vcols], vr_ref[:, cols])
        s_l = dot_nt(q2, kl) + (tri_ref[0] + bl_ref[...])
        s_c = dot_nt(q2, kc_ref[:, cols]) + bc_ref[...]
        s_r = dot_nt(q2, kr) + (tri_ref[1] + br_ref[...])
        top = jnp.max(jnp.maximum(jnp.maximum(s_l, s_c), s_r), axis=1, keepdims=True)
        top = jnp.maximum(top, FLOOR)
        e_l, e_c, e_r = jnp.exp(s_l - top), jnp.exp(s_c - top), jnp.exp(s_r - top)
        total = jnp.sum(e_l + e_c + e_r, axis=1, keepdims=True)
        acc = dot_nn(e_l.astype(BF16), vl) + dot_nn(e_c.astype(BF16), vc_ref[:, cols]) + dot_nn(e_r.astype(BF16), vr)
        acc_ref[:, cols] = merge_pair(acc)
        m_ref[:, cols] = merge_pair(top)
        l_ref[:, cols] = merge_pair(total)


def window_part(qkv, halo_l, halo_r, bias):
    n_rows = qkv.shape[0]
    n_blk = n_rows // QB
    left = lambda c: pl.BlockSpec((QB, 256), lambda i: (jnp.maximum(i - 1, 0), c))
    mid = lambda c: pl.BlockSpec((QB, 256), lambda i: (i, c))
    right = lambda c: pl.BlockSpec((QB, 256), lambda i: (jnp.minimum(i + 1, n_blk - 1), c))
    whole = lambda a: pl.BlockSpec(a.shape, lambda i: (0,) * a.ndim)
    out = jax.ShapeDtypeStruct((n_rows, 256), F32)
    return pl.pallas_call(
        window_kernel, grid=(n_blk,),
        in_specs=[mid(0), left(1), mid(1), right(1), left(2), mid(2), right(2), whole(halo_l), whole(halo_r),
                  pl.BlockSpec((1, QB), lambda i: (0, i)), pl.BlockSpec((1, QB), lambda i: (0, i + 1)),
                  pl.BlockSpec((1, QB), lambda i: (0, i + 2))],
        out_specs=[pl.BlockSpec((QB, 256), lambda i: (i, 0))] * 3,
        out_shape=[out, out, out], scratch_shapes=[pltpu.VMEM((2, 2 * QB, QB), F32)],
        compiler_params=params(1), cost_estimate=cost(30e9, 30e6, 12e6), name="window_part",
    )(qkv, qkv, qkv, qkv, qkv, qkv, qkv, halo_l, halo_r, bias, bias, bias)


def global_keys_kernel(q_ref, kg_ref, vg_ref, acc_ref, m_ref, l_ref, out_ref):
    for pr in range(2):
        cols = slice(pr * 128, pr * 128 + 128)
        q2 = stack_pair(q_ref[:, cols])
        s = dot_nt(q2, kg_ref[:, cols])
        top = merge_pair(jnp.max(s, axis=1, keepdims=True))
        m_win = m_ref[:, cols]
        m_all = jnp.maximum(top, m_win)
        alpha = jnp.exp(m_win - m_all)
        m_rows = jnp.concatenate([m_all[:, :1], m_all[:, 64:65]], axis=0)
        e = jnp.exp(s - m_rows)
        total = merge_pair(jnp.sum(e, axis=1, keepdims=True)) + alpha * l_ref[:, cols]
        acc = merge_pair(dot_nn(e.astype(BF16), vg_ref[:, cols])) + alpha * acc_ref[:, cols]
        out_ref[:, cols] = (acc / total).astype(out_ref.dtype)


def global_keys_part(qkv, qkv_g, acc, m, l, chunk, n_chunks):
    n_rows = qkv.shape[0] // n_chunks
    n_glob = qkv_g.shape[0]
    n_blk = n_rows // QB
    row = pl.BlockSpec((QB, 256), lambda i: (chunk * n_blk + i, 0))
    return pl.pallas_call(
        global_keys_kernel, grid=(n_blk,),
        in_specs=[row, pl.BlockSpec((n_glob, 256), lambda i: (0, 1)), pl.BlockSpec((n_glob, 256), lambda i: (0, 2)),
                  row, row, row],
        out_specs=pl.BlockSpec((QB, 256), lambda i: (i, 0)),
        out_shape=jax.ShapeDtypeStruct((n_rows, 256), BF16),
        compiler_params=params(1), cost_estimate=cost(40e9 / n_chunks, 20e6 / n_chunks, 16e6 / n_chunks),
        name="global_keys",
    )(qkv, qkv_g, qkv_g, acc, m, l)


def global_queries_kernel(q_ref, k_ref, v_ref, out_ref, acc_ref, m_ref, l_ref):
    j = pl.program_id(1)

    @pl.when(j == 0)
    def _():
        acc_ref[...] = jnp.zeros_like(acc_ref)
        l_ref[...] = jnp.zeros_like(l_ref)
        m_ref[...] = jnp.full_like(m_ref, FLOOR)

    for pr in range(2):
        cols = slice(pr * 128, pr * 128 + 128)
        q2 = stack_pair(q_ref[:, cols])
        s = dot_nt(q2, k_ref[:, cols])
        m_old = m_ref[pr]
        m_new = jnp.maximum(m_old, jnp.max(s, axis=1, keepdims=True))
        alpha = jnp.exp(m_old - m_new)
        e = jnp.exp(s - m_new[:, :1])
        part = e[:, :128]
        for c in range(1, e.shape[1] // 128):
            part = part + e[:, c * 128:(c + 1) * 128]
        l_ref[pr] = alpha * l_ref[pr] + part
        acc_ref[pr] = alpha * acc_ref[pr] + dot_nn(e.astype(BF16), v_ref[:, cols])
        m_ref[pr] = m_new

    @pl.when(j == pl.num_programs(1) - 1)
    def _():
        for pr in range(2):
            out_ref[:, pr * 128:pr * 128 + 128] = merge_pair(acc_ref[pr])
            out_ref[:, 256 + pr * 128:256 + pr * 128 + 128] = merge_pair(m_ref[pr])
            out_ref[:, 512 + pr * 128:512 + pr * 128 + 128] = merge_pair(jnp.sum(l_ref[pr], axis=1, keepdims=True))


def global_queries_part(qkv_g, qkv):
    n_glob = qkv_g.shape[0]
    n_rows = qkv.shape[0]
    kb = 1024
    return pl.pallas_call(
        global_queries_kernel, grid=(n_glob // QB, n_rows // kb),
        in_specs=[pl.BlockSpec((QB, 256), lambda i, j: (i, 0)), pl.BlockSpec((kb, 256), lambda i, j: (j, 1)),
                  pl.BlockSpec((kb, 256), lambda i, j: (j, 2))],
        out_specs=pl.BlockSpec((QB, 768), lambda i, j: (i, 0)),
        out_shape=jax.ShapeDtypeStruct((n_glob, 768), F32),
        scratch_shapes=[pltpu.VMEM((2, 2 * QB, 128), F32)] * 3,
        compiler_params=params(2), cost_estimate=cost(34e9, 20e6, 16e6), name="global_queries",
    )(qkv_g, qkv, qkv)


def place_kernel(pos_ref, idx_ref, glob_ref, o_ref, out_ref, acc_ref, hit_ref, *, chunk_row):
    lo = chunk_row + pl.program_id(0) * QB
    acc_ref[...] = jnp.zeros_like(acc_ref)
    hit_ref[...] = jnp.zeros_like(hit_ref)

    @pl.loop(0, glob_ref.shape[0] // 128)
    def _(b):
        g0 = b * 128

        @pl.when((pos_ref[g0] < lo + QB) & (pos_ref[g0 + 127] >= lo))
        def _():
            g = pl.multiple_of(g0, 128)
            hit = idx_ref[:, pl.ds(g, 128)] == lo + lax.broadcasted_iota(jnp.int32, (QB, 128), 0)
            hit = hit.astype(F32)
            acc_ref[...] += dot_nn(hit.astype(BF16), glob_ref[pl.ds(g, 128), :])
            hit_ref[...] += hit

    mine = jnp.sum(hit_ref[...], axis=1, keepdims=True) > 0.5
    out_ref[...] = jnp.where(mine, acc_ref[...], o_ref[...].astype(F32)).astype(out_ref.dtype)


def place_rows(o, glob_out, local_idx, chunk_row):
    n_rows, width = o.shape
    n_glob = local_idx.shape[0]
    return pl.pallas_call(
        functools.partial(place_kernel, chunk_row=chunk_row),
        grid_spec=pltpu.PrefetchScalarGridSpec(
            num_scalar_prefetch=1, grid=(n_rows // QB,),
            in_specs=[pl.BlockSpec((1, n_glob), lambda i, p: (0, 0)), pl.BlockSpec((n_glob, width), lambda i, p: (0, 0)),
                      pl.BlockSpec((QB, width), lambda i, p: (i, 0))],
            out_specs=pl.BlockSpec((QB, width), lambda i, p: (i, 0)),
            scratch_shapes=[pltpu.VMEM((QB, width), F32), pltpu.VMEM((QB, 128), F32)]),
        out_shape=jax.ShapeDtypeStruct((n_rows, width), BF16),
        compiler_params=params(1), cost_estimate=cost(1e9, 2e6), name="place",
    )(local_idx, local_idx[None, :], glob_out, o)


def mlp_kernel(x_ref, o_ref, w_ref, *refs, n_tp, n_rep, d_o, d_f):
    y_ref, wo_ref, w2_ref, w1_ref, sem = refs[-5:]

    @pl.when(pl.program_id(0) == 0)
    def _():
        copies = []
        piece = wo_ref.shape[1] // n_rep
        for j in range(n_rep):
            for t in range(n_tp):
                lanes = pl.ds(j * piece, piece)
                copies.append(pltpu.make_async_copy(
                    w_ref.at[j, t, pl.ds(0, d_o)], wo_ref.at[pl.ds(t * d_o, d_o), lanes], sem))
                copies.append(pltpu.make_async_copy(
                    w_ref.at[j, t, pl.ds(d_o, d_f)], w2_ref.at[pl.ds(t * d_f, d_f), lanes], sem))
                copies.append(pltpu.make_async_copy(
                    w_ref.at[j, t, pl.ds(d_o + d_f, d_f)], w1_ref.at[pl.ds(t * d_f, d_f), lanes], sem))
        for c in copies:
            c.start()
        for c in copies:
            c.wait()

    mixed = dot_nn(o_ref[0], wo_ref[:d_o, :])
    for t in range(1, n_tp):
        mixed += dot_nn(o_ref[t], wo_ref[t * d_o:(t + 1) * d_o, :])
    h = (x_ref[...].astype(F32) + mixed).astype(BF16)
    width = n_tp * d_f
    acc = h.astype(F32)
    for f0 in range(0, width, 512):
        f1 = min(f0 + 512, width)
        z = dot_nt(h, w1_ref[f0:f1, :])
        u = 0.5 * z * (1.0 + jnp.tanh(math.sqrt(2.0 / math.pi) * (z + 0.044715 * (z * z * z))))
        acc += dot_nn(u.astype(BF16), w2_ref[f0:f1, :])
    y_ref[...] = acc.astype(y_ref.dtype)


def mlp_rows(tokens, o_all, w_all, y, chunk, d_o, d_f):
    n_tp, n_rows, _ = o_all.shape
    n_rep = w_all.shape[0]
    dim = tokens.shape[1]
    rb = min(512, n_rows)
    n_blk = n_rows // rb
    earlier = () if y is None else (y,)
    return pl.pallas_call(
        functools.partial(mlp_kernel, n_tp=n_tp, n_rep=n_rep, d_o=d_o, d_f=d_f), grid=(n_blk,),
        in_specs=[pl.BlockSpec((rb, dim), lambda i: (chunk * n_blk + i, 0)),
                  pl.BlockSpec((n_tp, rb, d_o), lambda i: (0, i, 0)),
                  pl.BlockSpec(memory_space=pl.ANY)] + [pl.BlockSpec(memory_space=pl.ANY)] * len(earlier),
        out_specs=pl.BlockSpec((rb, dim), lambda i: (chunk * n_blk + i, 0)),
        out_shape=jax.ShapeDtypeStruct(tokens.shape, BF16),
        input_output_aliases={3: 0} if earlier else {},
        scratch_shapes=[pltpu.VMEM((n_tp * d_o, dim), BF16), pltpu.VMEM((n_tp * d_f, dim), BF16),
                        pltpu.VMEM((n_tp * d_f, dim), BF16), pltpu.SemaphoreType.DMA],
        compiler_params=params(1, 56), cost_estimate=cost(2 * n_rows * dim * (dim + 2 * n_tp * d_f), 20e6), name="mlp",
    )(tokens, o_all, w_all, *earlier)


def combine(a, b):
    acc_a, m_a, l_a = a[:, :256], a[:, 256:512], a[:, 512:]
    acc_b, m_b, l_b = b[:, :256], b[:, 256:512], b[:, 512:]
    m = jnp.maximum(m_a, m_b)
    e_a, e_b = jnp.exp(m_a - m), jnp.exp(m_b - m)
    return acc_a * e_a + acc_b * e_b, m, l_a * e_a + l_b * e_b


def solution(mesh):
    n_seq = mesh.shape['sp']
    to_right = [(i, i + 1) for i in range(n_seq - 1)]
    to_left = [(i + 1, i) for i in range(n_seq - 1)]
    core_swap = [(i, i ^ 1) for i in range(n_seq)]
    chip_swap = [(i, i ^ 2) for i in range(n_seq)]

    def device_layer(tokens, glob_pos, w_query, w_key, w_value, w_out, w_up, w_down):
        n_rows, dim = tokens.shape
        n_glob = glob_pos.shape[0]
        sp = lax.axis_index('sp')
        core, chip = sp % 2, sp // 2
        first_row = sp * n_rows
        seq_len = n_rows * n_seq
        local_idx = glob_pos - first_row

        d_o, d_f = w_out.shape[0] * w_out.shape[1], w_down.shape[0]
        shard = jnp.concatenate([w_out.reshape(d_o, dim), w_down, w_up.T], axis=0)
        rep = lax.axis_index('dp') * n_seq + sp
        n_tp, n_rep = mesh.shape['tp'], mesh.shape['dp'] * n_seq
        piece = dim // n_rep
        w_slice = lax.dynamic_slice_in_dim(shard, rep * piece, piece, axis=1)
        w_all = lax.all_gather(w_slice, ('dp', 'sp', 'tp'))
        w_all = w_all.reshape(n_rep, n_tp, d_o + 2 * d_f, piece)

        w_cat = jnp.concatenate([w_query.reshape(dim, -1) * jnp.asarray(0.125, BF16),
                                 w_key.reshape(dim, -1), w_value.reshape(dim, -1)], axis=1)
        qkv = jnp.dot(tokens, w_cat, preferred_element_type=F32).astype(BF16)
        halo_l = lax.ppermute(qkv[n_rows - WIN:, 256:], 'sp', to_right)
        halo_r = lax.ppermute(qkv[:WIN, 256:], 'sp', to_left)

        k_pos = first_row - WIN + jnp.arange(n_rows + 2 * WIN)
        k_off = jnp.any(glob_pos[:, None] == k_pos[None, :], axis=0) | (k_pos < 0) | (k_pos >= seq_len)
        bias = jnp.where(k_off, -jnp.inf, 0.0).astype(F32)[None, :]

        picked = pick_rows(qkv, local_idx)
        half = n_glob // 2
        mine = lax.dynamic_slice_in_dim(picked, core * half, half)
        other = lax.ppermute(lax.dynamic_slice_in_dim(picked, (1 - core) * half, half), 'sp', core_swap)
        mine = mine + other
        got = lax.ppermute(mine, 'sp', chip_swap)
        acc, m, l = window_part(qkv, halo_l, halo_r, bias)
        got, acc = lax.optimization_barrier((got, acc))
        mine = mine + got
        other = lax.ppermute(mine, 'sp', core_swap)
        qkv_g = jnp.concatenate([jnp.where(core == 0, mine, other), jnp.where(core == 0, other, mine)], axis=0)

        part = global_queries_part(qkv_g, qkv)

        quarter = n_glob // 4
        got = lax.ppermute(lax.dynamic_slice_in_dim(part, (1 - core) * half, half), 'sp', core_swap)
        joined = jnp.concatenate(combine(lax.dynamic_slice_in_dim(part, core * half, half), got), axis=1)
        got = lax.ppermute(lax.dynamic_slice_in_dim(joined, (1 - chip) * quarter, quarter), 'sp', chip_swap)
        n_chunks = 4
        o_first = global_keys_part(qkv, qkv_g, acc, m, l, 0, n_chunks)
        got, o_first = lax.optimization_barrier((got, o_first))
        g_acc, _, g_l = combine(lax.dynamic_slice_in_dim(joined, chip * quarter, quarter), got)
        mine = (g_acc / g_l).astype(BF16)
        other = lax.ppermute(mine, 'sp', chip_swap)
        mine = jnp.concatenate([jnp.where(chip == 0, mine, other), jnp.where(chip == 0, other, mine)], axis=0)
        other = lax.ppermute(mine, 'sp', core_swap)
        glob_out = jnp.concatenate([jnp.where(core == 0, mine, other), jnp.where(core == 0, other, mine)], axis=0)

        glob_out, w_all = lax.optimization_barrier((glob_out, w_all))
        y = None
        for c in range(n_chunks):
            o = o_first if c == 0 else global_keys_part(qkv, qkv_g, acc, m, l, c, n_chunks)
            o = place_rows(o, glob_out, local_idx, c * (n_rows // n_chunks))
            o_all = lax.all_gather(o, 'tp')
            y = mlp_rows(tokens, o_all, w_all, y, c, d_o, d_f)
        return y

    row_spec = P(('dp', 'sp'), None)
    head_spec = P(None, 'tp', None)
    in_specs = (row_spec, P('dp'), head_spec, head_spec, head_spec, P('tp', None, None), P(None, 'tp'), P('tp', None))
    return jax.shard_map(device_layer, mesh=mesh, in_specs=in_specs, out_specs=row_spec, check_vma=False)
```

```python
import functools
import math

import jax
import jax.numpy as jnp
from jax import lax
from jax.experimental import pallas as pl
from jax.experimental.pallas import tpu as pltpu
from jax.sharding import PartitionSpec as P

WIN = 256
QB = 256
CHUNKS = (4, 4, 4, 4)
FLOOR = -3.0e38
F32 = jnp.float32
BF16 = jnp.bfloat16
NT = (((1,), (1,)), ((), ()))


def dot_nt(a, b):
    return lax.dot_general(a, b, NT, preferred_element_type=F32)


def dot_nn(a, b):
    return jnp.dot(a, b, preferred_element_type=F32)


def params(n_axes, vmem_mib=48):
    return pltpu.CompilerParams(
        dimension_semantics=("arbitrary",) * n_axes, vmem_limit_bytes=vmem_mib << 20)


def cost(flops, bytes_accessed, exps=0):
    return pl.CostEstimate(flops=int(flops), bytes_accessed=int(bytes_accessed), transcendentals=int(exps))


def head_sums(rows):
    n = rows.shape[1]
    r = lax.broadcasted_iota(jnp.int32, (n, n), 0) // 64
    c = lax.broadcasted_iota(jnp.int32, (n, n), 1) // 64
    pick = jnp.where(r == (c + 1 - 2 * (c % 2)), 1.0, 0.0).astype(BF16)
    wide = rows.astype(F32)
    return dot_nn((wide * wide).astype(BF16), pick)


def qkv_kernel(pos_ref, idx_ref, x_ref, w_ref, qkv_ref, pick_ref, kmax_ref, acc_ref):
    step = pl.program_id(0)
    n_blk = x_ref.shape[0]
    lo = step * n_blk
    gb = 128

    @pl.when(step == 0)
    def _():
        acc_ref[...] = jnp.zeros_like(acc_ref)
        kmax_ref[...] = jnp.zeros_like(kmax_ref)

    rows = dot_nn(x_ref[...], w_ref[...]).astype(BF16)
    qkv_ref[...] = rows
    kmax_ref[...] = jnp.maximum(kmax_ref[...], jnp.max(head_sums(rows[:, 256:512]), axis=0, keepdims=True))

    @pl.loop(0, idx_ref.shape[0] // gb)
    def _(b):
        g0 = pl.multiple_of(b * gb, gb)

        @pl.when((pos_ref[g0] < lo + n_blk) & (pos_ref[g0 + gb - 1] >= lo))
        def _():
            hit = idx_ref[pl.ds(g0, gb), :] == lo + lax.broadcasted_iota(jnp.int32, (gb, n_blk), 1)
            acc_ref[pl.ds(g0, gb), :] += dot_nn(hit.astype(F32).astype(BF16), qkv_ref[...])

    @pl.when(step == pl.num_programs(0) - 1)
    def _():
        pick_ref[...] = acc_ref[...].astype(pick_ref.dtype)


def qkv_part(tokens, w_cat, local_idx):
    n_rows, dim = tokens.shape
    n_glob = local_idx.shape[0]
    width = w_cat.shape[1]
    rb = 512
    return pl.pallas_call(
        qkv_kernel,
        grid_spec=pltpu.PrefetchScalarGridSpec(
            num_scalar_prefetch=1, grid=(n_rows // rb,),
            in_specs=[pl.BlockSpec((n_glob, 1), lambda i, p: (0, 0)), pl.BlockSpec((rb, dim), lambda i, p: (i, 0)),
                      pl.BlockSpec((dim, width), lambda i, p: (0, 0))],
            out_specs=[pl.BlockSpec((rb, width), lambda i, p: (i, 0)), pl.BlockSpec((n_glob, width), lambda i, p: (0, 0)),
                       pl.BlockSpec((1, 256), lambda i, p: (0, 0))],
            scratch_shapes=[pltpu.VMEM((n_glob, width), F32)]),
        out_shape=[jax.ShapeDtypeStruct((n_rows, width), BF16), jax.ShapeDtypeStruct((n_glob, width), BF16),
                   jax.ShapeDtypeStruct((1, 256), F32)],
        compiler_params=params(1), cost_estimate=cost(8e9, 24e6), name="qkv",
    )(local_idx, local_idx[:, None], tokens, w_cat)


def low_lanes(n):
    return lax.broadcasted_iota(jnp.int32, (n, 128), 1) < 64


def shifts(q, kmax):
    return (-1.02 * jnp.sqrt(head_sums(q) * kmax)).astype(BF16)


def own_half(pair, other, half):
    low = low_lanes(pair.shape[0])
    return jnp.where(low, pair, other) if half == 0 else jnp.where(low, other, pair)


def query_rows(q, neg, half):
    lane = lax.broadcasted_iota(jnp.int32, q.shape, 1) % 64
    return own_half(q, jnp.where(lane == 0, neg, jnp.ones_like(neg)), half)


def key_extra(n):
    return jnp.where(lax.broadcasted_iota(jnp.int32, (n, 128), 1) % 64 == 0, 1.0, 0.0).astype(BF16)


def stream(q_rows, tiles):
    acc = total = None
    for keys, values in tiles:
        e = jnp.exp(dot_nt(q_rows, keys))
        part = e[:, :128] + e[:, 128:]
        out = dot_nn(e.astype(BF16), values)
        acc = out if acc is None else acc + out
        total = part if total is None else total + part
    return acc, total


def row_sum(lanes):
    return jnp.sum(lanes, axis=1, keepdims=True)


def out_of_range(*totals):
    good = [jnp.logical_and(jnp.min(t) > 1e-25, jnp.max(t) < 1e30) for t in totals]
    return jnp.logical_not(functools.reduce(jnp.logical_and, good))


def exact_head(q, half, n_keys, key_rows, acc_ref, m_ref, l_ref):
    low = low_lanes(q.shape[0])
    q1 = jnp.where(low if half == 0 else jnp.logical_not(low), q, jnp.zeros_like(q))
    acc_ref[half] = jnp.zeros(q.shape, F32)
    l_ref[half] = jnp.zeros(q.shape, F32)
    m_ref[half] = jnp.full(q.shape, FLOOR, F32)

    @pl.loop(0, n_keys // 256)
    def _(c):
        keys, values, bias = key_rows(c)
        s = dot_nt(q1, keys)
        if bias is not None:
            s = s + bias
        m_old = m_ref[half]
        m_new = jnp.maximum(m_old, jnp.max(s, axis=1, keepdims=True))
        alpha = jnp.exp(m_old - m_new)
        e = jnp.exp(s - m_new[:, :1])
        l_ref[half] = alpha * l_ref[half] + row_sum(e)
        acc_ref[half] = alpha * acc_ref[half] + dot_nn(e.astype(BF16), values)
        m_ref[half] = m_new


def window_kernel(q_ref, kl_ref, kc_ref, kr_ref, vl_ref, vc_ref, vr_ref, hkl_ref, hkr_ref, hvl_ref, hvr_ref,
                  extra_ref, bias_ref, kmax_ref, acc_ref, m_ref, l_ref, tri_ref, key_ref, val_ref, ea_ref, em_ref, el_ref):
    i = pl.program_id(1)
    n = q_ref.shape[0]
    is_first = i == 0
    is_last = i == pl.num_programs(1) - 1

    @pl.when(i == 0)
    def _():
        r_i = lax.broadcasted_iota(jnp.int32, (QB, QB), 0)
        c_i = lax.broadcasted_iota(jnp.int32, (QB, QB), 1)
        tri_ref[:QB] = jnp.where(c_i <= r_i, 0.0, -jnp.inf)
        tri_ref[QB:2 * QB] = jnp.zeros((QB, QB), F32)
        tri_ref[2 * QB:] = jnp.where(c_i >= r_i, 0.0, -jnp.inf)

    key_ref[:QB] = jnp.where(is_first, hkl_ref[...], kl_ref[...])
    key_ref[QB:QB + n] = kc_ref[...]
    key_ref[QB + n:] = jnp.where(is_last, hkr_ref[...], kr_ref[...])
    val_ref[:QB] = jnp.where(is_first, hvl_ref[...], vl_ref[...])
    val_ref[QB:QB + n] = vc_ref[...]
    val_ref[QB + n:] = jnp.where(is_last, hvr_ref[...], vr_ref[...])

    q = q_ref[...]
    neg = shifts(q, kmax_ref[...])
    accs, sums = [], []
    for half in range(2):
        qx = query_rows(q, neg, half)
        acc, total = [None] * (n // QB), [None] * (n // QB)
        for t in range(n // QB + 2):
            b0, b1 = max(t - 2, 0), min(t + 1, n // QB)
            extra = extra_ref[pl.ds(pl.multiple_of(i * n + t * QB, QB), QB), :]
            s = dot_nt(qx[b0 * QB:b1 * QB], own_half(key_ref[t * QB:(t + 1) * QB], extra, half))
            e = jnp.exp(s + window_mask(tri_ref, t, b0, b1))
            part = e[:, :128] + e[:, 128:]
            out = dot_nn(e.astype(BF16), val_ref[t * QB:(t + 1) * QB])
            for b in range(b0, b1):
                r = slice((b - b0) * QB, (b - b0 + 1) * QB)
                acc[b] = out[r] if acc[b] is None else acc[b] + out[r]
                total[b] = part[r] if total[b] is None else total[b] + part[r]
        accs.append(jnp.concatenate(acc, axis=0))
        sums.append(row_sum(jnp.concatenate(total, axis=0)))
    low = low_lanes(n)
    acc_ref[...] = jnp.where(low, accs[0], accs[1])
    l_ref[...] = jnp.where(low, sums[0], sums[1])
    m_ref[...] = -pltpu.roll(neg.astype(F32), 64, 1)

    @pl.when(out_of_range(*sums))
    def _():
        @pl.loop(0, n // QB)
        def _(b):
            rows = pl.ds(pl.multiple_of(b * QB, QB), QB)

            def key_rows(c):
                at = pl.ds(pl.multiple_of((b + c) * QB, QB), QB)
                bias = bias_ref[:, pl.ds(pl.multiple_of(i * n + (b + c) * QB, QB), QB)]
                return key_ref[at], val_ref[at], bias + tri_ref[pl.ds(pl.multiple_of((2 - c) * QB, QB), QB)]

            for half in range(2):
                exact_head(q_ref[rows], half, 3 * QB, key_rows, ea_ref, em_ref, el_ref)
            low = low_lanes(QB)
            for out, src in ((acc_ref, ea_ref), (m_ref, em_ref), (l_ref, el_ref)):
                out[rows] = jnp.where(low, src[0], src[1])


def window_mask(tri_ref, t, b0, b1):
    return tri_ref[(b0 - t + 2) * QB:(b1 - t + 2) * QB]


def window_part(qkv, halo_l, halo_r, extra, bias, kmax):
    n_rows = qkv.shape[0]
    rb = min(1024, n_rows)
    per = rb // QB
    n_blk, n_small = n_rows // rb, n_rows // QB
    mid = lambda c: pl.BlockSpec((rb, 128), lambda p, i: (i, 2 * c + p))
    left = lambda c: pl.BlockSpec((QB, 128), lambda p, i: (jnp.maximum(i * per - 1, 0), 2 * c + p))
    right = lambda c: pl.BlockSpec((QB, 128), lambda p, i: (jnp.minimum(i * per + per, n_small - 1), 2 * c + p))
    halo = lambda c: pl.BlockSpec((QB, 128), lambda p, i: (0, 2 * c + p))
    whole = lambda a: pl.BlockSpec(a.shape, lambda p, i: (0,) * a.ndim)
    out = jax.ShapeDtypeStruct((n_rows, 256), F32)
    pair = pltpu.VMEM((2, QB, 128), F32)
    return pl.pallas_call(
        window_kernel, grid=(2, n_blk),
        in_specs=[mid(0), left(1), mid(1), right(1), left(2), mid(2), right(2), halo(0), halo(0), halo(1), halo(1),
                  whole(extra), whole(bias), pl.BlockSpec((1, 128), lambda p, i: (0, p))],
        out_specs=[pl.BlockSpec((rb, 128), lambda p, i: (i, p))] * 3,
        out_shape=[out, out, out],
        scratch_shapes=[pltpu.VMEM((3 * QB, QB), F32), pltpu.VMEM((rb + 2 * QB, 128), BF16),
                        pltpu.VMEM((rb + 2 * QB, 128), BF16), pair, pair, pair],
        compiler_params=params(2), cost_estimate=cost(30e9, 30e6, 12e6), name="window_part",
    )(qkv, qkv, qkv, qkv, qkv, qkv, qkv, halo_l, halo_r, halo_l, halo_r, extra, bias, kmax)


def global_keys_kernel(q_ref, kg_ref, vg_ref, kmax_ref, acc_ref, m_ref, l_ref, idx_ref, glob_ref, out_ref,
                       k_ref, o_ref, ea_ref, em_ref, el_ref, *, first):
    n = q_ref.shape[0]
    i = pl.program_id(1)

    @pl.when(i == 0)
    def _():
        extra = key_extra(kg_ref.shape[0])
        for half in range(2):
            k_ref[half] = own_half(kg_ref[...], extra, half)

    def finish(acc, m, total):
        m_all = jnp.maximum(m, m_ref[...])
        a, b = jnp.exp(m - m_all), jnp.exp(m_ref[...] - m_all)
        o_ref[...] = (acc * a + acc_ref[...] * b) / (total * a + l_ref[...] * b)

    q = q_ref[...]
    neg = shifts(q, kmax_ref[...])
    low = low_lanes(n)
    res = [stream(query_rows(q, neg, half), [(k_ref[half, t:t + 256], vg_ref[t:t + 256]) for t in range(0, vg_ref.shape[0], 256)])
           for half in range(2)]
    sums = [row_sum(r[1]) for r in res]
    finish(jnp.where(low, res[0][0], res[1][0]), -pltpu.roll(neg.astype(F32), 64, 1), jnp.where(low, sums[0], sums[1]))

    @pl.when(out_of_range(*sums))
    def _():
        def key_rows(c):
            at = pl.ds(pl.multiple_of(c * 256, 256), 256)
            return kg_ref[at], vg_ref[at], None

        for half in range(2):
            exact_head(q_ref[...], half, vg_ref.shape[0], key_rows, ea_ref, em_ref, el_ref)
        finish(*(jnp.where(low, r[0], r[1]) for r in (ea_ref, em_ref, el_ref)))

    row = first * QB + i * n + lax.broadcasted_iota(jnp.int32, (n, 1), 0)
    hit = jnp.where(idx_ref[...] == row, 1.0, 0.0)
    placed = dot_nn(hit.astype(BF16), glob_ref[...])
    mine = row_sum(hit) > 0.5
    out_ref[...] = jnp.where(mine, placed, o_ref[...]).astype(out_ref.dtype)


def global_keys_part(qkv, qkv_g, kmax, win, local_idx, glob_out, first, n_blk):
    n_glob = qkv_g.shape[0]
    rb = min(512, n_blk * QB)
    base = first * QB // rb
    n_rows = n_blk * QB
    row = pl.BlockSpec((rb, 128), lambda p, i: (base + i, p))
    whole = lambda a: pl.BlockSpec(a.shape, lambda p, i: (0,) * a.ndim)
    idx = local_idx[None, :]
    pair = pltpu.VMEM((2, rb, 128), F32)
    return pl.pallas_call(
        functools.partial(global_keys_kernel, first=first), grid=(2, n_rows // rb),
        in_specs=[row, pl.BlockSpec((n_glob, 128), lambda p, i: (0, 2 + p)), pl.BlockSpec((n_glob, 128), lambda p, i: (0, 4 + p)),
                  pl.BlockSpec((1, 128), lambda p, i: (0, p)), row, row, row, whole(idx),
                  pl.BlockSpec((n_glob, 128), lambda p, i: (0, p))],
        out_specs=pl.BlockSpec((rb, 128), lambda p, i: (i, p)),
        out_shape=jax.ShapeDtypeStruct((n_rows, 256), BF16),
        scratch_shapes=[pltpu.VMEM((2, n_glob, 128), BF16), pltpu.VMEM((rb, 128), F32), pair, pair, pair],
        compiler_params=params(2), cost_estimate=cost(2.5e9 * n_blk, 2e6 * n_blk, 1e6 * n_blk),
        name="global_keys",
    )(qkv, qkv_g, qkv_g, kmax, *win, idx, glob_out)


def global_queries_kernel(q_ref, k_ref, v_ref, kmax_ref, out_ref, acc_ref, m_ref, l_ref, *, kb):
    j = pl.program_id(2)
    n = q_ref.shape[0]
    low = low_lanes(n)

    @pl.when(j == 0)
    def _():
        acc_ref[...] = jnp.zeros_like(acc_ref)
        l_ref[...] = jnp.zeros_like(l_ref)

    extra = key_extra(256)
    q = q_ref[...]
    neg = shifts(q, kmax_ref[...])
    for half in range(2):
        rows = [pl.ds(pl.multiple_of(j * kb, kb) + t, 256) for t in range(0, kb, 256)]
        acc, total = stream(query_rows(q, neg, half), [(own_half(k_ref[r], extra, half), v_ref[r]) for r in rows])
        acc_ref[half] += acc
        l_ref[half] += total

    @pl.when(j == pl.num_programs(2) - 1)
    def _():
        sums = [row_sum(l_ref[half]) for half in range(2)]
        out_ref[0] = jnp.where(low, acc_ref[0], acc_ref[1])
        out_ref[1] = -pltpu.roll(neg.astype(F32), 64, 1)
        out_ref[2] = jnp.where(low, sums[0], sums[1])

        @pl.when(out_of_range(*sums))
        def _():
            def key_rows(c):
                at = pl.ds(pl.multiple_of(c * 256, 256), 256)
                return k_ref[at], v_ref[at], None

            for half in range(2):
                exact_head(q_ref[...], half, v_ref.shape[0], key_rows, acc_ref, m_ref, l_ref)
            for k, r in enumerate((acc_ref, m_ref, l_ref)):
                out_ref[k] = jnp.where(low, r[0], r[1])


def global_queries_part(qkv_g, qkv, kmax):
    n_glob = qkv_g.shape[0]
    n_rows = qkv.shape[0]
    rb = 512
    kb = min(1024, n_rows)
    return pl.pallas_call(
        functools.partial(global_queries_kernel, kb=kb), grid=(2, n_glob // rb, n_rows // kb),
        in_specs=[pl.BlockSpec((rb, 128), lambda p, i, j: (i, p)), pl.BlockSpec((n_rows, 128), lambda p, i, j: (0, 2 + p)),
                  pl.BlockSpec((n_rows, 128), lambda p, i, j: (0, 4 + p)), pl.BlockSpec((1, 128), lambda p, i, j: (0, p))],
        out_specs=pl.BlockSpec((3, rb, 128), lambda p, i, j: (0, i, p)),
        out_shape=jax.ShapeDtypeStruct((3, n_glob, 256), F32),
        scratch_shapes=[pltpu.VMEM((2, rb, 128), F32)] * 3,
        compiler_params=params(3), cost_estimate=cost(34e9, 20e6, 16e6), name="global_queries",
    )(qkv_g, qkv, qkv, kmax)


def mlp_kernel(x_ref, o_ref, w_ref, *refs, n_tp, n_rep, d_o, d_f):
    y_ref, wo_ref, w2_ref, w1_ref, sem = refs[-5:]

    @pl.when(pl.program_id(0) == 0)
    def _():
        copies = []
        piece = wo_ref.shape[1] // n_rep
        for j in range(n_rep):
            for t in range(n_tp):
                lanes = pl.ds(j * piece, piece)
                copies.append(pltpu.make_async_copy(
                    w_ref.at[j, t, pl.ds(0, d_o)], wo_ref.at[pl.ds(t * d_o, d_o), lanes], sem))
                copies.append(pltpu.make_async_copy(
                    w_ref.at[j, t, pl.ds(d_o, d_f)], w2_ref.at[pl.ds(t * d_f, d_f), lanes], sem))
                copies.append(pltpu.make_async_copy(
                    w_ref.at[j, t, pl.ds(d_o + d_f, d_f)], w1_ref.at[pl.ds(t * d_f, d_f), lanes], sem))
        for c in copies:
            c.start()
        for c in copies:
            c.wait()

    mixed = dot_nn(o_ref[0], wo_ref[:d_o, :])
    for t in range(1, n_tp):
        mixed += dot_nn(o_ref[t], wo_ref[t * d_o:(t + 1) * d_o, :])
    h = (x_ref[...].astype(F32) + mixed).astype(BF16)
    width = n_tp * d_f
    acc = h.astype(F32)
    for f0 in range(0, width, 512):
        f1 = min(f0 + 512, width)
        z = dot_nt(h, w1_ref[f0:f1, :])
        u = 0.5 * z * (1.0 + jnp.tanh(math.sqrt(2.0 / math.pi) * (z + 0.044715 * (z * z * z))))
        acc += dot_nn(u.astype(BF16), w2_ref[f0:f1, :])
    y_ref[...] = acc.astype(y_ref.dtype)


def mlp_rows(tokens, o_all, w_all, y, first, d_o, d_f):
    n_tp, n_rows, _ = o_all.shape
    n_rep = w_all.shape[0]
    dim = tokens.shape[1]
    rb = min(512, n_rows)
    n_blk = n_rows // rb
    base = first * QB // rb
    earlier = () if y is None else (y,)
    return pl.pallas_call(
        functools.partial(mlp_kernel, n_tp=n_tp, n_rep=n_rep, d_o=d_o, d_f=d_f), grid=(n_blk,),
        in_specs=[pl.BlockSpec((rb, dim), lambda i: (base + i, 0)),
                  pl.BlockSpec((n_tp, rb, d_o), lambda i: (0, i, 0)),
                  pl.BlockSpec(memory_space=pl.ANY)] + [pl.BlockSpec(memory_space=pl.ANY)] * len(earlier),
        out_specs=pl.BlockSpec((rb, dim), lambda i: (base + i, 0)),
        out_shape=jax.ShapeDtypeStruct(tokens.shape, BF16),
        input_output_aliases={3: 0} if earlier else {},
        scratch_shapes=[pltpu.VMEM((n_tp * d_o, dim), BF16), pltpu.VMEM((n_tp * d_f, dim), BF16),
                        pltpu.VMEM((n_tp * d_f, dim), BF16), pltpu.SemaphoreType.DMA],
        compiler_params=params(1, 56), cost_estimate=cost(2 * n_rows * dim * (dim + 2 * n_tp * d_f), 20e6), name="mlp",
    )(tokens, o_all, w_all, *earlier)


def combine(a, b):
    m = jnp.maximum(a[1], b[1])
    e_a, e_b = jnp.exp(a[1] - m), jnp.exp(b[1] - m)
    return a[0] * e_a + b[0] * e_b, m, a[2] * e_a + b[2] * e_b


def solution(mesh):
    n_seq = mesh.shape['sp']
    to_right = [(i, i + 1) for i in range(n_seq - 1)]
    to_left = [(i + 1, i) for i in range(n_seq - 1)]
    core_swap = [(i, i ^ 1) for i in range(n_seq)]
    chip_swap = [(i, i ^ 2) for i in range(n_seq)]

    def device_layer(tokens, glob_pos, w_query, w_key, w_value, w_out, w_up, w_down):
        n_rows, dim = tokens.shape
        n_glob = glob_pos.shape[0]
        sp = lax.axis_index('sp')
        core, chip = sp % 2, sp // 2
        first_row = sp * n_rows
        seq_len = n_rows * n_seq
        local_idx = glob_pos - first_row

        d_o, d_f = w_out.shape[0] * w_out.shape[1], w_down.shape[0]
        shard = jnp.concatenate([w_out.reshape(d_o, dim), w_down, w_up.T], axis=0)
        rep = lax.axis_index('dp') * n_seq + sp
        n_tp, n_rep = mesh.shape['tp'], mesh.shape['dp'] * n_seq
        piece = dim // n_rep
        w_slice = lax.dynamic_slice_in_dim(shard, rep * piece, piece, axis=1)
        w_all = lax.all_gather(w_slice, ('dp', 'sp', 'tp'))
        w_all = w_all.reshape(n_rep, n_tp, d_o + 2 * d_f, piece)

        w_cat = jnp.concatenate([w_query.reshape(dim, -1) * jnp.asarray(0.125, BF16),
                                 w_key.reshape(dim, -1), w_value.reshape(dim, -1)], axis=1)
        qkv, picked, kmax = qkv_part(tokens, w_cat, local_idx)
        halo_l = lax.ppermute(qkv[n_rows - WIN:, 256:], 'sp', to_right)
        halo_r = lax.ppermute(qkv[:WIN, 256:], 'sp', to_left)

        k_pos = first_row - WIN + jnp.arange(n_rows + 2 * WIN)
        k_off = jnp.any(glob_pos[:, None] == k_pos[None, :], axis=0) | (k_pos < 0) | (k_pos >= seq_len)
        bias = jnp.where(k_off, -jnp.inf, 0.0).astype(F32)[None, :]
        lane = jnp.arange(128) % 64
        extra = jnp.where(lane == 0, 1.0, jnp.where((lane == 1) & k_off[:, None], FLOOR, 0.0)).astype(BF16)

        half = n_glob // 2
        mine = lax.dynamic_slice_in_dim(picked, core * half, half)
        other = lax.ppermute(lax.dynamic_slice_in_dim(picked, (1 - core) * half, half), 'sp', core_swap)
        mine = mine + other
        got = lax.ppermute(mine, 'sp', chip_swap)
        win = window_part(qkv, halo_l, halo_r, extra, bias, kmax)
        got, win = lax.optimization_barrier((got, win))
        mine = mine + got
        other = lax.ppermute(mine, 'sp', core_swap)
        qkv_g = jnp.concatenate([jnp.where(core == 0, mine, other), jnp.where(core == 0, other, mine)], axis=0)

        part = global_queries_part(qkv_g, qkv, kmax)

        quarter = n_glob // 4
        got = lax.ppermute(lax.dynamic_slice_in_dim(part, (1 - core) * half, half, axis=1), 'sp', core_swap)
        joined = jnp.stack(combine(lax.dynamic_slice_in_dim(part, core * half, half, axis=1), got))
        got = lax.ppermute(lax.dynamic_slice_in_dim(joined, (1 - chip) * quarter, quarter, axis=1), 'sp', chip_swap)
        g_acc, _, g_l = combine(lax.dynamic_slice_in_dim(joined, chip * quarter, quarter, axis=1), got)
        mine = (g_acc / g_l).astype(BF16)
        other = lax.ppermute(mine, 'sp', chip_swap)
        mine = jnp.concatenate([jnp.where(chip == 0, mine, other), jnp.where(chip == 0, other, mine)], axis=0)
        other = lax.ppermute(mine, 'sp', core_swap)
        glob_out = jnp.concatenate([jnp.where(core == 0, mine, other), jnp.where(core == 0, other, mine)], axis=0)

        glob_out, w_all = lax.optimization_barrier((glob_out, w_all))
        y, first = None, 0
        for n_blk in CHUNKS if n_rows == 16 * QB else (n_rows // QB // 2,) * 2:
            o = global_keys_part(qkv, qkv_g, kmax, win, local_idx, glob_out, first, n_blk)
            o_all = lax.all_gather(o, 'tp')
            y = mlp_rows(tokens, o_all, w_all, y, first, d_o, d_f)
            first += n_blk
        return y

    row_spec = P(('dp', 'sp'), None)
    head_spec = P(None, 'tp', None)
    in_specs = (row_spec, P('dp'), head_spec, head_spec, head_spec, P('tp', None, None), P(None, 'tp'), P('tp', None))
    return jax.shard_map(device_layer, mesh=mesh, in_specs=in_specs, out_specs=row_spec, check_vma=False)
```

```python
import functools
import math

import jax
import jax.numpy as jnp
from jax import lax
from jax.experimental import pallas as pl
from jax.experimental.pallas import tpu as pltpu
from jax.sharding import PartitionSpec as P

WIN = 256
QB = 256
FLOOR = -3.0e38
F32 = jnp.float32
BF16 = jnp.bfloat16
NT = (((1,), (1,)), ((), ()))


def dot_nt(a, b):
    return lax.dot_general(a, b, NT, preferred_element_type=F32)


def dot_nn(a, b):
    return jnp.dot(a, b, preferred_element_type=F32)


def params(n_axes, vmem_mib=48):
    return pltpu.CompilerParams(
        dimension_semantics=("arbitrary",) * n_axes, vmem_limit_bytes=vmem_mib << 20)


def cost(flops, bytes_accessed, exps=0):
    return pl.CostEstimate(flops=int(flops), bytes_accessed=int(bytes_accessed), transcendentals=int(exps))


def head_sums(rows):
    n = rows.shape[1]
    r = lax.broadcasted_iota(jnp.int32, (n, n), 0) // 64
    c = lax.broadcasted_iota(jnp.int32, (n, n), 1) // 64
    pick = jnp.where(r == (c + 1 - 2 * (c % 2)), 1.0, 0.0).astype(BF16)
    wide = rows.astype(F32)
    return dot_nn((wide * wide).astype(BF16), pick)


def qkv_kernel(pos_ref, idx_ref, x_ref, w_ref, qkv_ref, pick_ref, kmax_ref, acc_ref):
    step = pl.program_id(0)
    n_blk = x_ref.shape[0]
    lo = step * n_blk
    gb = 128

    @pl.when(step == 0)
    def _():
        acc_ref[...] = jnp.zeros_like(acc_ref)
        kmax_ref[...] = jnp.zeros_like(kmax_ref)

    rows = dot_nn(x_ref[...], w_ref[...]).astype(BF16)
    qkv_ref[...] = rows
    kmax_ref[...] = jnp.maximum(kmax_ref[...], jnp.max(head_sums(rows[:, 256:512]), axis=0, keepdims=True))

    @pl.loop(0, idx_ref.shape[0] // gb)
    def _(b):
        g0 = pl.multiple_of(b * gb, gb)

        @pl.when((pos_ref[g0] < lo + n_blk) & (pos_ref[g0 + gb - 1] >= lo))
        def _():
            hit = idx_ref[pl.ds(g0, gb), :] == lo + lax.broadcasted_iota(jnp.int32, (gb, n_blk), 1)
            acc_ref[pl.ds(g0, gb), :] += dot_nn(hit.astype(F32).astype(BF16), qkv_ref[...])

    @pl.when(step == pl.num_programs(0) - 1)
    def _():
        pick_ref[...] = acc_ref[...].astype(pick_ref.dtype)


def qkv_part(tokens, w_cat, local_idx):
    n_rows, dim = tokens.shape
    n_glob = local_idx.shape[0]
    width = w_cat.shape[1]
    rb = 512
    return pl.pallas_call(
        qkv_kernel,
        grid_spec=pltpu.PrefetchScalarGridSpec(
            num_scalar_prefetch=1, grid=(n_rows // rb,),
            in_specs=[pl.BlockSpec((n_glob, 1), lambda i, p: (0, 0)), pl.BlockSpec((rb, dim), lambda i, p: (i, 0)),
                      pl.BlockSpec((dim, width), lambda i, p: (0, 0))],
            out_specs=[pl.BlockSpec((rb, width), lambda i, p: (i, 0)), pl.BlockSpec((n_glob, width), lambda i, p: (0, 0)),
                       pl.BlockSpec((1, 256), lambda i, p: (0, 0))],
            scratch_shapes=[pltpu.VMEM((n_glob, width), F32)]),
        out_shape=[jax.ShapeDtypeStruct((n_rows, width), BF16), jax.ShapeDtypeStruct((n_glob, width), BF16),
                   jax.ShapeDtypeStruct((1, 256), F32)],
        compiler_params=params(1), cost_estimate=cost(8e9, 24e6), name="qkv",
    )(local_idx, local_idx[:, None], tokens, w_cat)


def low_lanes(n):
    return lax.broadcasted_iota(jnp.int32, (n, 128), 1) < 64


def shifts(q, kmax):
    return (-1.02 * jnp.sqrt(head_sums(q) * kmax)).astype(BF16)


def own_half(pair, other, half):
    low = low_lanes(pair.shape[0])
    return jnp.where(low, pair, other) if half == 0 else jnp.where(low, other, pair)


def query_rows(q, neg, half):
    lane = lax.broadcasted_iota(jnp.int32, q.shape, 1) % 64
    return own_half(q, jnp.where(lane == 0, neg, jnp.ones_like(neg)), half)


def key_extra(n):
    return jnp.where(lax.broadcasted_iota(jnp.int32, (n, 128), 1) % 64 == 0, 1.0, 0.0).astype(BF16)


def stream(q_rows, tiles):
    acc = total = None
    for keys, values in tiles:
        e = jnp.exp(dot_nt(q_rows, keys))
        part = e[:, :128] + e[:, 128:]
        out = dot_nn(e.astype(BF16), values)
        acc = out if acc is None else acc + out
        total = part if total is None else total + part
    return acc, total


def row_sum(lanes):
    return jnp.sum(lanes, axis=1, keepdims=True)


def out_of_range(*totals):
    good = [jnp.logical_and(jnp.min(t) > 1e-25, jnp.max(t) < 1e30) for t in totals]
    return jnp.logical_not(functools.reduce(jnp.logical_and, good))


def exact_head(q, half, n_keys, key_rows, acc_ref, m_ref, l_ref):
    low = low_lanes(q.shape[0])
    q1 = jnp.where(low if half == 0 else jnp.logical_not(low), q, jnp.zeros_like(q))
    acc_ref[half] = jnp.zeros(q.shape, F32)
    l_ref[half] = jnp.zeros(q.shape, F32)
    m_ref[half] = jnp.full(q.shape, FLOOR, F32)

    @pl.loop(0, n_keys // 256)
    def _(c):
        keys, values, bias = key_rows(c)
        s = dot_nt(q1, keys)
        if bias is not None:
            s = s + bias
        m_old = m_ref[half]
        m_new = jnp.maximum(m_old, jnp.max(s, axis=1, keepdims=True))
        alpha = jnp.exp(m_old - m_new)
        e = jnp.exp(s - m_new[:, :1])
        l_ref[half] = alpha * l_ref[half] + row_sum(e)
        acc_ref[half] = alpha * acc_ref[half] + dot_nn(e.astype(BF16), values)
        m_ref[half] = m_new


def window_kernel(q_ref, kl_ref, kc_ref, kr_ref, vl_ref, vc_ref, vr_ref, hkl_ref, hkr_ref, hvl_ref, hvr_ref,
                  extra_ref, bias_ref, kmax_ref, acc_ref, m_ref, l_ref, tri_ref, key_ref, val_ref, ea_ref, em_ref, el_ref):
    i = pl.program_id(1)
    n = q_ref.shape[0]
    is_first = i == 0
    is_last = i == pl.num_programs(1) - 1

    @pl.when(i == 0)
    def _():
        r_i = lax.broadcasted_iota(jnp.int32, (QB, QB), 0)
        c_i = lax.broadcasted_iota(jnp.int32, (QB, QB), 1)
        tri_ref[:QB] = jnp.where(c_i <= r_i, 0.0, -jnp.inf)
        tri_ref[QB:2 * QB] = jnp.zeros((QB, QB), F32)
        tri_ref[2 * QB:] = jnp.where(c_i >= r_i, 0.0, -jnp.inf)

    key_ref[:QB] = jnp.where(is_first, hkl_ref[...], kl_ref[...])
    key_ref[QB:QB + n] = kc_ref[...]
    key_ref[QB + n:] = jnp.where(is_last, hkr_ref[...], kr_ref[...])
    val_ref[:QB] = jnp.where(is_first, hvl_ref[...], vl_ref[...])
    val_ref[QB:QB + n] = vc_ref[...]
    val_ref[QB + n:] = jnp.where(is_last, hvr_ref[...], vr_ref[...])

    q = q_ref[...]
    neg = shifts(q, kmax_ref[...])
    accs, sums = [], []
    for half in range(2):
        qx = query_rows(q, neg, half)
        acc, total = [None] * (n // QB), [None] * (n // QB)
        for t in range(n // QB + 2):
            b0, b1 = max(t - 2, 0), min(t + 1, n // QB)
            extra = extra_ref[pl.ds(pl.multiple_of(i * n + t * QB, QB), QB), :]
            s = dot_nt(qx[b0 * QB:b1 * QB], own_half(key_ref[t * QB:(t + 1) * QB], extra, half))
            e = jnp.exp(s + window_mask(tri_ref, t, b0, b1))
            part = e[:, :128] + e[:, 128:]
            out = dot_nn(e.astype(BF16), val_ref[t * QB:(t + 1) * QB])
            for b in range(b0, b1):
                r = slice((b - b0) * QB, (b - b0 + 1) * QB)
                acc[b] = out[r] if acc[b] is None else acc[b] + out[r]
                total[b] = part[r] if total[b] is None else total[b] + part[r]
        accs.append(jnp.concatenate(acc, axis=0))
        sums.append(row_sum(jnp.concatenate(total, axis=0)))
    low = low_lanes(n)
    acc_ref[...] = jnp.where(low, accs[0], accs[1])
    l_ref[...] = jnp.where(low, sums[0], sums[1])
    m_ref[...] = -pltpu.roll(neg.astype(F32), 64, 1)

    @pl.when(out_of_range(*sums))
    def _():
        @pl.loop(0, n // QB)
        def _(b):
            rows = pl.ds(pl.multiple_of(b * QB, QB), QB)

            def key_rows(c):
                at = pl.ds(pl.multiple_of((b + c) * QB, QB), QB)
                bias = bias_ref[:, pl.ds(pl.multiple_of(i * n + (b + c) * QB, QB), QB)]
                return key_ref[at], val_ref[at], bias + tri_ref[pl.ds(pl.multiple_of((2 - c) * QB, QB), QB)]

            for half in range(2):
                exact_head(q_ref[rows], half, 3 * QB, key_rows, ea_ref, em_ref, el_ref)
            low = low_lanes(QB)
            for out, src in ((acc_ref, ea_ref), (m_ref, em_ref), (l_ref, el_ref)):
                out[rows] = jnp.where(low, src[0], src[1])


def window_mask(tri_ref, t, b0, b1):
    return tri_ref[(b0 - t + 2) * QB:(b1 - t + 2) * QB]


def window_part(qkv, halo_l, halo_r, extra, bias, kmax):
    n_rows = qkv.shape[0]
    rb = min(1024, n_rows)
    per = rb // QB
    n_blk, n_small = n_rows // rb, n_rows // QB
    mid = lambda c: pl.BlockSpec((rb, 128), lambda p, i: (i, 2 * c + p))
    left = lambda c: pl.BlockSpec((QB, 128), lambda p, i: (jnp.maximum(i * per - 1, 0), 2 * c + p))
    right = lambda c: pl.BlockSpec((QB, 128), lambda p, i: (jnp.minimum(i * per + per, n_small - 1), 2 * c + p))
    halo = lambda c: pl.BlockSpec((QB, 128), lambda p, i: (0, 2 * c + p))
    whole = lambda a: pl.BlockSpec(a.shape, lambda p, i: (0,) * a.ndim)
    out = jax.ShapeDtypeStruct((n_rows, 256), F32)
    pair = pltpu.VMEM((2, QB, 128), F32)
    return pl.pallas_call(
        window_kernel, grid=(2, n_blk),
        in_specs=[mid(0), left(1), mid(1), right(1), left(2), mid(2), right(2), halo(0), halo(0), halo(1), halo(1),
                  whole(extra), whole(bias), pl.BlockSpec((1, 128), lambda p, i: (0, p))],
        out_specs=[pl.BlockSpec((rb, 128), lambda p, i: (i, p))] * 3,
        out_shape=[out, out, out],
        scratch_shapes=[pltpu.VMEM((3 * QB, QB), F32), pltpu.VMEM((rb + 2 * QB, 128), BF16),
                        pltpu.VMEM((rb + 2 * QB, 128), BF16), pair, pair, pair],
        compiler_params=params(2), cost_estimate=cost(30e9, 30e6, 12e6), name="window_part",
    )(qkv, qkv, qkv, qkv, qkv, qkv, qkv, halo_l, halo_r, halo_l, halo_r, extra, bias, kmax)


def global_keys_kernel(q_ref, kg_ref, vg_ref, kmax_ref, acc_ref, m_ref, l_ref, out_ref,
                       k_ref, ea_ref, em_ref, el_ref):
    n = q_ref.shape[0]
    i = pl.program_id(1)

    @pl.when(i == 0)
    def _():
        extra = key_extra(kg_ref.shape[0])
        for half in range(2):
            k_ref[half] = own_half(kg_ref[...], extra, half)

    def finish(acc, m, total):
        m_all = jnp.maximum(m, m_ref[...])
        a, b = jnp.exp(m - m_all), jnp.exp(m_ref[...] - m_all)
        out_ref[...] = ((acc * a + acc_ref[...] * b) / (total * a + l_ref[...] * b)).astype(out_ref.dtype)

    q = q_ref[...]
    neg = shifts(q, kmax_ref[...])
    low = low_lanes(n)
    res = [stream(query_rows(q, neg, half), [(k_ref[half, t:t + 256], vg_ref[t:t + 256]) for t in range(0, vg_ref.shape[0], 256)])
           for half in range(2)]
    sums = [row_sum(r[1]) for r in res]
    finish(jnp.where(low, res[0][0], res[1][0]), -pltpu.roll(neg.astype(F32), 64, 1), jnp.where(low, sums[0], sums[1]))

    @pl.when(out_of_range(*sums))
    def _():
        def key_rows(c):
            at = pl.ds(pl.multiple_of(c * 256, 256), 256)
            return kg_ref[at], vg_ref[at], None

        for half in range(2):
            exact_head(q_ref[...], half, vg_ref.shape[0], key_rows, ea_ref, em_ref, el_ref)
        finish(*(jnp.where(low, r[0], r[1]) for r in (ea_ref, em_ref, el_ref)))


def global_keys_part(qkv, qkv_g, kmax, win):
    n_rows, n_glob = qkv.shape[0], qkv_g.shape[0]
    rb = 512
    row = pl.BlockSpec((rb, 128), lambda p, i: (i, p))
    pair = pltpu.VMEM((2, rb, 128), F32)
    return pl.pallas_call(
        global_keys_kernel, grid=(2, n_rows // rb),
        in_specs=[row, pl.BlockSpec((n_glob, 128), lambda p, i: (0, 2 + p)), pl.BlockSpec((n_glob, 128), lambda p, i: (0, 4 + p)),
                  pl.BlockSpec((1, 128), lambda p, i: (0, p)), row, row, row],
        out_specs=row, out_shape=jax.ShapeDtypeStruct((n_rows, 256), BF16),
        scratch_shapes=[pltpu.VMEM((2, n_glob, 128), BF16), pair, pair, pair],
        compiler_params=params(2), cost_estimate=cost(40e9, 32e6, 16e6), name="global_keys",
    )(qkv, qkv_g, qkv_g, kmax, *win)


def place_kernel(idx_ref, glob_ref, o_ref, out_ref):
    n = o_ref.shape[0]
    row = pl.program_id(0) * n + lax.broadcasted_iota(jnp.int32, (n, 1), 0)
    hit = jnp.where(idx_ref[...] == row, 1.0, 0.0)
    placed = dot_nn(hit.astype(BF16), glob_ref[...])
    out_ref[...] = jnp.where(row_sum(hit) > 0.5, placed, o_ref[...].astype(F32)).astype(out_ref.dtype)


def place_rows(o, glob_out, local_idx):
    n_rows, width = o.shape
    n_glob = local_idx.shape[0]
    rb = 512
    return pl.pallas_call(
        place_kernel, grid=(n_rows // rb,),
        in_specs=[pl.BlockSpec((1, n_glob), lambda i: (0, 0)), pl.BlockSpec((n_glob, width), lambda i: (0, 0)),
                  pl.BlockSpec((rb, width), lambda i: (i, 0))],
        out_specs=pl.BlockSpec((rb, width), lambda i: (i, 0)),
        out_shape=jax.ShapeDtypeStruct((n_rows, width), BF16),
        compiler_params=params(1), cost_estimate=cost(2e9, 5e6), name="place",
    )(local_idx[None, :], glob_out, o)


def global_queries_kernel(q_ref, k_ref, v_ref, kmax_ref, out_ref, acc_ref, m_ref, l_ref, *, kb):
    j = pl.program_id(2)
    n = q_ref.shape[0]
    low = low_lanes(n)

    @pl.when(j == 0)
    def _():
        acc_ref[...] = jnp.zeros_like(acc_ref)
        l_ref[...] = jnp.zeros_like(l_ref)

    extra = key_extra(256)
    q = q_ref[...]
    neg = shifts(q, kmax_ref[...])
    for half in range(2):
        rows = [pl.ds(pl.multiple_of(j * kb, kb) + t, 256) for t in range(0, kb, 256)]
        acc, total = stream(query_rows(q, neg, half), [(own_half(k_ref[r], extra, half), v_ref[r]) for r in rows])
        acc_ref[half] += acc
        l_ref[half] += total

    @pl.when(j == pl.num_programs(2) - 1)
    def _():
        sums = [row_sum(l_ref[half]) for half in range(2)]
        out_ref[0] = jnp.where(low, acc_ref[0], acc_ref[1])
        out_ref[1] = -pltpu.roll(neg.astype(F32), 64, 1)
        out_ref[2] = jnp.where(low, sums[0], sums[1])

        @pl.when(out_of_range(*sums))
        def _():
            def key_rows(c):
                at = pl.ds(pl.multiple_of(c * 256, 256), 256)
                return k_ref[at], v_ref[at], None

            for half in range(2):
                exact_head(q_ref[...], half, v_ref.shape[0], key_rows, acc_ref, m_ref, l_ref)
            for k, r in enumerate((acc_ref, m_ref, l_ref)):
                out_ref[k] = jnp.where(low, r[0], r[1])


def global_queries_part(qkv_g, qkv, kmax):
    n_glob = qkv_g.shape[0]
    n_rows = qkv.shape[0]
    rb = 512
    kb = min(1024, n_rows)
    return pl.pallas_call(
        functools.partial(global_queries_kernel, kb=kb), grid=(2, n_glob // rb, n_rows // kb),
        in_specs=[pl.BlockSpec((rb, 128), lambda p, i, j: (i, p)), pl.BlockSpec((n_rows, 128), lambda p, i, j: (0, 2 + p)),
                  pl.BlockSpec((n_rows, 128), lambda p, i, j: (0, 4 + p)), pl.BlockSpec((1, 128), lambda p, i, j: (0, p))],
        out_specs=pl.BlockSpec((3, rb, 128), lambda p, i, j: (0, i, p)),
        out_shape=jax.ShapeDtypeStruct((3, n_glob, 256), F32),
        scratch_shapes=[pltpu.VMEM((2, rb, 128), F32)] * 3,
        compiler_params=params(3), cost_estimate=cost(34e9, 20e6, 16e6), name="global_queries",
    )(qkv_g, qkv, qkv, kmax)


def exchange_mlp_kernel(x_hbm, o_hbm, w_hbm, y_hbm, x_ref, o_ref, wo_ref, w2_ref, w1_ref, load_sem, y_sem,
                        up_send, up_recv, down_send, down_recv, *, n_tp, n_rep, d_o, d_f, rb):
    me = lax.axis_index('tp')
    n_blk = x_ref.shape[0] // rb
    width = n_tp * d_f

    barrier = pltpu.get_barrier_semaphore()

    @pl.when(me > 0)
    def _():
        pl.semaphore_signal(barrier, inc=1, device_id={'tp': me - 1}, device_id_type=pl.DeviceIdType.MESH)

    @pl.when(me < n_tp - 1)
    def _():
        pl.semaphore_signal(barrier, inc=1, device_id={'tp': me + 1}, device_id_type=pl.DeviceIdType.MESH)

    own = pltpu.make_async_copy(o_hbm, o_ref.at[me], load_sem.at[0])
    own.start()
    copies = [pltpu.make_async_copy(x_hbm, x_ref, load_sem.at[1])]
    piece = wo_ref.shape[1] // n_rep
    for j in range(n_rep):
        for t in range(n_tp):
            lanes = pl.ds(j * piece, piece)
            for src, n, dst in ((0, d_o, wo_ref), (d_o, d_f, w2_ref), (d_o + d_f, d_f, w1_ref)):
                copies.append(pltpu.make_async_copy(w_hbm.at[j, t, pl.ds(src, n)], dst.at[pl.ds(t * n, n), lanes],
                                                    load_sem.at[2 + len(copies)]))
    for c in copies:
        c.start()

    ends = jnp.logical_or(me == 0, me == n_tp - 1)

    @pl.when(ends)
    def _():
        pl.semaphore_wait(barrier, 1)

    @pl.when(jnp.logical_not(ends))
    def _():
        pl.semaphore_wait(barrier, 2)

    own.wait()

    def rows_of(b):
        return pl.ds(pl.multiple_of(b * rb, rb), rb)

    def up(d, b):
        at = o_ref.at[me - d, rows_of(b)]
        return pltpu.make_async_remote_copy(at, at, up_send.at[d, b], up_recv.at[d, b], device_id={'tp': me + 1},
                                            device_id_type=pl.DeviceIdType.MESH)

    def down(d, b):
        at = o_ref.at[me + d, rows_of(b)]
        return pltpu.make_async_remote_copy(at, at, down_send.at[d, b], down_recv.at[d, b], device_id={'tp': me - 1},
                                            device_id_type=pl.DeviceIdType.MESH)

    def landed(recv, d, shard, b):
        at = o_ref.at[shard, rows_of(b)]
        pltpu.make_async_remote_copy(at, at, up_send.at[0, b], recv.at[d - 1, b], device_id={'tp': me},
                                     device_id_type=pl.DeviceIdType.MESH).wait_recv()

    def send_own(b):
        @pl.when(me < n_tp - 1)
        def _():
            up(0, b).start()

        @pl.when(me > 0)
        def _():
            down(0, b).start()

    ahead = min(2, n_blk)
    for b in range(ahead):
        send_own(b)

    def step(s, carry):
        @pl.when(s + ahead < n_blk)
        def _():
            send_own(s + ahead)

        for d in range(1, n_tp):
            b = s - (d - 1)

            @pl.when((b >= 0) & (b < n_blk) & (me >= d))
            def _():
                landed(up_recv, d, me - d, b)
                if d < n_tp - 1:
                    @pl.when(me < n_tp - 1)
                    def _():
                        up(d, b).start()

            @pl.when((b >= 0) & (b < n_blk) & (me + d <= n_tp - 1))
            def _():
                landed(down_recv, d, me + d, b)
                if d < n_tp - 1:
                    @pl.when(me > 0)
                    def _():
                        down(d, b).start()

        @pl.when(s == n_tp - 2)
        def _():
            for c in copies:
                c.wait()

        @pl.when(s >= n_tp - 2)
        def _():
            b = s - (n_tp - 2)
            rows = rows_of(b)
            mixed = dot_nn(o_ref[0, rows], wo_ref[:d_o, :])
            for t in range(1, n_tp):
                mixed += dot_nn(o_ref[t, rows], wo_ref[t * d_o:(t + 1) * d_o, :])
            h = (x_ref[rows].astype(F32) + mixed).astype(BF16)
            acc = h.astype(F32)
            for f0 in range(0, width, 512):
                f1 = min(f0 + 512, width)
                z = dot_nt(h, w1_ref[f0:f1, :])
                u = 0.5 * z * (1.0 + jnp.tanh(math.sqrt(2.0 / math.pi) * (z + 0.044715 * (z * z * z))))
                acc += dot_nn(u.astype(BF16), w2_ref[f0:f1, :])
            x_ref[rows] = acc.astype(BF16)
            pltpu.make_async_copy(x_ref.at[rows], y_hbm.at[rows], y_sem.at[b]).start()

        return carry

    lax.fori_loop(0, n_blk + n_tp - 2, step, 0)

    def finish(b, carry):
        rows = rows_of(b)
        pltpu.make_async_copy(x_ref.at[rows], y_hbm.at[rows], y_sem.at[b]).wait()
        for d in range(n_tp - 1):
            @pl.when((me < n_tp - 1) & (me >= d))
            def _():
                up(d, b).wait_send()

            @pl.when((me > 0) & (me + d <= n_tp - 1))
            def _():
                down(d, b).wait_send()

        return carry

    lax.fori_loop(0, n_blk, finish, 0)


def exchange_mlp(tokens, o, w_all, n_tp, d_o, d_f):
    n_rows, dim = tokens.shape
    n_rep = w_all.shape[0]
    rb = min(512, n_rows // 2)
    n_blk = n_rows // rb
    anywhere = pl.BlockSpec(memory_space=pl.ANY)
    dma = pltpu.SemaphoreType.DMA
    return pl.pallas_call(
        functools.partial(exchange_mlp_kernel, n_tp=n_tp, n_rep=n_rep, d_o=d_o, d_f=d_f, rb=rb),
        in_specs=[anywhere] * 3, out_specs=anywhere, out_shape=jax.ShapeDtypeStruct(tokens.shape, BF16),
        scratch_shapes=[pltpu.VMEM((n_rows, dim), BF16), pltpu.VMEM((n_tp, n_rows, d_o), BF16),
                        pltpu.VMEM((n_tp * d_o, dim), BF16), pltpu.VMEM((n_tp * d_f, dim), BF16),
                        pltpu.VMEM((n_tp * d_f, dim), BF16), dma((2 + 3 * n_rep * n_tp + 1,)), dma((n_blk,)),
                        dma((n_tp - 1, n_blk)), dma((n_tp - 1, n_blk)), dma((n_tp - 1, n_blk)), dma((n_tp - 1, n_blk))],
        compiler_params=pltpu.CompilerParams(collective_id=1, has_side_effects=True, vmem_limit_bytes=56 << 20),
        cost_estimate=cost(2 * n_rows * dim * (dim + 2 * n_tp * d_f), 40e6), name="exchange_mlp",
    )(tokens, o, w_all)


def combine(a, b):
    m = jnp.maximum(a[1], b[1])
    e_a, e_b = jnp.exp(a[1] - m), jnp.exp(b[1] - m)
    return a[0] * e_a + b[0] * e_b, m, a[2] * e_a + b[2] * e_b


def solution(mesh):
    n_seq = mesh.shape['sp']
    to_right = [(i, i + 1) for i in range(n_seq - 1)]
    to_left = [(i + 1, i) for i in range(n_seq - 1)]
    core_swap = [(i, i ^ 1) for i in range(n_seq)]
    chip_swap = [(i, i ^ 2) for i in range(n_seq)]

    def device_layer(tokens, glob_pos, w_query, w_key, w_value, w_out, w_up, w_down):
        n_rows, dim = tokens.shape
        n_glob = glob_pos.shape[0]
        sp = lax.axis_index('sp')
        core, chip = sp % 2, sp // 2
        first_row = sp * n_rows
        seq_len = n_rows * n_seq
        local_idx = glob_pos - first_row

        d_o, d_f = w_out.shape[0] * w_out.shape[1], w_down.shape[0]
        shard = jnp.concatenate([w_out.reshape(d_o, dim), w_down, w_up.T], axis=0)
        rep = lax.axis_index('dp') * n_seq + sp
        n_tp, n_rep = mesh.shape['tp'], mesh.shape['dp'] * n_seq
        piece = dim // n_rep
        w_slice = lax.dynamic_slice_in_dim(shard, rep * piece, piece, axis=1)
        w_all = lax.all_gather(w_slice, ('dp', 'sp', 'tp'))
        w_all = w_all.reshape(n_rep, n_tp, d_o + 2 * d_f, piece)

        w_cat = jnp.concatenate([w_query.reshape(dim, -1) * jnp.asarray(0.125, BF16),
                                 w_key.reshape(dim, -1), w_value.reshape(dim, -1)], axis=1)
        qkv, picked, kmax = qkv_part(tokens, w_cat, local_idx)
        halo_l = lax.ppermute(qkv[n_rows - WIN:, 256:], 'sp', to_right)
        halo_r = lax.ppermute(qkv[:WIN, 256:], 'sp', to_left)

        k_pos = first_row - WIN + jnp.arange(n_rows + 2 * WIN)
        k_off = jnp.any(glob_pos[:, None] == k_pos[None, :], axis=0) | (k_pos < 0) | (k_pos >= seq_len)
        bias = jnp.where(k_off, -jnp.inf, 0.0).astype(F32)[None, :]
        lane = jnp.arange(128) % 64
        extra = jnp.where(lane == 0, 1.0, jnp.where((lane == 1) & k_off[:, None], FLOOR, 0.0)).astype(BF16)

        half = n_glob // 2
        mine = lax.dynamic_slice_in_dim(picked, core * half, half)
        other = lax.ppermute(lax.dynamic_slice_in_dim(picked, (1 - core) * half, half), 'sp', core_swap)
        mine = mine + other
        got = lax.ppermute(mine, 'sp', chip_swap)
        win = window_part(qkv, halo_l, halo_r, extra, bias, kmax)
        got, win = lax.optimization_barrier((got, win))
        mine = mine + got
        other = lax.ppermute(mine, 'sp', core_swap)
        qkv_g = jnp.concatenate([jnp.where(core == 0, mine, other), jnp.where(core == 0, other, mine)], axis=0)

        part = global_queries_part(qkv_g, qkv, kmax)

        quarter = n_glob // 4
        got = lax.ppermute(lax.dynamic_slice_in_dim(part, (1 - core) * half, half, axis=1), 'sp', core_swap)
        joined = jnp.stack(combine(lax.dynamic_slice_in_dim(part, core * half, half, axis=1), got))
        got = lax.ppermute(lax.dynamic_slice_in_dim(joined, (1 - chip) * quarter, quarter, axis=1), 'sp', chip_swap)
        o = global_keys_part(qkv, qkv_g, kmax, win)
        got, o = lax.optimization_barrier((got, o))
        g_acc, _, g_l = combine(lax.dynamic_slice_in_dim(joined, chip * quarter, quarter, axis=1), got)
        mine = (g_acc / g_l).astype(BF16)
        other = lax.ppermute(mine, 'sp', chip_swap)
        mine = jnp.concatenate([jnp.where(chip == 0, mine, other), jnp.where(chip == 0, other, mine)], axis=0)
        other = lax.ppermute(mine, 'sp', core_swap)
        glob_out = jnp.concatenate([jnp.where(core == 0, mine, other), jnp.where(core == 0, other, mine)], axis=0)

        o = place_rows(o, glob_out, local_idx)
        return exchange_mlp(tokens, o, w_all, n_tp, d_o, d_f)

    row_spec = P(('dp', 'sp'), None)
    head_spec = P(None, 'tp', None)
    in_specs = (row_spec, P('dp'), head_spec, head_spec, head_spec, P('tp', None, None), P(None, 'tp'), P('tp', None))
    return jax.shard_map(device_layer, mesh=mesh, in_specs=in_specs, out_specs=row_spec, check_vma=False)
```

```python
import functools
import math

import jax
import jax.numpy as jnp
from jax import lax
from jax.experimental import pallas as pl
from jax.experimental.pallas import tpu as pltpu
from jax.sharding import PartitionSpec as P

WIN = 256
QB = 256
FLOOR = -3.0e38
F32 = jnp.float32
BF16 = jnp.bfloat16
NT = (((1,), (1,)), ((), ()))


def dot_nt(a, b):
    return lax.dot_general(a, b, NT, preferred_element_type=F32)


def dot_nn(a, b):
    return jnp.dot(a, b, preferred_element_type=F32)


def params(n_axes, vmem_mib=48):
    return pltpu.CompilerParams(
        dimension_semantics=("arbitrary",) * n_axes, vmem_limit_bytes=vmem_mib << 20)


def cost(flops, bytes_accessed, exps=0):
    return pl.CostEstimate(flops=int(flops), bytes_accessed=int(bytes_accessed), transcendentals=int(exps))


def head_sums(rows):
    n = rows.shape[1]
    r = lax.broadcasted_iota(jnp.int32, (n, n), 0) // 64
    c = lax.broadcasted_iota(jnp.int32, (n, n), 1) // 64
    pick = jnp.where(r == (c + 1 - 2 * (c % 2)), 1.0, 0.0).astype(BF16)
    wide = rows.astype(F32)
    return dot_nn((wide * wide).astype(BF16), pick)


def qkv_kernel(pos_ref, idx_ref, x_ref, w_ref, qkv_ref, pick_ref, kmax_ref, acc_ref):
    step = pl.program_id(0)
    n_blk = x_ref.shape[0]
    lo = step * n_blk
    gb = 128

    @pl.when(step == 0)
    def _():
        acc_ref[...] = jnp.zeros_like(acc_ref)
        kmax_ref[...] = jnp.zeros_like(kmax_ref)

    rows = dot_nn(x_ref[...], w_ref[...]).astype(BF16)
    qkv_ref[...] = rows
    kmax_ref[...] = jnp.maximum(kmax_ref[...], jnp.max(head_sums(rows[:, 256:512]), axis=0, keepdims=True))

    @pl.loop(0, idx_ref.shape[0] // gb)
    def _(b):
        g0 = pl.multiple_of(b * gb, gb)

        @pl.when((pos_ref[g0] < lo + n_blk) & (pos_ref[g0 + gb - 1] >= lo))
        def _():
            hit = idx_ref[pl.ds(g0, gb), :] == lo + lax.broadcasted_iota(jnp.int32, (gb, n_blk), 1)
            acc_ref[pl.ds(g0, gb), :] += dot_nn(hit.astype(F32).astype(BF16), qkv_ref[...])

    @pl.when(step == pl.num_programs(0) - 1)
    def _():
        pick_ref[...] = acc_ref[...].astype(pick_ref.dtype)


def qkv_part(tokens, w_cat, local_idx):
    n_rows, dim = tokens.shape
    n_glob = local_idx.shape[0]
    width = w_cat.shape[1]
    rb = 512
    return pl.pallas_call(
        qkv_kernel,
        grid_spec=pltpu.PrefetchScalarGridSpec(
            num_scalar_prefetch=1, grid=(n_rows // rb,),
            in_specs=[pl.BlockSpec((n_glob, 1), lambda i, p: (0, 0)), pl.BlockSpec((rb, dim), lambda i, p: (i, 0)),
                      pl.BlockSpec((dim, width), lambda i, p: (0, 0))],
            out_specs=[pl.BlockSpec((rb, width), lambda i, p: (i, 0)), pl.BlockSpec((n_glob, width), lambda i, p: (0, 0)),
                       pl.BlockSpec((1, 256), lambda i, p: (0, 0))],
            scratch_shapes=[pltpu.VMEM((n_glob, width), F32)]),
        out_shape=[jax.ShapeDtypeStruct((n_rows, width), BF16), jax.ShapeDtypeStruct((n_glob, width), BF16),
                   jax.ShapeDtypeStruct((1, 256), F32)],
        compiler_params=params(1), cost_estimate=cost(8e9, 24e6), name="qkv",
    )(local_idx, local_idx[:, None], tokens, w_cat)


def low_lanes(n):
    return lax.broadcasted_iota(jnp.int32, (n, 128), 1) < 64


def shifts(q, kmax):
    return (-1.02 * jnp.sqrt(head_sums(q) * kmax)).astype(BF16)


def own_half(pair, other, half):
    low = low_lanes(pair.shape[0])
    return jnp.where(low, pair, other) if half == 0 else jnp.where(low, other, pair)


def query_rows(q, neg, half):
    lane = lax.broadcasted_iota(jnp.int32, q.shape, 1) % 64
    return own_half(q, jnp.where(lane == 0, neg, jnp.ones_like(neg)), half)


def key_extra(n):
    return jnp.where(lax.broadcasted_iota(jnp.int32, (n, 128), 1) % 64 == 0, 1.0, 0.0).astype(BF16)


def stream(q_rows, tiles):
    acc = total = None
    for keys, values in tiles:
        e = jnp.exp(dot_nt(q_rows, keys))
        part = e[:, :128] + e[:, 128:]
        out = dot_nn(e.astype(BF16), values)
        acc = out if acc is None else acc + out
        total = part if total is None else total + part
    return acc, total


def row_sum(lanes):
    return jnp.sum(lanes, axis=1, keepdims=True)


def out_of_range(*totals):
    good = [jnp.logical_and(jnp.min(t) > 1e-25, jnp.max(t) < 1e30) for t in totals]
    return jnp.logical_not(functools.reduce(jnp.logical_and, good))


def exact_head(q, half, n_keys, key_rows, acc_ref, m_ref, l_ref):
    low = low_lanes(q.shape[0])
    q1 = jnp.where(low if half == 0 else jnp.logical_not(low), q, jnp.zeros_like(q))
    acc_ref[half] = jnp.zeros(q.shape, F32)
    l_ref[half] = jnp.zeros(q.shape, F32)
    m_ref[half] = jnp.full(q.shape, FLOOR, F32)

    @pl.loop(0, n_keys // 256)
    def _(c):
        keys, values, bias = key_rows(c)
        s = dot_nt(q1, keys)
        if bias is not None:
            s = s + bias
        m_old = m_ref[half]
        m_new = jnp.maximum(m_old, jnp.max(s, axis=1, keepdims=True))
        alpha = jnp.exp(m_old - m_new)
        e = jnp.exp(s - m_new[:, :1])
        l_ref[half] = alpha * l_ref[half] + row_sum(e)
        acc_ref[half] = alpha * acc_ref[half] + dot_nn(e.astype(BF16), values)
        m_ref[half] = m_new


def window_kernel(q_ref, kl_ref, kc_ref, kr_ref, vl_ref, vc_ref, vr_ref, hkl_ref, hkr_ref, hvl_ref, hvr_ref,
                  extra_ref, bias_ref, kmax_ref, acc_ref, m_ref, l_ref, tri_ref, key_ref, val_ref, ea_ref, em_ref, el_ref):
    i = pl.program_id(1)
    n = q_ref.shape[0]
    is_first = i == 0
    is_last = i == pl.num_programs(1) - 1

    @pl.when(i == 0)
    def _():
        r_i = lax.broadcasted_iota(jnp.int32, (QB, QB), 0)
        c_i = lax.broadcasted_iota(jnp.int32, (QB, QB), 1)
        tri_ref[:QB] = jnp.where(c_i <= r_i, 0.0, -jnp.inf)
        tri_ref[QB:2 * QB] = jnp.zeros((QB, QB), F32)
        tri_ref[2 * QB:] = jnp.where(c_i >= r_i, 0.0, -jnp.inf)

    key_ref[:QB] = jnp.where(is_first, hkl_ref[...], kl_ref[...])
    key_ref[QB:QB + n] = kc_ref[...]
    key_ref[QB + n:] = jnp.where(is_last, hkr_ref[...], kr_ref[...])
    val_ref[:QB] = jnp.where(is_first, hvl_ref[...], vl_ref[...])
    val_ref[QB:QB + n] = vc_ref[...]
    val_ref[QB + n:] = jnp.where(is_last, hvr_ref[...], vr_ref[...])

    q = q_ref[...]
    neg = shifts(q, kmax_ref[...])
    accs, sums = [], []
    for half in range(2):
        qx = query_rows(q, neg, half)
        acc, total = [None] * (n // QB), [None] * (n // QB)
        for t in range(n // QB + 2):
            b0, b1 = max(t - 2, 0), min(t + 1, n // QB)
            extra = extra_ref[pl.ds(pl.multiple_of(i * n + t * QB, QB), QB), :]
            s = dot_nt(qx[b0 * QB:b1 * QB], own_half(key_ref[t * QB:(t + 1) * QB], extra, half))
            e = jnp.exp(s + window_mask(tri_ref, t, b0, b1))
            part = e[:, :128] + e[:, 128:]
            out = dot_nn(e.astype(BF16), val_ref[t * QB:(t + 1) * QB])
            for b in range(b0, b1):
                r = slice((b - b0) * QB, (b - b0 + 1) * QB)
                acc[b] = out[r] if acc[b] is None else acc[b] + out[r]
                total[b] = part[r] if total[b] is None else total[b] + part[r]
        accs.append(jnp.concatenate(acc, axis=0))
        sums.append(row_sum(jnp.concatenate(total, axis=0)))
    low = low_lanes(n)
    acc_ref[...] = jnp.where(low, accs[0], accs[1])
    l_ref[...] = jnp.where(low, sums[0], sums[1])
    m_ref[...] = -pltpu.roll(neg.astype(F32), 64, 1)

    @pl.when(out_of_range(*sums))
    def _():
        @pl.loop(0, n // QB)
        def _(b):
            rows = pl.ds(pl.multiple_of(b * QB, QB), QB)

            def key_rows(c):
                at = pl.ds(pl.multiple_of((b + c) * QB, QB), QB)
                bias = bias_ref[:, pl.ds(pl.multiple_of(i * n + (b + c) * QB, QB), QB)]
                return key_ref[at], val_ref[at], bias + tri_ref[pl.ds(pl.multiple_of((2 - c) * QB, QB), QB)]

            for half in range(2):
                exact_head(q_ref[rows], half, 3 * QB, key_rows, ea_ref, em_ref, el_ref)
            low = low_lanes(QB)
            for out, src in ((acc_ref, ea_ref), (m_ref, em_ref), (l_ref, el_ref)):
                out[rows] = jnp.where(low, src[0], src[1])


def window_mask(tri_ref, t, b0, b1):
    return tri_ref[(b0 - t + 2) * QB:(b1 - t + 2) * QB]


def window_part(qkv, halo_l, halo_r, extra, bias, kmax):
    n_rows = qkv.shape[0]
    rb = min(1024, n_rows)
    per = rb // QB
    n_blk, n_small = n_rows // rb, n_rows // QB
    mid = lambda c: pl.BlockSpec((rb, 128), lambda p, i: (i, 2 * c + p))
    left = lambda c: pl.BlockSpec((QB, 128), lambda p, i: (jnp.maximum(i * per - 1, 0), 2 * c + p))
    right = lambda c: pl.BlockSpec((QB, 128), lambda p, i: (jnp.minimum(i * per + per, n_small - 1), 2 * c + p))
    halo = lambda c: pl.BlockSpec((QB, 128), lambda p, i: (0, 2 * c + p))
    whole = lambda a: pl.BlockSpec(a.shape, lambda p, i: (0,) * a.ndim)
    out = jax.ShapeDtypeStruct((n_rows, 256), F32)
    pair = pltpu.VMEM((2, QB, 128), F32)
    return pl.pallas_call(
        window_kernel, grid=(2, n_blk),
        in_specs=[mid(0), left(1), mid(1), right(1), left(2), mid(2), right(2), halo(0), halo(0), halo(1), halo(1),
                  whole(extra), whole(bias), pl.BlockSpec((1, 128), lambda p, i: (0, p))],
        out_specs=[pl.BlockSpec((rb, 128), lambda p, i: (i, p))] * 3,
        out_shape=[out, out, out],
        scratch_shapes=[pltpu.VMEM((3 * QB, QB), F32), pltpu.VMEM((rb + 2 * QB, 128), BF16),
                        pltpu.VMEM((rb + 2 * QB, 128), BF16), pair, pair, pair],
        compiler_params=params(2), cost_estimate=cost(30e9, 30e6, 12e6), name="window_part",
    )(qkv, qkv, qkv, qkv, qkv, qkv, qkv, halo_l, halo_r, halo_l, halo_r, extra, bias, kmax)


def global_queries_kernel(q_ref, k_ref, v_ref, kmax_ref, out_ref, acc_ref, m_ref, l_ref, *, kb):
    j = pl.program_id(2)
    n = q_ref.shape[0]
    low = low_lanes(n)

    @pl.when(j == 0)
    def _():
        acc_ref[...] = jnp.zeros_like(acc_ref)
        l_ref[...] = jnp.zeros_like(l_ref)

    extra = key_extra(256)
    q = q_ref[...]
    neg = shifts(q, kmax_ref[...])
    for half in range(2):
        rows = [pl.ds(pl.multiple_of(j * kb, kb) + t, 256) for t in range(0, kb, 256)]
        acc, total = stream(query_rows(q, neg, half), [(own_half(k_ref[r], extra, half), v_ref[r]) for r in rows])
        acc_ref[half] += acc
        l_ref[half] += total

    @pl.when(j == pl.num_programs(2) - 1)
    def _():
        sums = [row_sum(l_ref[half]) for half in range(2)]
        out_ref[0] = jnp.where(low, acc_ref[0], acc_ref[1])
        out_ref[1] = -pltpu.roll(neg.astype(F32), 64, 1)
        out_ref[2] = jnp.where(low, sums[0], sums[1])

        @pl.when(out_of_range(*sums))
        def _():
            def key_rows(c):
                at = pl.ds(pl.multiple_of(c * 256, 256), 256)
                return k_ref[at], v_ref[at], None

            for half in range(2):
                exact_head(q_ref[...], half, v_ref.shape[0], key_rows, acc_ref, m_ref, l_ref)
            for k, r in enumerate((acc_ref, m_ref, l_ref)):
                out_ref[k] = jnp.where(low, r[0], r[1])


def global_queries_part(qkv_g, qkv, kmax):
    n_glob = qkv_g.shape[0]
    n_rows = qkv.shape[0]
    rb = 512
    kb = min(1024, n_rows)
    return pl.pallas_call(
        functools.partial(global_queries_kernel, kb=kb), grid=(2, n_glob // rb, n_rows // kb),
        in_specs=[pl.BlockSpec((rb, 128), lambda p, i, j: (i, p)), pl.BlockSpec((n_rows, 128), lambda p, i, j: (0, 2 + p)),
                  pl.BlockSpec((n_rows, 128), lambda p, i, j: (0, 4 + p)), pl.BlockSpec((1, 128), lambda p, i, j: (0, p))],
        out_specs=pl.BlockSpec((3, rb, 128), lambda p, i, j: (0, i, p)),
        out_shape=jax.ShapeDtypeStruct((3, n_glob, 256), F32),
        scratch_shapes=[pltpu.VMEM((2, rb, 128), F32)] * 3,
        compiler_params=params(3), cost_estimate=cost(34e9, 20e6, 16e6), name="global_queries",
    )(qkv_g, qkv, qkv, kmax)


def exchange_mlp_kernel(x_hbm, w_hbm, qkv_hbm, qkvg_hbm, acc_hbm, m_hbm, l_hbm, glob_hbm, idx_ref, y_hbm,
                        x_ref, o_ref, wo_ref, w2_ref, w1_ref, q_ref, kg_ref, glob_ref, win_ref, load_sem, win_sem, y_sem,
                        up_send, up_recv, down_send, down_recv, *, n_tp, n_rep, d_o, d_f, rb):
    me = lax.axis_index('tp')
    n_blk = x_ref.shape[0] // rb
    width = n_tp * d_f

    barrier = pltpu.get_barrier_semaphore()

    @pl.when(me > 0)
    def _():
        pl.semaphore_signal(barrier, inc=1, device_id={'tp': me - 1}, device_id_type=pl.DeviceIdType.MESH)

    @pl.when(me < n_tp - 1)
    def _():
        pl.semaphore_signal(barrier, inc=1, device_id={'tp': me + 1}, device_id_type=pl.DeviceIdType.MESH)

    early = [pltpu.make_async_copy(qkv_hbm.at[:, pl.ds(0, 256)], q_ref, load_sem.at[0]),
             pltpu.make_async_copy(qkvg_hbm.at[:, pl.ds(256, 512)], kg_ref, load_sem.at[1]),
             pltpu.make_async_copy(glob_hbm, glob_ref, load_sem.at[2])]

    def rows_of(b):
        return pl.ds(pl.multiple_of(b * rb, rb), rb)

    def fetch(b):
        return [pltpu.make_async_copy(h.at[rows_of(b)], win_ref.at[b % 2, n], win_sem.at[b % 2, n])
                for n, h in enumerate((acc_hbm, m_hbm, l_hbm))]

    for c in early + fetch(0):
        c.start()
    copies = [pltpu.make_async_copy(x_hbm, x_ref, load_sem.at[3])]
    piece = wo_ref.shape[1] // n_rep
    for j in range(n_rep):
        for t in range(n_tp):
            lanes = pl.ds(j * piece, piece)
            for src, n, dst in ((0, d_o, wo_ref), (d_o, d_f, w2_ref), (d_o + d_f, d_f, w1_ref)):
                copies.append(pltpu.make_async_copy(w_hbm.at[j, t, pl.ds(src, n)], dst.at[pl.ds(t * n, n), lanes],
                                                    load_sem.at[3 + len(copies)]))
    for c in copies:
        c.start()

    ends = jnp.logical_or(me == 0, me == n_tp - 1)

    @pl.when(ends)
    def _():
        pl.semaphore_wait(barrier, 1)

    @pl.when(jnp.logical_not(ends))
    def _():
        pl.semaphore_wait(barrier, 2)

    for c in early:
        c.wait()

    def attend(b):
        @pl.when(b + 1 < n_blk)
        def _():
            for c in fetch(b + 1):
                c.start()

        for c in fetch(b):
            c.wait()

        @pl.loop(0, rb // QB)
        def _(r):
            at = pl.ds(pl.multiple_of(r * QB, QB), QB)
            rows = pl.ds(pl.multiple_of(b * rb + r * QB, QB), QB)
            low = low_lanes(QB)
            parts = []
            for pr in range(2):
                cols = slice(pr * 128, pr * 128 + 128)
                q = q_ref[rows, cols]
                zero = jnp.zeros_like(q)
                q2 = jnp.concatenate([jnp.where(low, q, zero), jnp.where(low, zero, q)], axis=0)
                sc = dot_nt(q2, kg_ref[:, cols])
                top = jnp.max(sc, axis=1, keepdims=True)
                e = jnp.exp(sc - top)
                total = row_sum(e)
                acc = dot_nn(e.astype(BF16), kg_ref[:, 256 + pr * 128:256 + pr * 128 + 128])
                acc, m, total = (jnp.where(low, v[:QB], v[QB:]) for v in (acc, top, total))
                acc_w, m_w, l_w = (win_ref[b % 2, n, at, cols] for n in range(3))
                m_all = jnp.maximum(m, m_w)
                f, f_w = jnp.exp(m - m_all), jnp.exp(m_w - m_all)
                parts.append((acc * f + acc_w * f_w) / (total * f + l_w * f_w))
            row = b * rb + r * QB + lax.broadcasted_iota(jnp.int32, (QB, 1), 0)
            hit = jnp.where(idx_ref[...] == row, 1.0, 0.0)
            placed = dot_nn(hit.astype(BF16), glob_ref[...])
            mine = row_sum(hit) > 0.5
            o_ref[me, rows] = jnp.where(mine, placed, jnp.concatenate(parts, axis=1)).astype(BF16)

    def up(d, b):
        at = o_ref.at[me - d, rows_of(b)]
        return pltpu.make_async_remote_copy(at, at, up_send.at[d, b], up_recv.at[d, b], device_id={'tp': me + 1},
                                            device_id_type=pl.DeviceIdType.MESH)

    def down(d, b):
        at = o_ref.at[me + d, rows_of(b)]
        return pltpu.make_async_remote_copy(at, at, down_send.at[d, b], down_recv.at[d, b], device_id={'tp': me - 1},
                                            device_id_type=pl.DeviceIdType.MESH)

    def landed(recv, d, shard, b):
        at = o_ref.at[shard, rows_of(b)]
        pltpu.make_async_remote_copy(at, at, up_send.at[0, b], recv.at[d - 1, b], device_id={'tp': me},
                                     device_id_type=pl.DeviceIdType.MESH).wait_recv()

    def send_own(b):
        @pl.when(me < n_tp - 1)
        def _():
            up(0, b).start()

        @pl.when(me > 0)
        def _():
            down(0, b).start()

    attend(0)
    attend(1)
    send_own(0)

    def step(s, carry):
        @pl.when(s + 1 < n_blk)
        def _():
            send_own(s + 1)

        for d in range(1, n_tp):
            b = s - (d - 1)

            @pl.when((b >= 0) & (b < n_blk) & (me >= d))
            def _():
                landed(up_recv, d, me - d, b)
                if d < n_tp - 1:
                    @pl.when(me < n_tp - 1)
                    def _():
                        up(d, b).start()

            @pl.when((b >= 0) & (b < n_blk) & (me + d <= n_tp - 1))
            def _():
                landed(down_recv, d, me + d, b)
                if d < n_tp - 1:
                    @pl.when(me > 0)
                    def _():
                        down(d, b).start()

        @pl.when(s + 2 < n_blk)
        def _():
            attend(s + 2)

        @pl.when(s == n_tp - 2)
        def _():
            for c in copies:
                c.wait()

        @pl.when(s >= n_tp - 2)
        def _():
            b = s - (n_tp - 2)
            rows = rows_of(b)
            mixed = dot_nn(o_ref[0, rows], wo_ref[:d_o, :])
            for t in range(1, n_tp):
                mixed += dot_nn(o_ref[t, rows], wo_ref[t * d_o:(t + 1) * d_o, :])
            h = (x_ref[rows].astype(F32) + mixed).astype(BF16)
            acc = h.astype(F32)
            for f0 in range(0, width, 512):
                f1 = min(f0 + 512, width)
                z = dot_nt(h, w1_ref[f0:f1, :])
                u = 0.5 * z * (1.0 + jnp.tanh(math.sqrt(2.0 / math.pi) * (z + 0.044715 * (z * z * z))))
                acc += dot_nn(u.astype(BF16), w2_ref[f0:f1, :])
            x_ref[rows] = acc.astype(BF16)
            pltpu.make_async_copy(x_ref.at[rows], y_hbm.at[rows], y_sem.at[b]).start()

        return carry

    lax.fori_loop(0, n_blk + n_tp - 2, step, 0)

    def finish(b, carry):
        rows = rows_of(b)
        pltpu.make_async_copy(x_ref.at[rows], y_hbm.at[rows], y_sem.at[b]).wait()
        for d in range(n_tp - 1):
            @pl.when((me < n_tp - 1) & (me >= d))
            def _():
                up(d, b).wait_send()

            @pl.when((me > 0) & (me + d <= n_tp - 1))
            def _():
                down(d, b).wait_send()

        return carry

    lax.fori_loop(0, n_blk, finish, 0)


def exchange_mlp(tokens, w_all, qkv, qkv_g, win, glob_out, local_idx, n_tp, d_o, d_f):
    n_rows, dim = tokens.shape
    n_glob = local_idx.shape[0]
    n_rep = w_all.shape[0]
    rb = min(512, n_rows // 2)
    n_blk = n_rows // rb
    anywhere = pl.BlockSpec(memory_space=pl.ANY)
    dma = pltpu.SemaphoreType.DMA
    return pl.pallas_call(
        functools.partial(exchange_mlp_kernel, n_tp=n_tp, n_rep=n_rep, d_o=d_o, d_f=d_f, rb=rb),
        in_specs=[anywhere] * 8 + [pl.BlockSpec(memory_space=pltpu.VMEM)], out_specs=anywhere,
        out_shape=jax.ShapeDtypeStruct(tokens.shape, BF16),
        scratch_shapes=[pltpu.VMEM((n_rows, dim), BF16), pltpu.VMEM((n_tp, n_rows, d_o), BF16),
                        pltpu.VMEM((n_tp * d_o, dim), BF16), pltpu.VMEM((n_tp * d_f, dim), BF16),
                        pltpu.VMEM((n_tp * d_f, dim), BF16), pltpu.VMEM((n_rows, d_o), BF16),
                        pltpu.VMEM((n_glob, 2 * d_o), BF16), pltpu.VMEM((n_glob, d_o), BF16),
                        pltpu.VMEM((2, 3, rb, d_o), F32), dma((4 + 3 * n_rep * n_tp,)), dma((2, 3)), dma((n_blk,)),
                        dma((n_tp - 1, n_blk)), dma((n_tp - 1, n_blk)), dma((n_tp - 1, n_blk)), dma((n_tp - 1, n_blk))],
        compiler_params=pltpu.CompilerParams(collective_id=1, has_side_effects=True, vmem_limit_bytes=60 << 20),
        cost_estimate=cost(2 * n_rows * dim * (dim + 2 * n_tp * d_f), 40e6), name="exchange_mlp",
    )(tokens, w_all, qkv, qkv_g, *win, glob_out, local_idx[None, :])


def copy_kernel(a_ref, b_ref):
    b_ref[...] = a_ref[...]


def streamed(a):
    rb = a.shape[0] // 4
    spec = pl.BlockSpec((rb, a.shape[1]), lambda i: (i, 0))
    return pl.pallas_call(copy_kernel, grid=(4,), in_specs=[spec], out_specs=spec,
                          out_shape=jax.ShapeDtypeStruct(a.shape, a.dtype),
                          compiler_params=params(1), name="result")(a)


def combine(a, b):
    m = jnp.maximum(a[1], b[1])
    e_a, e_b = jnp.exp(a[1] - m), jnp.exp(b[1] - m)
    return a[0] * e_a + b[0] * e_b, m, a[2] * e_a + b[2] * e_b


def solution(mesh):
    n_seq = mesh.shape['sp']
    to_right = [(i, i + 1) for i in range(n_seq - 1)]
    to_left = [(i + 1, i) for i in range(n_seq - 1)]
    core_swap = [(i, i ^ 1) for i in range(n_seq)]
    chip_swap = [(i, i ^ 2) for i in range(n_seq)]

    def device_layer(tokens, glob_pos, w_query, w_key, w_value, w_out, w_up, w_down):
        n_rows, dim = tokens.shape
        n_glob = glob_pos.shape[0]
        sp = lax.axis_index('sp')
        core, chip = sp % 2, sp // 2
        first_row = sp * n_rows
        seq_len = n_rows * n_seq
        local_idx = glob_pos - first_row

        d_o, d_f = w_out.shape[0] * w_out.shape[1], w_down.shape[0]
        shard = jnp.concatenate([w_out.reshape(d_o, dim), w_down, w_up.T], axis=0)
        rep = lax.axis_index('dp') * n_seq + sp
        n_tp, n_rep = mesh.shape['tp'], mesh.shape['dp'] * n_seq
        piece = dim // n_rep
        w_slice = lax.dynamic_slice_in_dim(shard, rep * piece, piece, axis=1)
        w_all = lax.all_gather(w_slice, ('dp', 'sp', 'tp'))
        w_all = w_all.reshape(n_rep, n_tp, d_o + 2 * d_f, piece)

        w_cat = jnp.concatenate([w_query.reshape(dim, -1) * jnp.asarray(0.125, BF16),
                                 w_key.reshape(dim, -1), w_value.reshape(dim, -1)], axis=1)
        qkv, picked, kmax = qkv_part(tokens, w_cat, local_idx)
        halo_l = lax.ppermute(qkv[n_rows - WIN:, 256:], 'sp', to_right)
        halo_r = lax.ppermute(qkv[:WIN, 256:], 'sp', to_left)

        k_pos = first_row - WIN + jnp.arange(n_rows + 2 * WIN)
        k_off = jnp.any(glob_pos[:, None] == k_pos[None, :], axis=0) | (k_pos < 0) | (k_pos >= seq_len)
        bias = jnp.where(k_off, -jnp.inf, 0.0).astype(F32)[None, :]
        lane = jnp.arange(128) % 64
        extra = jnp.where(lane == 0, 1.0, jnp.where((lane == 1) & k_off[:, None], FLOOR, 0.0)).astype(BF16)

        half = n_glob // 2
        mine = lax.dynamic_slice_in_dim(picked, core * half, half)
        other = lax.ppermute(lax.dynamic_slice_in_dim(picked, (1 - core) * half, half), 'sp', core_swap)
        mine = mine + other
        got = lax.ppermute(mine, 'sp', chip_swap)
        mine = mine + got
        other = lax.ppermute(mine, 'sp', core_swap)
        qkv_g = jnp.concatenate([jnp.where(core == 0, mine, other), jnp.where(core == 0, other, mine)], axis=0)

        part = global_queries_part(qkv_g, qkv, kmax)
        part, kmax = lax.optimization_barrier((part, kmax))

        quarter = n_glob // 4
        got = lax.ppermute(lax.dynamic_slice_in_dim(part, (1 - core) * half, half, axis=1), 'sp', core_swap)
        joined = jnp.stack(combine(lax.dynamic_slice_in_dim(part, core * half, half, axis=1), got))
        got = lax.ppermute(lax.dynamic_slice_in_dim(joined, (1 - chip) * quarter, quarter, axis=1), 'sp', chip_swap)
        win = window_part(qkv, halo_l, halo_r, extra, bias, kmax)
        got, win = lax.optimization_barrier((got, win))
        g_acc, _, g_l = combine(lax.dynamic_slice_in_dim(joined, chip * quarter, quarter, axis=1), got)
        mine = (g_acc / g_l).astype(BF16)
        other = lax.ppermute(mine, 'sp', chip_swap)
        mine = jnp.concatenate([jnp.where(chip == 0, mine, other), jnp.where(chip == 0, other, mine)], axis=0)
        other = lax.ppermute(mine, 'sp', core_swap)
        glob_out = jnp.concatenate([jnp.where(core == 0, mine, other), jnp.where(core == 0, other, mine)], axis=0)

        return streamed(exchange_mlp(tokens, w_all, qkv, qkv_g, win, glob_out, local_idx, n_tp, d_o, d_f))

    row_spec = P(('dp', 'sp'), None)
    head_spec = P(None, 'tp', None)
    in_specs = (row_spec, P('dp'), head_spec, head_spec, head_spec, P('tp', None, None), P(None, 'tp'), P('tp', None))
    return jax.shard_map(device_layer, mesh=mesh, in_specs=in_specs, out_specs=row_spec, check_vma=False)
```

```python
import functools
import math

import jax
import jax.numpy as jnp
from jax import lax
from jax.experimental import pallas as pl
from jax.experimental.pallas import tpu as pltpu
from jax.sharding import PartitionSpec as P

WIN = 256
QB = 256
FLOOR = -3.0e38
F32 = jnp.float32
BF16 = jnp.bfloat16
LANES = 128
HEAD = 64
NT = (((1,), (1,)), ((), ()))


def dot_nt(a, b):
    return lax.dot_general(a, b, NT, preferred_element_type=F32)


def dot_nn(a, b):
    return jnp.dot(a, b, preferred_element_type=F32)


def params(n_axes, vmem_mib=60):
    return pltpu.CompilerParams(
        dimension_semantics=("arbitrary",) * n_axes, vmem_limit_bytes=vmem_mib << 20)


def cost(flops, bytes_accessed, exps=0):
    return pl.CostEstimate(flops=int(flops), bytes_accessed=int(bytes_accessed), transcendentals=int(exps))


def head_sums(rows):
    n = rows.shape[1]
    r = lax.broadcasted_iota(jnp.int32, (n, n), 0) // HEAD
    c = lax.broadcasted_iota(jnp.int32, (n, n), 1) // HEAD
    pick = jnp.where(r == (c + 1 - 2 * (c % 2)), 1.0, 0.0).astype(BF16)
    wide = rows.astype(F32)
    return dot_nn((wide * wide).astype(BF16), pick)


def qkv_kernel(pos_ref, idx_ref, x_ref, w_ref, qkv_ref, pick_ref, kmax_ref, acc_ref):
    step = pl.program_id(0)
    n_blk = x_ref.shape[0]
    lo = step * n_blk
    gb = LANES

    @pl.when(step == 0)
    def _():
        acc_ref[...] = jnp.zeros_like(acc_ref)
        kmax_ref[...] = jnp.zeros_like(kmax_ref)

    rows = dot_nn(x_ref[...], w_ref[...]).astype(BF16)
    qkv_ref[...] = rows
    kmax_ref[...] = jnp.maximum(kmax_ref[...], jnp.max(head_sums(rows[:, QB:512]), axis=0, keepdims=True))

    @pl.loop(0, idx_ref.shape[0] // gb)
    def _(b):
        g0 = pl.multiple_of(b * gb, gb)

        @pl.when((pos_ref[g0] < lo + n_blk) & (pos_ref[g0 + gb - 1] >= lo))
        def _():
            hit = idx_ref[pl.ds(g0, gb), :] == lo + lax.broadcasted_iota(jnp.int32, (gb, n_blk), 1)
            acc_ref[pl.ds(g0, gb), :] += dot_nn(hit.astype(F32).astype(BF16), qkv_ref[...])

    @pl.when(step == pl.num_programs(0) - 1)
    def _():
        pick_ref[...] = acc_ref[...].astype(pick_ref.dtype)


def qkv_part(tokens, w_cat, local_idx):
    n_rows, dim = tokens.shape
    n_glob = local_idx.shape[0]
    width = w_cat.shape[1]
    rb = 512
    return pl.pallas_call(
        qkv_kernel,
        grid_spec=pltpu.PrefetchScalarGridSpec(
            num_scalar_prefetch=1, grid=(n_rows // rb,),
            in_specs=[pl.BlockSpec((n_glob, 1), lambda i, p: (0, 0)), pl.BlockSpec((rb, dim), lambda i, p: (i, 0)),
                      pl.BlockSpec((dim, width), lambda i, p: (0, 0))],
            out_specs=[pl.BlockSpec((rb, width), lambda i, p: (i, 0)), pl.BlockSpec((n_glob, width), lambda i, p: (0, 0)),
                       pl.BlockSpec((1, QB), lambda i, p: (0, 0))],
            scratch_shapes=[pltpu.VMEM((n_glob, width), F32)]),
        out_shape=[jax.ShapeDtypeStruct((n_rows, width), BF16), jax.ShapeDtypeStruct((n_glob, width), BF16),
                   jax.ShapeDtypeStruct((1, QB), F32)],
        compiler_params=params(1), cost_estimate=cost(8e9, 24e6), name="qkv",
    )(local_idx, local_idx[:, None], tokens, w_cat)


def low_lanes(n):
    return lax.broadcasted_iota(jnp.int32, (n, LANES), 1) < HEAD


def shifts(q, kmax):
    return (-1.02 * jnp.sqrt(head_sums(q) * kmax)).astype(BF16)


def own_half(pair, other, half):
    low = low_lanes(pair.shape[0])
    return jnp.where(low, pair, other) if half == 0 else jnp.where(low, other, pair)


def query_rows(q, neg, half):
    lane = lax.broadcasted_iota(jnp.int32, q.shape, 1) % HEAD
    return own_half(q, jnp.where(lane == 0, neg, jnp.ones_like(neg)), half)


def key_extra(n):
    return jnp.where(lax.broadcasted_iota(jnp.int32, (n, LANES), 1) % HEAD == 0, 1.0, 0.0).astype(BF16)


def stream(q_rows, tiles):
    acc = total = None
    for keys, values in tiles:
        e = jnp.exp(dot_nt(q_rows, keys))
        part = e[:, :LANES] + e[:, LANES:]
        out = dot_nn(e.astype(BF16), values)
        acc = out if acc is None else acc + out
        total = part if total is None else total + part
    return acc, total


def row_sum(lanes):
    return jnp.sum(lanes, axis=1, keepdims=True)


def out_of_range(*totals):
    good = [jnp.logical_and(jnp.min(t) > 1e-25, jnp.max(t) < 1e30) for t in totals]
    return jnp.logical_not(functools.reduce(jnp.logical_and, good))


def exact_heads(q, n_keys, key_rows, acc_ref, m_ref, l_ref):
    @pl.loop(0, 2)
    def _(half):
        exact_head(q, half, n_keys, key_rows, acc_ref, m_ref, l_ref)


def exact_head(q, half, n_keys, key_rows, acc_ref, m_ref, l_ref):
    mine = lax.broadcasted_iota(jnp.int32, q.shape, 1) // HEAD == half
    q1 = jnp.where(mine, q, jnp.zeros_like(q))
    acc_ref[half] = jnp.zeros(q.shape, F32)
    l_ref[half] = jnp.zeros(q.shape, F32)
    m_ref[half] = jnp.full(q.shape, FLOOR, F32)

    @pl.loop(0, n_keys // QB)
    def _(c):
        keys, values, bias = key_rows(c)
        s = dot_nt(q1, keys)
        if bias is not None:
            s = s + bias
        m_old = m_ref[half]
        m_new = jnp.maximum(m_old, jnp.max(s, axis=1, keepdims=True))
        alpha = jnp.exp(m_old - m_new)
        e = jnp.exp(s - m_new[:, :1])
        l_ref[half] = alpha * l_ref[half] + row_sum(e)
        acc_ref[half] = alpha * acc_ref[half] + dot_nn(e.astype(BF16), values)
        m_ref[half] = m_new


def window_kernel(q_ref, kl_ref, kc_ref, kr_ref, vl_ref, vc_ref, vr_ref, hkl_ref, hkr_ref, hvl_ref, hvr_ref,
                  extra_ref, bias_ref, kmax_ref, *refs, first, n_blk):
    acc_ref, m_ref, l_ref, tri_ref, key_ref, val_ref, ea_ref, em_ref, el_ref = refs[-9:]
    i = first + pl.program_id(1)
    n = q_ref.shape[0]
    is_first = i == 0
    is_last = i == n_blk - 1

    @pl.when(pl.program_id(1) == 0)
    def _():
        r_i = lax.broadcasted_iota(jnp.int32, (QB, QB), 0)
        c_i = lax.broadcasted_iota(jnp.int32, (QB, QB), 1)
        tri_ref[:QB] = jnp.where(c_i <= r_i, 0.0, -jnp.inf)
        tri_ref[QB:2 * QB] = jnp.zeros((QB, QB), F32)
        tri_ref[2 * QB:] = jnp.where(c_i >= r_i, 0.0, -jnp.inf)

    key_ref[:QB] = jnp.where(is_first, hkl_ref[...], kl_ref[...])
    key_ref[QB:QB + n] = kc_ref[...]
    key_ref[QB + n:] = jnp.where(is_last, hkr_ref[...], kr_ref[...])
    val_ref[:QB] = jnp.where(is_first, hvl_ref[...], vl_ref[...])
    val_ref[QB:QB + n] = vc_ref[...]
    val_ref[QB + n:] = jnp.where(is_last, hvr_ref[...], vr_ref[...])

    q = q_ref[...]
    neg = shifts(q, kmax_ref[...])
    accs, sums = [], []
    for half in range(2):
        qx = query_rows(q, neg, half)
        acc, total = [None] * (n // QB), [None] * (n // QB)
        for t in range(n // QB + 2):
            b0, b1 = max(t - 2, 0), min(t + 1, n // QB)
            extra = extra_ref[pl.ds(pl.multiple_of(i * n + t * QB, QB), QB), :]
            s = dot_nt(qx[b0 * QB:b1 * QB], own_half(key_ref[t * QB:(t + 1) * QB], extra, half))
            e = jnp.exp(s + window_mask(tri_ref, t, b0, b1))
            part = e[:, :LANES] + e[:, LANES:]
            out = dot_nn(e.astype(BF16), val_ref[t * QB:(t + 1) * QB])
            for b in range(b0, b1):
                r = slice((b - b0) * QB, (b - b0 + 1) * QB)
                acc[b] = out[r] if acc[b] is None else acc[b] + out[r]
                total[b] = part[r] if total[b] is None else total[b] + part[r]
        accs.append(jnp.concatenate(acc, axis=0))
        sums.append(row_sum(jnp.concatenate(total, axis=0)))
    low = low_lanes(n)
    acc_ref[...] = jnp.where(low, accs[0], accs[1])
    l_ref[...] = jnp.where(low, sums[0], sums[1])
    m_ref[...] = -pltpu.roll(neg.astype(F32), HEAD, 1)

    @pl.when(out_of_range(*sums))
    def _():
        @pl.loop(0, n // QB)
        def _(b):
            rows = pl.ds(pl.multiple_of(b * QB, QB), QB)

            def key_rows(c):
                at = pl.ds(pl.multiple_of((b + c) * QB, QB), QB)
                bias = bias_ref[:, pl.ds(pl.multiple_of(i * n + (b + c) * QB, QB), QB)]
                return key_ref[at], val_ref[at], bias + tri_ref[pl.ds(pl.multiple_of((2 - c) * QB, QB), QB)]

            exact_heads(q_ref[rows], 3 * QB, key_rows, ea_ref, em_ref, el_ref)
            low = low_lanes(QB)
            for out, src in ((acc_ref, ea_ref), (m_ref, em_ref), (l_ref, el_ref)):
                out[rows] = jnp.where(low, src[0], src[1])


def window_mask(tri_ref, t, b0, b1):
    return tri_ref[(b0 - t + 2) * QB:(b1 - t + 2) * QB]


def window_part(qkv, halo_l, halo_r, extra, bias, kmax, first, last, win=()):
    n_rows = qkv.shape[0]
    rb = n_rows // 4
    per = rb // QB
    n_blk, n_small = n_rows // rb, n_rows // QB
    mid = lambda c: pl.BlockSpec((rb, LANES), lambda p, i: (first + i, 2 * c + p))
    left = lambda c: pl.BlockSpec((QB, LANES), lambda p, i: (jnp.maximum((first + i) * per - 1, 0), 2 * c + p))
    right = lambda c: pl.BlockSpec((QB, LANES), lambda p, i: (jnp.minimum((first + i) * per + per, n_small - 1), 2 * c + p))
    halo = lambda c: pl.BlockSpec((QB, LANES), lambda p, i: (0, 2 * c + p))
    whole = lambda a: pl.BlockSpec(a.shape, lambda p, i: (0,) * a.ndim)
    out = jax.ShapeDtypeStruct((n_rows, QB), F32)
    pair = pltpu.VMEM((2, QB, LANES), F32)
    part = (last - first) / n_blk
    return pl.pallas_call(
        functools.partial(window_kernel, first=first, n_blk=n_blk), grid=(2, last - first),
        in_specs=[mid(0), left(1), mid(1), right(1), left(2), mid(2), right(2), halo(0), halo(0), halo(1), halo(1),
                  whole(extra), whole(bias), pl.BlockSpec((1, LANES), lambda p, i: (0, p))]
        + [pl.BlockSpec(memory_space=pl.ANY)] * len(win),
        out_specs=[pl.BlockSpec((rb, LANES), lambda p, i: (first + i, p))] * 3,
        out_shape=[out, out, out], input_output_aliases={14 + n: n for n in range(len(win))},
        scratch_shapes=[pltpu.VMEM((3 * QB, QB), F32), pltpu.VMEM((rb + 2 * QB, LANES), BF16),
                        pltpu.VMEM((rb + 2 * QB, LANES), BF16), pair, pair, pair],
        compiler_params=params(2), cost_estimate=cost(30e9 * part, 30e6 * part, 12e6 * part), name="window_part",
    )(qkv, qkv, qkv, qkv, qkv, qkv, qkv, halo_l, halo_r, halo_l, halo_r, extra, bias, kmax, *win)


def global_keys_kernel(q_ref, kg_ref, vg_ref, kmax_ref, acc_ref, m_ref, l_ref, out_ref,
                       k_ref, ea_ref, em_ref, el_ref):
    n = q_ref.shape[0]
    i = pl.program_id(1)

    @pl.when(i == 0)
    def _():
        extra = key_extra(kg_ref.shape[0])
        for half in range(2):
            k_ref[half] = own_half(kg_ref[...], extra, half)

    def finish(acc, m, total):
        m_all = jnp.maximum(m, m_ref[...])
        a, b = jnp.exp(m - m_all), jnp.exp(m_ref[...] - m_all)
        out_ref[...] = ((acc * a + acc_ref[...] * b) / (total * a + l_ref[...] * b)).astype(out_ref.dtype)

    q = q_ref[...]
    neg = shifts(q, kmax_ref[...])
    low = low_lanes(n)
    res = [stream(query_rows(q, neg, half), [(k_ref[half, t:t + QB], vg_ref[t:t + QB]) for t in range(0, vg_ref.shape[0], QB)])
           for half in range(2)]
    sums = [row_sum(r[1]) for r in res]
    finish(jnp.where(low, res[0][0], res[1][0]), -pltpu.roll(neg.astype(F32), HEAD, 1), jnp.where(low, sums[0], sums[1]))

    @pl.when(out_of_range(*sums))
    def _():
        def key_rows(c):
            at = pl.ds(pl.multiple_of(c * QB, QB), QB)
            return kg_ref[at], vg_ref[at], None

        exact_heads(q_ref[...], vg_ref.shape[0], key_rows, ea_ref, em_ref, el_ref)
        finish(*(jnp.where(low, r[0], r[1]) for r in (ea_ref, em_ref, el_ref)))


def global_keys_part(qkv, qkv_g, kmax, win, n_rows):
    n_glob = qkv_g.shape[0]
    rb = min(512, n_rows)
    row = pl.BlockSpec((rb, LANES), lambda p, i: (i, p))
    pair = pltpu.VMEM((2, rb, LANES), F32)
    return pl.pallas_call(
        global_keys_kernel, grid=(2, n_rows // rb),
        in_specs=[row, pl.BlockSpec((n_glob, LANES), lambda p, i: (0, 2 + p)), pl.BlockSpec((n_glob, LANES), lambda p, i: (0, 4 + p)),
                  pl.BlockSpec((1, LANES), lambda p, i: (0, p)), row, row, row],
        out_specs=row, out_shape=jax.ShapeDtypeStruct((n_rows, QB), BF16),
        scratch_shapes=[pltpu.VMEM((2, n_glob, LANES), BF16), pair, pair, pair],
        compiler_params=params(2), cost_estimate=cost(10e9, 8e6, 4e6), name="global_keys",
    )(qkv, qkv_g, qkv_g, kmax, *win)


def global_queries_kernel(q_ref, k_ref, v_ref, kmax_ref, out_ref, acc_ref, m_ref, l_ref, *, kb):
    j = pl.program_id(2)
    n = q_ref.shape[0]
    low = low_lanes(n)

    @pl.when(j == 0)
    def _():
        acc_ref[...] = jnp.zeros_like(acc_ref)
        l_ref[...] = jnp.zeros_like(l_ref)

    extra = key_extra(QB)
    q = q_ref[...]
    neg = shifts(q, kmax_ref[...])
    for half in range(2):
        rows = [pl.ds(pl.multiple_of(j * kb, kb) + t, QB) for t in range(0, kb, QB)]
        acc, total = stream(query_rows(q, neg, half), [(own_half(k_ref[r], extra, half), v_ref[r]) for r in rows])
        acc_ref[half] += acc
        l_ref[half] += total

    @pl.when(j == pl.num_programs(2) - 1)
    def _():
        sums = [row_sum(l_ref[half]) for half in range(2)]
        out_ref[0] = jnp.where(low, acc_ref[0], acc_ref[1])
        out_ref[1] = -pltpu.roll(neg.astype(F32), HEAD, 1)
        out_ref[2] = jnp.where(low, sums[0], sums[1])

        @pl.when(out_of_range(*sums))
        def _():
            def key_rows(c):
                at = pl.ds(pl.multiple_of(c * QB, QB), QB)
                return k_ref[at], v_ref[at], None

            exact_heads(q_ref[...], v_ref.shape[0], key_rows, acc_ref, m_ref, l_ref)
            for k, r in enumerate((acc_ref, m_ref, l_ref)):
                out_ref[k] = jnp.where(low, r[0], r[1])


def global_queries_part(qkv_g, qkv, kmax):
    n_glob = qkv_g.shape[0]
    n_rows = qkv.shape[0]
    rb = 512
    kb = min(1024, n_rows)
    return pl.pallas_call(
        functools.partial(global_queries_kernel, kb=kb), grid=(2, n_glob // rb, n_rows // kb),
        in_specs=[pl.BlockSpec((rb, LANES), lambda p, i, j: (i, p)), pl.BlockSpec((n_rows, LANES), lambda p, i, j: (0, 2 + p)),
                  pl.BlockSpec((n_rows, LANES), lambda p, i, j: (0, 4 + p)), pl.BlockSpec((1, LANES), lambda p, i, j: (0, p))],
        out_specs=pl.BlockSpec((3, rb, LANES), lambda p, i, j: (0, i, p)),
        out_shape=jax.ShapeDtypeStruct((3, n_glob, QB), F32),
        scratch_shapes=[pltpu.VMEM((2, rb, LANES), F32)] * 3,
        compiler_params=params(3), cost_estimate=cost(34e9, 20e6, 16e6), name="global_queries",
    )(qkv_g, qkv, qkv, kmax)


def exchange_mlp_kernel(x_hbm, w_hbm, qkv_hbm, qkvg_hbm, acc_hbm, m_hbm, l_hbm, glob_hbm, idx_ref, pre_ref, y_hbm,
                        x_ref, o_ref, wo_ref, w2_ref, w1_ref, q_ref, kg_ref, glob_ref, win_ref, load_sem, win_sem, y_sem,
                        up_send, up_recv, down_send, down_recv, *, n_tp, n_rep, d_o, d_f, rb):
    me = lax.axis_index('tp')
    n_blk = x_ref.shape[0] // rb
    width = n_tp * d_f
    qb = min(QB, rb)

    barrier = pltpu.get_barrier_semaphore()

    @pl.when(me > 0)
    def _():
        pl.semaphore_signal(barrier, inc=1, device_id={'tp': me - 1}, device_id_type=pl.DeviceIdType.MESH)

    @pl.when(me < n_tp - 1)
    def _():
        pl.semaphore_signal(barrier, inc=1, device_id={'tp': me + 1}, device_id_type=pl.DeviceIdType.MESH)

    early = [pltpu.make_async_copy(qkv_hbm.at[:, pl.ds(0, QB)], q_ref, load_sem.at[0]),
             pltpu.make_async_copy(qkvg_hbm.at[:, pl.ds(QB, 512)], kg_ref, load_sem.at[1]),
             pltpu.make_async_copy(glob_hbm, glob_ref, load_sem.at[2])]

    def rows_of(b):
        return pl.ds(pl.multiple_of(b * rb, rb), rb)

    def fetch(b):
        return [pltpu.make_async_copy(h.at[rows_of(b)], win_ref.at[b % 2, n], win_sem.at[b % 2, n])
                for n, h in enumerate((acc_hbm, m_hbm, l_hbm))]

    for c in early + fetch(2):
        c.start()
    copies = [pltpu.make_async_copy(x_hbm, x_ref, load_sem.at[3])]
    piece = wo_ref.shape[1] // n_rep
    for j in range(n_rep):
        for t in range(n_tp):
            lanes = pl.ds(j * piece, piece)
            for src, n, dst in ((0, d_o, wo_ref), (d_o, d_f, w2_ref), (d_o + d_f, d_f, w1_ref)):
                copies.append(pltpu.make_async_copy(w_hbm.at[j, t, pl.ds(src, n)], dst.at[pl.ds(t * n, n), lanes],
                                                    load_sem.at[3 + len(copies)]))
    for c in copies:
        c.start()

    ends = jnp.logical_or(me == 0, me == n_tp - 1)

    @pl.when(ends)
    def _():
        pl.semaphore_wait(barrier, 1)

    @pl.when(jnp.logical_not(ends))
    def _():
        pl.semaphore_wait(barrier, 2)

    for c in early:
        c.wait()

    def attend(b):
        @pl.when(b + 1 < n_blk)
        def _():
            for c in fetch(b + 1):
                c.start()

        for c in fetch(b):
            c.wait()

        @pl.loop(0, rb // qb)
        def _(r):
            at = pl.ds(pl.multiple_of(r * qb, qb), qb)
            rows = pl.ds(pl.multiple_of(b * rb + r * qb, qb), qb)
            low = low_lanes(qb)
            parts = []
            for pr in range(2):
                cols = slice(pr * LANES, pr * LANES + LANES)
                q = q_ref[rows, cols]
                zero = jnp.zeros_like(q)
                q2 = jnp.concatenate([jnp.where(low, q, zero), jnp.where(low, zero, q)], axis=0)
                sc = dot_nt(q2, kg_ref[:, cols])
                top = jnp.max(sc, axis=1, keepdims=True)
                e = jnp.exp(sc - top)
                total = row_sum(e)
                acc = dot_nn(e.astype(BF16), kg_ref[:, QB + pr * LANES:QB + pr * LANES + LANES])
                acc, m, total = (jnp.where(low, v[:qb], v[qb:]) for v in (acc, top, total))
                acc_w, m_w, l_w = (win_ref[b % 2, n, at, cols] for n in range(3))
                m_all = jnp.maximum(m, m_w)
                f, f_w = jnp.exp(m - m_all), jnp.exp(m_w - m_all)
                parts.append((acc * f + acc_w * f_w) / (total * f + l_w * f_w))
            place(rows, b * rb + r * qb, jnp.concatenate(parts, axis=1))

    def place(rows, row0, o):
        row = row0 + lax.broadcasted_iota(jnp.int32, (o.shape[0], 1), 0)
        hit = jnp.where(idx_ref[...] == row, 1.0, 0.0)
        placed = dot_nn(hit.astype(BF16), glob_ref[...])
        o_ref[me, rows] = jnp.where(row_sum(hit) > 0.5, placed, o).astype(BF16)

    def up(d, b):
        at = o_ref.at[me - d, rows_of(b)]
        return pltpu.make_async_remote_copy(at, at, up_send.at[d, b], up_recv.at[d, b], device_id={'tp': me + 1},
                                            device_id_type=pl.DeviceIdType.MESH)

    def down(d, b):
        at = o_ref.at[me + d, rows_of(b)]
        return pltpu.make_async_remote_copy(at, at, down_send.at[d, b], down_recv.at[d, b], device_id={'tp': me - 1},
                                            device_id_type=pl.DeviceIdType.MESH)

    def landed(recv, d, shard, b):
        at = o_ref.at[shard, rows_of(b)]
        pltpu.make_async_remote_copy(at, at, up_send.at[0, b], recv.at[d - 1, b], device_id={'tp': me},
                                     device_id_type=pl.DeviceIdType.MESH).wait_recv()

    def send_own(b):
        @pl.when(me < n_tp - 1)
        def _():
            up(0, b).start()

        @pl.when(me > 0)
        def _():
            down(0, b).start()

    for b in range(2):
        place(pl.ds(b * rb, rb), b * rb, pre_ref[b * rb:(b + 1) * rb, :].astype(F32))
    send_own(0)

    def step(s, carry):
        @pl.when(s + 1 < n_blk)
        def _():
            send_own(s + 1)

        for d in range(1, n_tp):
            b = s - (d - 1)

            @pl.when((b >= 0) & (b < n_blk) & (me >= d))
            def _():
                landed(up_recv, d, me - d, b)
                if d < n_tp - 1:
                    @pl.when(me < n_tp - 1)
                    def _():
                        up(d, b).start()

            @pl.when((b >= 0) & (b < n_blk) & (me + d <= n_tp - 1))
            def _():
                landed(down_recv, d, me + d, b)
                if d < n_tp - 1:
                    @pl.when(me > 0)
                    def _():
                        down(d, b).start()

        @pl.when(s + 2 < n_blk)
        def _():
            attend(s + 2)

        @pl.when(s == n_tp - 2)
        def _():
            for c in copies:
                c.wait()

        @pl.when(s >= n_tp - 2)
        def _():
            b = s - (n_tp - 2)
            rows = rows_of(b)
            mixed = dot_nn(o_ref[0, rows], wo_ref[:d_o, :])
            for t in range(1, n_tp):
                mixed += dot_nn(o_ref[t, rows], wo_ref[t * d_o:(t + 1) * d_o, :])
            h = (x_ref[rows].astype(F32) + mixed).astype(BF16)
            acc = h.astype(F32)
            for f0 in range(0, width, 512):
                f1 = min(f0 + 512, width)
                z = dot_nt(h, w1_ref[f0:f1, :])
                u = 0.5 * z * (1.0 + jnp.tanh(math.sqrt(2.0 / math.pi) * (z + 0.044715 * (z * z * z))))
                acc += dot_nn(u.astype(BF16), w2_ref[f0:f1, :])
            x_ref[rows] = acc.astype(BF16)
            pltpu.make_async_copy(x_ref.at[rows], y_hbm.at[rows], y_sem.at[b]).start()

        return carry

    lax.fori_loop(0, n_blk + n_tp - 2, step, 0)

    def finish(b, carry):
        rows = rows_of(b)
        pltpu.make_async_copy(x_ref.at[rows], y_hbm.at[rows], y_sem.at[b]).wait()
        for d in range(n_tp - 1):
            @pl.when((me < n_tp - 1) & (me >= d))
            def _():
                up(d, b).wait_send()

            @pl.when((me > 0) & (me + d <= n_tp - 1))
            def _():
                down(d, b).wait_send()

        return carry

    lax.fori_loop(0, n_blk, finish, 0)


def exchange_mlp(tokens, w_all, qkv, qkv_g, win, o_pre, glob_out, local_idx, n_tp, d_o, d_f):
    n_rows, dim = tokens.shape
    n_glob = local_idx.shape[0]
    n_rep = w_all.shape[0]
    rb = n_rows // 8
    n_blk = n_rows // rb
    anywhere = pl.BlockSpec(memory_space=pl.ANY)
    dma = pltpu.SemaphoreType.DMA
    return pl.pallas_call(
        functools.partial(exchange_mlp_kernel, n_tp=n_tp, n_rep=n_rep, d_o=d_o, d_f=d_f, rb=rb),
        in_specs=[anywhere] * 8 + [pl.BlockSpec(memory_space=pltpu.VMEM)] * 2, out_specs=anywhere,
        out_shape=jax.ShapeDtypeStruct(tokens.shape, BF16),
        scratch_shapes=[pltpu.VMEM((n_rows, dim), BF16), pltpu.VMEM((n_tp, n_rows, d_o), BF16),
                        pltpu.VMEM((n_tp * d_o, dim), BF16), pltpu.VMEM((n_tp * d_f, dim), BF16),
                        pltpu.VMEM((n_tp * d_f, dim), BF16), pltpu.VMEM((n_rows, d_o), BF16),
                        pltpu.VMEM((n_glob, 2 * d_o), BF16), pltpu.VMEM((n_glob, d_o), BF16),
                        pltpu.VMEM((2, 3, rb, d_o), F32), dma((4 + 3 * n_rep * n_tp,)), dma((2, 3)), dma((n_blk,)),
                        dma((n_tp - 1, n_blk)), dma((n_tp - 1, n_blk)), dma((n_tp - 1, n_blk)), dma((n_tp - 1, n_blk))],
        compiler_params=pltpu.CompilerParams(collective_id=1, has_side_effects=True, vmem_limit_bytes=60 << 20),
        cost_estimate=cost(2 * n_rows * dim * (dim + 2 * n_tp * d_f), 40e6), name="exchange_mlp",
    )(tokens, w_all, qkv, qkv_g, *win, glob_out, local_idx[None, :], o_pre)


def copy_kernel(a_ref, b_ref):
    b_ref[...] = a_ref[...]


def streamed(a):
    rb = a.shape[0] // 16
    spec = pl.BlockSpec((rb, a.shape[1]), lambda i: (i, 0))
    return pl.pallas_call(copy_kernel, grid=(16,), in_specs=[spec], out_specs=spec,
                          out_shape=jax.ShapeDtypeStruct(a.shape, a.dtype),
                          compiler_params=params(1), name="result")(a)


def combine(a, b):
    m = jnp.maximum(a[1], b[1])
    e_a, e_b = jnp.exp(a[1] - m), jnp.exp(b[1] - m)
    return a[0] * e_a + b[0] * e_b, m, a[2] * e_a + b[2] * e_b


def solution(mesh):
    n_seq = mesh.shape['sp']
    to_right = [(i, i + 1) for i in range(n_seq - 1)]
    to_left = [(i + 1, i) for i in range(n_seq - 1)]
    core_swap = [(i, i ^ 1) for i in range(n_seq)]
    chip_swap = [(i, i ^ 2) for i in range(n_seq)]

    def device_layer(tokens, glob_pos, w_query, w_key, w_value, w_out, w_up, w_down):
        n_rows, dim = tokens.shape
        n_glob = glob_pos.shape[0]
        sp = lax.axis_index('sp')
        core, chip = sp % 2, sp // 2
        first_row = sp * n_rows
        seq_len = n_rows * n_seq
        local_idx = glob_pos - first_row

        d_o, d_f = w_out.shape[0] * w_out.shape[1], w_down.shape[0]
        shard = jnp.concatenate([w_out.reshape(d_o, dim), w_down, w_up.T], axis=0)
        rep = lax.axis_index('dp') * n_seq + sp
        n_tp, n_rep = mesh.shape['tp'], mesh.shape['dp'] * n_seq
        piece = dim // n_rep
        w_slice = lax.dynamic_slice_in_dim(shard, rep * piece, piece, axis=1)
        w_all = lax.all_gather(w_slice, ('dp', 'sp', 'tp'))
        w_all = w_all.reshape(n_rep, n_tp, d_o + 2 * d_f, piece)

        w_cat = jnp.concatenate([w_query.reshape(dim, -1) * jnp.asarray(0.125, BF16),
                                 w_key.reshape(dim, -1), w_value.reshape(dim, -1)], axis=1)
        qkv, picked, kmax = qkv_part(tokens, w_cat, local_idx)
        halo_l = lax.ppermute(qkv[n_rows - WIN:, QB:], 'sp', to_right)
        halo_r = lax.ppermute(qkv[:WIN, QB:], 'sp', to_left)

        k_pos = first_row - WIN + jnp.arange(n_rows + 2 * WIN)
        k_off = jnp.any(glob_pos[:, None] == k_pos[None, :], axis=0) | (k_pos < 0) | (k_pos >= seq_len)
        bias = jnp.where(k_off, -jnp.inf, 0.0).astype(F32)[None, :]
        lane = jnp.arange(LANES) % HEAD
        extra = jnp.where(lane == 0, 1.0, jnp.where((lane == 1) & k_off[:, None], FLOOR, 0.0)).astype(BF16)

        half = n_glob // 2
        mine = lax.dynamic_slice_in_dim(picked, core * half, half)
        other = lax.ppermute(lax.dynamic_slice_in_dim(picked, (1 - core) * half, half), 'sp', core_swap)
        mine = mine + other
        got = lax.ppermute(mine, 'sp', chip_swap)
        win = window_part(qkv, halo_l, halo_r, extra, bias, kmax, 0, 3)
        got, win = lax.optimization_barrier((got, win))
        mine = mine + got
        other = lax.ppermute(mine, 'sp', core_swap)
        qkv_g = jnp.concatenate([jnp.where(core == 0, mine, other), jnp.where(core == 0, other, mine)], axis=0)

        part = global_queries_part(qkv_g, qkv, kmax)

        quarter = n_glob // 4
        got = lax.ppermute(lax.dynamic_slice_in_dim(part, (1 - core) * half, half, axis=1), 'sp', core_swap)
        joined = jnp.stack(combine(lax.dynamic_slice_in_dim(part, core * half, half, axis=1), got))
        joined, kmax = lax.optimization_barrier((joined, kmax))
        got = lax.ppermute(lax.dynamic_slice_in_dim(joined, (1 - chip) * quarter, quarter, axis=1), 'sp', chip_swap)
        win = window_part(qkv, halo_l, halo_r, extra, bias, kmax, 3, 4, win)
        o_pre = global_keys_part(qkv, qkv_g, kmax, win, n_rows // 4)
        got, win, o_pre = lax.optimization_barrier((got, win, o_pre))
        g_acc, _, g_l = combine(lax.dynamic_slice_in_dim(joined, chip * quarter, quarter, axis=1), got)
        mine = (g_acc / g_l).astype(BF16)
        other = lax.ppermute(mine, 'sp', chip_swap)
        mine = jnp.concatenate([jnp.where(chip == 0, mine, other), jnp.where(chip == 0, other, mine)], axis=0)
        other = lax.ppermute(mine, 'sp', core_swap)
        glob_out = jnp.concatenate([jnp.where(core == 0, mine, other), jnp.where(core == 0, other, mine)], axis=0)

        return streamed(exchange_mlp(tokens, w_all, qkv, qkv_g, win, o_pre, glob_out, local_idx, n_tp, d_o, d_f))

    row_spec = P(('dp', 'sp'), None)
    head_spec = P(None, 'tp', None)
    in_specs = (row_spec, P('dp'), head_spec, head_spec, head_spec, P('tp', None, None), P(None, 'tp'), P('tp', None))
    return jax.shard_map(device_layer, mesh=mesh, in_specs=in_specs, out_specs=row_spec, check_vma=False)
```

```python
import functools
import math

import jax
import jax.numpy as jnp
from jax import lax
from jax.experimental import pallas as pl
from jax.experimental.pallas import tpu as pltpu
from jax.sharding import PartitionSpec as P

WIN = 256
QB = 256
FLOOR = -3.0e38
F32 = jnp.float32
BF16 = jnp.bfloat16
LANES = 128
HEAD = 64
NT = (((1,), (1,)), ((), ()))


def dot_nt(a, b):
    return lax.dot_general(a, b, NT, preferred_element_type=F32)


def dot_nn(a, b):
    return jnp.dot(a, b, preferred_element_type=F32)


def params(n_axes, vmem_mib=48):
    return pltpu.CompilerParams(
        dimension_semantics=("arbitrary",) * n_axes, vmem_limit_bytes=vmem_mib << 20)


def cost(flops, bytes_accessed, exps=0):
    return pl.CostEstimate(flops=int(flops), bytes_accessed=int(bytes_accessed), transcendentals=int(exps))


def head_sums(rows):
    n = rows.shape[1]
    r = lax.broadcasted_iota(jnp.int32, (n, n), 0) // HEAD
    c = lax.broadcasted_iota(jnp.int32, (n, n), 1) // HEAD
    pick = jnp.where(r == (c + 1 - 2 * (c % 2)), 1.0, 0.0).astype(BF16)
    wide = rows.astype(F32)
    return dot_nn((wide * wide).astype(BF16), pick)


def qkv_kernel(pos_ref, idx_ref, x_ref, w_ref, qkv_ref, pick_ref, kmax_ref, acc_ref):
    step = pl.program_id(0)
    n_blk = x_ref.shape[0]
    lo = step * n_blk
    gb = LANES

    @pl.when(step == 0)
    def _():
        acc_ref[...] = jnp.zeros_like(acc_ref)
        kmax_ref[...] = jnp.zeros_like(kmax_ref)

    rows = dot_nn(x_ref[...], w_ref[...]).astype(BF16)
    qkv_ref[...] = rows
    kmax_ref[...] = jnp.maximum(kmax_ref[...], jnp.max(head_sums(rows[:, QB:512]), axis=0, keepdims=True))

    @pl.loop(0, idx_ref.shape[0] // gb)
    def _(b):
        g0 = pl.multiple_of(b * gb, gb)

        @pl.when((pos_ref[g0] < lo + n_blk) & (pos_ref[g0 + gb - 1] >= lo))
        def _():
            hit = idx_ref[pl.ds(g0, gb), :] == lo + lax.broadcasted_iota(jnp.int32, (gb, n_blk), 1)
            acc_ref[pl.ds(g0, gb), :] += dot_nn(hit.astype(F32).astype(BF16), qkv_ref[...])

    @pl.when(step == pl.num_programs(0) - 1)
    def _():
        pick_ref[...] = acc_ref[...].astype(pick_ref.dtype)


def qkv_part(tokens, w_cat, local_idx):
    n_rows, dim = tokens.shape
    n_glob = local_idx.shape[0]
    width = w_cat.shape[1]
    rb = 512
    return pl.pallas_call(
        qkv_kernel,
        grid_spec=pltpu.PrefetchScalarGridSpec(
            num_scalar_prefetch=1, grid=(n_rows // rb,),
            in_specs=[pl.BlockSpec((n_glob, 1), lambda i, p: (0, 0)), pl.BlockSpec((rb, dim), lambda i, p: (i, 0)),
                      pl.BlockSpec((dim, width), lambda i, p: (0, 0))],
            out_specs=[pl.BlockSpec((rb, width), lambda i, p: (i, 0)), pl.BlockSpec((n_glob, width), lambda i, p: (0, 0)),
                       pl.BlockSpec((1, QB), lambda i, p: (0, 0))],
            scratch_shapes=[pltpu.VMEM((n_glob, width), F32)]),
        out_shape=[jax.ShapeDtypeStruct((n_rows, width), BF16), jax.ShapeDtypeStruct((n_glob, width), BF16),
                   jax.ShapeDtypeStruct((1, QB), F32)],
        compiler_params=params(1), cost_estimate=cost(8e9, 24e6), name="qkv",
    )(local_idx, local_idx[:, None], tokens, w_cat)


def low_lanes(n):
    return lax.broadcasted_iota(jnp.int32, (n, LANES), 1) < HEAD


def shifts(q, kmax):
    return (-1.02 * jnp.sqrt(head_sums(q) * kmax)).astype(BF16)


def own_half(pair, other, half):
    low = low_lanes(pair.shape[0])
    return jnp.where(low, pair, other) if half == 0 else jnp.where(low, other, pair)


def query_rows(q, neg, half):
    lane = lax.broadcasted_iota(jnp.int32, q.shape, 1) % HEAD
    return own_half(q, jnp.where(lane == 0, neg, jnp.ones_like(neg)), half)


def key_extra(n):
    return jnp.where(lax.broadcasted_iota(jnp.int32, (n, LANES), 1) % HEAD == 0, 1.0, 0.0).astype(BF16)


def stream(q_rows, tiles):
    acc = total = None
    for keys, values in tiles:
        e = jnp.exp(dot_nt(q_rows, keys))
        part = e[:, :LANES] + e[:, LANES:]
        out = dot_nn(e.astype(BF16), values)
        acc = out if acc is None else acc + out
        total = part if total is None else total + part
    return acc, total


def row_sum(lanes):
    return jnp.sum(lanes, axis=1, keepdims=True)


def out_of_range(*totals):
    good = [jnp.logical_and(jnp.min(t) > 1e-25, jnp.max(t) < 1e30) for t in totals]
    return jnp.logical_not(functools.reduce(jnp.logical_and, good))


def exact_heads(q, n_keys, key_rows, acc_ref, m_ref, l_ref):
    @pl.loop(0, 2)
    def _(half):
        exact_head(q, half, n_keys, key_rows, acc_ref, m_ref, l_ref)


def exact_head(q, half, n_keys, key_rows, acc_ref, m_ref, l_ref):
    mine = lax.broadcasted_iota(jnp.int32, q.shape, 1) // HEAD == half
    q1 = jnp.where(mine, q, jnp.zeros_like(q))
    acc_ref[half] = jnp.zeros(q.shape, F32)
    l_ref[half] = jnp.zeros(q.shape, F32)
    m_ref[half] = jnp.full(q.shape, FLOOR, F32)

    @pl.loop(0, n_keys // QB)
    def _(c):
        keys, values, bias = key_rows(c)
        s = dot_nt(q1, keys)
        if bias is not None:
            s = s + bias
        m_old = m_ref[half]
        m_new = jnp.maximum(m_old, jnp.max(s, axis=1, keepdims=True))
        alpha = jnp.exp(m_old - m_new)
        e = jnp.exp(s - m_new[:, :1])
        l_ref[half] = alpha * l_ref[half] + row_sum(e)
        acc_ref[half] = alpha * acc_ref[half] + dot_nn(e.astype(BF16), values)
        m_ref[half] = m_new


def window_kernel(q_ref, kl_ref, kc_ref, kr_ref, vl_ref, vc_ref, vr_ref, hkl_ref, hkr_ref, hvl_ref, hvr_ref,
                  extra_ref, bias_ref, kmax_ref, *refs, first, n_blk):
    acc_ref, m_ref, l_ref, tri_ref, key_ref, val_ref, ea_ref, em_ref, el_ref = refs[-9:]
    i = first + pl.program_id(1)
    n = q_ref.shape[0]
    is_first = i == 0
    is_last = i == n_blk - 1

    @pl.when(pl.program_id(1) == 0)
    def _():
        r_i = lax.broadcasted_iota(jnp.int32, (QB, QB), 0)
        c_i = lax.broadcasted_iota(jnp.int32, (QB, QB), 1)
        tri_ref[:QB] = jnp.where(c_i <= r_i, 0.0, -jnp.inf)
        tri_ref[QB:2 * QB] = jnp.zeros((QB, QB), F32)
        tri_ref[2 * QB:] = jnp.where(c_i >= r_i, 0.0, -jnp.inf)

    key_ref[:QB] = jnp.where(is_first, hkl_ref[...], kl_ref[...])
    key_ref[QB:QB + n] = kc_ref[...]
    key_ref[QB + n:] = jnp.where(is_last, hkr_ref[...], kr_ref[...])
    val_ref[:QB] = jnp.where(is_first, hvl_ref[...], vl_ref[...])
    val_ref[QB:QB + n] = vc_ref[...]
    val_ref[QB + n:] = jnp.where(is_last, hvr_ref[...], vr_ref[...])

    q = q_ref[...]
    neg = shifts(q, kmax_ref[...])
    accs, sums = [], []
    for half in range(2):
        qx = query_rows(q, neg, half)
        acc, total = [None] * (n // QB), [None] * (n // QB)
        for t in range(n // QB + 2):
            b0, b1 = max(t - 2, 0), min(t + 1, n // QB)
            extra = extra_ref[pl.ds(pl.multiple_of(i * n + t * QB, QB), QB), :]
            s = dot_nt(qx[b0 * QB:b1 * QB], own_half(key_ref[t * QB:(t + 1) * QB], extra, half))
            e = jnp.exp(s + window_mask(tri_ref, t, b0, b1))
            part = e[:, :LANES] + e[:, LANES:]
            out = dot_nn(e.astype(BF16), val_ref[t * QB:(t + 1) * QB])
            for b in range(b0, b1):
                r = slice((b - b0) * QB, (b - b0 + 1) * QB)
                acc[b] = out[r] if acc[b] is None else acc[b] + out[r]
                total[b] = part[r] if total[b] is None else total[b] + part[r]
        accs.append(jnp.concatenate(acc, axis=0))
        sums.append(row_sum(jnp.concatenate(total, axis=0)))
    low = low_lanes(n)
    acc_ref[...] = jnp.where(low, accs[0], accs[1])
    l_ref[...] = jnp.where(low, sums[0], sums[1])
    m_ref[...] = -pltpu.roll(neg.astype(F32), HEAD, 1)

    @pl.when(out_of_range(*sums))
    def _():
        @pl.loop(0, n // QB)
        def _(b):
            rows = pl.ds(pl.multiple_of(b * QB, QB), QB)

            def key_rows(c):
                at = pl.ds(pl.multiple_of((b + c) * QB, QB), QB)
                bias = bias_ref[:, pl.ds(pl.multiple_of(i * n + (b + c) * QB, QB), QB)]
                return key_ref[at], val_ref[at], bias + tri_ref[pl.ds(pl.multiple_of((2 - c) * QB, QB), QB)]

            exact_heads(q_ref[rows], 3 * QB, key_rows, ea_ref, em_ref, el_ref)
            low = low_lanes(QB)
            for out, src in ((acc_ref, ea_ref), (m_ref, em_ref), (l_ref, el_ref)):
                out[rows] = jnp.where(low, src[0], src[1])


def window_mask(tri_ref, t, b0, b1):
    return tri_ref[(b0 - t + 2) * QB:(b1 - t + 2) * QB]


def window_part(qkv, halo_l, halo_r, extra, bias, kmax, first, last, win=()):
    n_rows = qkv.shape[0]
    rb = n_rows // 4
    per = rb // QB
    n_blk, n_small = n_rows // rb, n_rows // QB
    mid = lambda c: pl.BlockSpec((rb, LANES), lambda p, i: (first + i, 2 * c + p))
    left = lambda c: pl.BlockSpec((QB, LANES), lambda p, i: (jnp.maximum((first + i) * per - 1, 0), 2 * c + p))
    right = lambda c: pl.BlockSpec((QB, LANES), lambda p, i: (jnp.minimum((first + i) * per + per, n_small - 1), 2 * c + p))
    halo = lambda c: pl.BlockSpec((QB, LANES), lambda p, i: (0, 2 * c + p))
    whole = lambda a: pl.BlockSpec(a.shape, lambda p, i: (0,) * a.ndim)
    out = jax.ShapeDtypeStruct((n_rows, QB), F32)
    pair = pltpu.VMEM((2, QB, LANES), F32)
    part = (last - first) / n_blk
    return pl.pallas_call(
        functools.partial(window_kernel, first=first, n_blk=n_blk), grid=(2, last - first),
        in_specs=[mid(0), left(1), mid(1), right(1), left(2), mid(2), right(2), halo(0), halo(0), halo(1), halo(1),
                  whole(extra), whole(bias), pl.BlockSpec((1, LANES), lambda p, i: (0, p))]
        + [pl.BlockSpec(memory_space=pl.ANY)] * len(win),
        out_specs=[pl.BlockSpec((rb, LANES), lambda p, i: (first + i, p))] * 3,
        out_shape=[out, out, out], input_output_aliases={14 + n: n for n in range(len(win))},
        scratch_shapes=[pltpu.VMEM((3 * QB, QB), F32), pltpu.VMEM((rb + 2 * QB, LANES), BF16),
                        pltpu.VMEM((rb + 2 * QB, LANES), BF16), pair, pair, pair],
        compiler_params=params(2, 60), cost_estimate=cost(30e9 * part, 30e6 * part, 12e6 * part), name="window_part",
    )(qkv, qkv, qkv, qkv, qkv, qkv, qkv, halo_l, halo_r, halo_l, halo_r, extra, bias, kmax, *win)


def global_keys_kernel(q_ref, kg_ref, vg_ref, kmax_ref, acc_ref, m_ref, l_ref, out_ref,
                       k_ref, ea_ref, em_ref, el_ref):
    n = q_ref.shape[0]
    i = pl.program_id(1)

    @pl.when(i == 0)
    def _():
        extra = key_extra(kg_ref.shape[0])
        for half in range(2):
            k_ref[half] = own_half(kg_ref[...], extra, half)

    def finish(acc, m, total):
        m_all = jnp.maximum(m, m_ref[...])
        a, b = jnp.exp(m - m_all), jnp.exp(m_ref[...] - m_all)
        out_ref[...] = ((acc * a + acc_ref[...] * b) / (total * a + l_ref[...] * b)).astype(out_ref.dtype)

    q = q_ref[...]
    neg = shifts(q, kmax_ref[...])
    low = low_lanes(n)
    res = [stream(query_rows(q, neg, half), [(k_ref[half, t:t + QB], vg_ref[t:t + QB]) for t in range(0, vg_ref.shape[0], QB)])
           for half in range(2)]
    sums = [row_sum(r[1]) for r in res]
    finish(jnp.where(low, res[0][0], res[1][0]), -pltpu.roll(neg.astype(F32), HEAD, 1), jnp.where(low, sums[0], sums[1]))

    @pl.when(out_of_range(*sums))
    def _():
        def key_rows(c):
            at = pl.ds(pl.multiple_of(c * QB, QB), QB)
            return kg_ref[at], vg_ref[at], None

        exact_heads(q_ref[...], vg_ref.shape[0], key_rows, ea_ref, em_ref, el_ref)
        finish(*(jnp.where(low, r[0], r[1]) for r in (ea_ref, em_ref, el_ref)))


def global_keys_part(qkv, qkv_g, kmax, win, n_rows):
    n_glob = qkv_g.shape[0]
    rb = min(512, n_rows)
    row = pl.BlockSpec((rb, LANES), lambda p, i: (i, p))
    pair = pltpu.VMEM((2, rb, LANES), F32)
    return pl.pallas_call(
        global_keys_kernel, grid=(2, n_rows // rb),
        in_specs=[row, pl.BlockSpec((n_glob, LANES), lambda p, i: (0, 2 + p)), pl.BlockSpec((n_glob, LANES), lambda p, i: (0, 4 + p)),
                  pl.BlockSpec((1, LANES), lambda p, i: (0, p)), row, row, row],
        out_specs=row, out_shape=jax.ShapeDtypeStruct((n_rows, QB), BF16),
        scratch_shapes=[pltpu.VMEM((2, n_glob, LANES), BF16), pair, pair, pair],
        compiler_params=params(2), cost_estimate=cost(10e9, 8e6, 4e6), name="global_keys",
    )(qkv, qkv_g, qkv_g, kmax, *win)


def global_queries_kernel(q_ref, k_ref, v_ref, kmax_ref, out_ref, acc_ref, m_ref, l_ref, *, kb):
    j = pl.program_id(2)
    n = q_ref.shape[0]
    low = low_lanes(n)

    @pl.when(j == 0)
    def _():
        acc_ref[...] = jnp.zeros_like(acc_ref)
        l_ref[...] = jnp.zeros_like(l_ref)

    extra = key_extra(QB)
    q = q_ref[...]
    neg = shifts(q, kmax_ref[...])
    for half in range(2):
        rows = [pl.ds(pl.multiple_of(j * kb, kb) + t, QB) for t in range(0, kb, QB)]
        acc, total = stream(query_rows(q, neg, half), [(own_half(k_ref[r], extra, half), v_ref[r]) for r in rows])
        acc_ref[half] += acc
        l_ref[half] += total

    @pl.when(j == pl.num_programs(2) - 1)
    def _():
        sums = [row_sum(l_ref[half]) for half in range(2)]
        out_ref[0] = jnp.where(low, acc_ref[0], acc_ref[1])
        out_ref[1] = -pltpu.roll(neg.astype(F32), HEAD, 1)
        out_ref[2] = jnp.where(low, sums[0], sums[1])

        @pl.when(out_of_range(*sums))
        def _():
            def key_rows(c):
                at = pl.ds(pl.multiple_of(c * QB, QB), QB)
                return k_ref[at], v_ref[at], None

            exact_heads(q_ref[...], v_ref.shape[0], key_rows, acc_ref, m_ref, l_ref)
            for k, r in enumerate((acc_ref, m_ref, l_ref)):
                out_ref[k] = jnp.where(low, r[0], r[1])


def global_queries_part(qkv_g, qkv, kmax):
    n_glob = qkv_g.shape[0]
    n_rows = qkv.shape[0]
    rb = 512
    kb = min(1024, n_rows)
    return pl.pallas_call(
        functools.partial(global_queries_kernel, kb=kb), grid=(2, n_glob // rb, n_rows // kb),
        in_specs=[pl.BlockSpec((rb, LANES), lambda p, i, j: (i, p)), pl.BlockSpec((n_rows, LANES), lambda p, i, j: (0, 2 + p)),
                  pl.BlockSpec((n_rows, LANES), lambda p, i, j: (0, 4 + p)), pl.BlockSpec((1, LANES), lambda p, i, j: (0, p))],
        out_specs=pl.BlockSpec((3, rb, LANES), lambda p, i, j: (0, i, p)),
        out_shape=jax.ShapeDtypeStruct((3, n_glob, QB), F32),
        scratch_shapes=[pltpu.VMEM((2, rb, LANES), F32)] * 3,
        compiler_params=params(3), cost_estimate=cost(34e9, 20e6, 16e6), name="global_queries",
    )(qkv_g, qkv, qkv, kmax)


def exchange_mlp_kernel(x_hbm, w_hbm, qkv_hbm, qkvg_hbm, acc_hbm, m_hbm, l_hbm, glob_hbm, idx_ref, pre_ref, y_hbm,
                        x_ref, o_ref, wo_ref, w2_ref, w1_ref, q_ref, kg_ref, glob_ref, win_ref, load_sem, win_sem, y_sem,
                        up_send, up_recv, down_send, down_recv, *, n_tp, n_rep, d_o, d_f, rb):
    me = lax.axis_index('tp')
    n_blk = x_ref.shape[0] // rb
    width = n_tp * d_f
    qb = min(QB, rb)

    barrier = pltpu.get_barrier_semaphore()

    @pl.when(me > 0)
    def _():
        pl.semaphore_signal(barrier, inc=1, device_id={'tp': me - 1}, device_id_type=pl.DeviceIdType.MESH)

    @pl.when(me < n_tp - 1)
    def _():
        pl.semaphore_signal(barrier, inc=1, device_id={'tp': me + 1}, device_id_type=pl.DeviceIdType.MESH)

    early = [pltpu.make_async_copy(qkv_hbm.at[:, pl.ds(0, QB)], q_ref, load_sem.at[0]),
             pltpu.make_async_copy(qkvg_hbm.at[:, pl.ds(QB, 512)], kg_ref, load_sem.at[1]),
             pltpu.make_async_copy(glob_hbm, glob_ref, load_sem.at[2])]

    def rows_of(b):
        return pl.ds(pl.multiple_of(b * rb, rb), rb)

    def fetch(b):
        return [pltpu.make_async_copy(h.at[rows_of(b)], win_ref.at[b % 2, n], win_sem.at[b % 2, n])
                for n, h in enumerate((acc_hbm, m_hbm, l_hbm))]

    for c in early + fetch(2):
        c.start()
    copies = [pltpu.make_async_copy(x_hbm, x_ref, load_sem.at[3])]
    piece = wo_ref.shape[1] // n_rep
    for j in range(n_rep):
        for t in range(n_tp):
            lanes = pl.ds(j * piece, piece)
            for src, n, dst in ((0, d_o, wo_ref), (d_o, d_f, w2_ref), (d_o + d_f, d_f, w1_ref)):
                copies.append(pltpu.make_async_copy(w_hbm.at[j, t, pl.ds(src, n)], dst.at[pl.ds(t * n, n), lanes],
                                                    load_sem.at[3 + len(copies)]))
    for c in copies:
        c.start()

    ends = jnp.logical_or(me == 0, me == n_tp - 1)

    @pl.when(ends)
    def _():
        pl.semaphore_wait(barrier, 1)

    @pl.when(jnp.logical_not(ends))
    def _():
        pl.semaphore_wait(barrier, 2)

    for c in early:
        c.wait()

    def attend(b):
        @pl.when(b + 1 < n_blk)
        def _():
            for c in fetch(b + 1):
                c.start()

        for c in fetch(b):
            c.wait()

        @pl.loop(0, rb // qb)
        def _(r):
            at = pl.ds(pl.multiple_of(r * qb, qb), qb)
            rows = pl.ds(pl.multiple_of(b * rb + r * qb, qb), qb)
            low = low_lanes(qb)
            parts = []
            for pr in range(2):
                cols = slice(pr * LANES, pr * LANES + LANES)
                q = q_ref[rows, cols]
                zero = jnp.zeros_like(q)
                q2 = jnp.concatenate([jnp.where(low, q, zero), jnp.where(low, zero, q)], axis=0)
                sc = dot_nt(q2, kg_ref[:, cols])
                top = jnp.max(sc, axis=1, keepdims=True)
                e = jnp.exp(sc - top)
                total = row_sum(e)
                acc = dot_nn(e.astype(BF16), kg_ref[:, QB + pr * LANES:QB + pr * LANES + LANES])
                acc, m, total = (jnp.where(low, v[:qb], v[qb:]) for v in (acc, top, total))
                acc_w, m_w, l_w = (win_ref[b % 2, n, at, cols] for n in range(3))
                m_all = jnp.maximum(m, m_w)
                f, f_w = jnp.exp(m - m_all), jnp.exp(m_w - m_all)
                parts.append((acc * f + acc_w * f_w) / (total * f + l_w * f_w))
            place(rows, b * rb + r * qb, jnp.concatenate(parts, axis=1))

    def place(rows, row0, o):
        row = row0 + lax.broadcasted_iota(jnp.int32, (o.shape[0], 1), 0)
        hit = jnp.where(idx_ref[...] == row, 1.0, 0.0)
        placed = dot_nn(hit.astype(BF16), glob_ref[...])
        o_ref[me, rows] = jnp.where(row_sum(hit) > 0.5, placed, o).astype(BF16)

    def up(d, b):
        at = o_ref.at[me - d, rows_of(b)]
        return pltpu.make_async_remote_copy(at, at, up_send.at[d, b], up_recv.at[d, b], device_id={'tp': me + 1},
                                            device_id_type=pl.DeviceIdType.MESH)

    def down(d, b):
        at = o_ref.at[me + d, rows_of(b)]
        return pltpu.make_async_remote_copy(at, at, down_send.at[d, b], down_recv.at[d, b], device_id={'tp': me - 1},
                                            device_id_type=pl.DeviceIdType.MESH)

    def landed(recv, d, shard, b):
        at = o_ref.at[shard, rows_of(b)]
        pltpu.make_async_remote_copy(at, at, up_send.at[0, b], recv.at[d - 1, b], device_id={'tp': me},
                                     device_id_type=pl.DeviceIdType.MESH).wait_recv()

    def send_own(b):
        @pl.when(me < n_tp - 1)
        def _():
            up(0, b).start()

        @pl.when(me > 0)
        def _():
            down(0, b).start()

    for b in range(2):
        place(pl.ds(b * rb, rb), b * rb, pre_ref[b * rb:(b + 1) * rb, :].astype(F32))
    send_own(0)

    def step(s, carry):
        @pl.when(s + 1 < n_blk)
        def _():
            send_own(s + 1)

        for d in range(1, n_tp):
            b = s - (d - 1)

            @pl.when((b >= 0) & (b < n_blk) & (me >= d))
            def _():
                landed(up_recv, d, me - d, b)
                if d < n_tp - 1:
                    @pl.when(me < n_tp - 1)
                    def _():
                        up(d, b).start()

            @pl.when((b >= 0) & (b < n_blk) & (me + d <= n_tp - 1))
            def _():
                landed(down_recv, d, me + d, b)
                if d < n_tp - 1:
                    @pl.when(me > 0)
                    def _():
                        down(d, b).start()

        @pl.when(s + 2 < n_blk)
        def _():
            attend(s + 2)

        @pl.when(s == n_tp - 2)
        def _():
            for c in copies:
                c.wait()

        @pl.when(s >= n_tp - 2)
        def _():
            b = s - (n_tp - 2)
            rows = rows_of(b)
            mixed = dot_nn(o_ref[0, rows], wo_ref[:d_o, :])
            for t in range(1, n_tp):
                mixed += dot_nn(o_ref[t, rows], wo_ref[t * d_o:(t + 1) * d_o, :])
            h = (x_ref[rows].astype(F32) + mixed).astype(BF16)
            acc = h.astype(F32)
            for f0 in range(0, width, 512):
                f1 = min(f0 + 512, width)
                z = dot_nt(h, w1_ref[f0:f1, :])
                u = 0.5 * z * (1.0 + jnp.tanh(math.sqrt(2.0 / math.pi) * (z + 0.044715 * (z * z * z))))
                acc += dot_nn(u.astype(BF16), w2_ref[f0:f1, :])
            x_ref[rows] = acc.astype(BF16)
            pltpu.make_async_copy(x_ref.at[rows], y_hbm.at[rows], y_sem.at[b]).start()

        return carry

    lax.fori_loop(0, n_blk + n_tp - 2, step, 0)

    def finish(b, carry):
        rows = rows_of(b)
        pltpu.make_async_copy(x_ref.at[rows], y_hbm.at[rows], y_sem.at[b]).wait()
        for d in range(n_tp - 1):
            @pl.when((me < n_tp - 1) & (me >= d))
            def _():
                up(d, b).wait_send()

            @pl.when((me > 0) & (me + d <= n_tp - 1))
            def _():
                down(d, b).wait_send()

        return carry

    lax.fori_loop(0, n_blk, finish, 0)


def exchange_mlp(tokens, w_all, qkv, qkv_g, win, o_pre, glob_out, local_idx, n_tp, d_o, d_f):
    n_rows, dim = tokens.shape
    n_glob = local_idx.shape[0]
    n_rep = w_all.shape[0]
    rb = n_rows // 8
    n_blk = n_rows // rb
    anywhere = pl.BlockSpec(memory_space=pl.ANY)
    dma = pltpu.SemaphoreType.DMA
    return pl.pallas_call(
        functools.partial(exchange_mlp_kernel, n_tp=n_tp, n_rep=n_rep, d_o=d_o, d_f=d_f, rb=rb),
        in_specs=[anywhere] * 8 + [pl.BlockSpec(memory_space=pltpu.VMEM)] * 2, out_specs=anywhere,
        out_shape=jax.ShapeDtypeStruct(tokens.shape, BF16),
        scratch_shapes=[pltpu.VMEM((n_rows, dim), BF16), pltpu.VMEM((n_tp, n_rows, d_o), BF16),
                        pltpu.VMEM((n_tp * d_o, dim), BF16), pltpu.VMEM((n_tp * d_f, dim), BF16),
                        pltpu.VMEM((n_tp * d_f, dim), BF16), pltpu.VMEM((n_rows, d_o), BF16),
                        pltpu.VMEM((n_glob, 2 * d_o), BF16), pltpu.VMEM((n_glob, d_o), BF16),
                        pltpu.VMEM((2, 3, rb, d_o), F32), dma((4 + 3 * n_rep * n_tp,)), dma((2, 3)), dma((n_blk,)),
                        dma((n_tp - 1, n_blk)), dma((n_tp - 1, n_blk)), dma((n_tp - 1, n_blk)), dma((n_tp - 1, n_blk))],
        compiler_params=pltpu.CompilerParams(collective_id=1, has_side_effects=True, vmem_limit_bytes=60 << 20),
        cost_estimate=cost(2 * n_rows * dim * (dim + 2 * n_tp * d_f), 40e6), name="exchange_mlp",
    )(tokens, w_all, qkv, qkv_g, *win, glob_out, local_idx[None, :], o_pre)


def copy_kernel(a_hbm, b_hbm, buf_ref, in_sem, out_sem):
    n, rows = buf_ref.shape[:2]
    at = [pl.ds(i * rows, rows) for i in range(n)]
    loads = [pltpu.make_async_copy(a_hbm.at[r], buf_ref.at[i], in_sem.at[i]) for i, r in enumerate(at)]
    stores = [pltpu.make_async_copy(buf_ref.at[i], b_hbm.at[r], out_sem.at[i]) for i, r in enumerate(at)]
    for c in loads:
        c.start()
    for load, store in zip(loads, stores):
        load.wait()
        store.start()
    for c in stores:
        c.wait()


def streamed(a):
    n = 8
    anywhere = pl.BlockSpec(memory_space=pl.ANY)
    dma = pltpu.SemaphoreType.DMA
    return pl.pallas_call(copy_kernel, in_specs=[anywhere], out_specs=anywhere,
                          out_shape=jax.ShapeDtypeStruct(a.shape, a.dtype),
                          scratch_shapes=[pltpu.VMEM((n, a.shape[0] // n, a.shape[1]), a.dtype), dma((n,)), dma((n,))],
                          compiler_params=pltpu.CompilerParams(vmem_limit_bytes=params(0).vmem_limit_bytes), name="result")(a)


def combine(a, b):
    m = jnp.maximum(a[1], b[1])
    e_a, e_b = jnp.exp(a[1] - m), jnp.exp(b[1] - m)
    return a[0] * e_a + b[0] * e_b, m, a[2] * e_a + b[2] * e_b


def solution(mesh):
    n_seq = mesh.shape['sp']
    to_right = [(i, i + 1) for i in range(n_seq - 1)]
    to_left = [(i + 1, i) for i in range(n_seq - 1)]
    core_swap = [(i, i ^ 1) for i in range(n_seq)]
    chip_swap = [(i, i ^ 2) for i in range(n_seq)]

    def device_layer(tokens, glob_pos, w_query, w_key, w_value, w_out, w_up, w_down):
        n_rows, dim = tokens.shape
        n_glob = glob_pos.shape[0]
        sp = lax.axis_index('sp')
        core, chip = sp % 2, sp // 2
        first_row = sp * n_rows
        seq_len = n_rows * n_seq
        local_idx = glob_pos - first_row

        d_o, d_f = w_out.shape[0] * w_out.shape[1], w_down.shape[0]
        shard = jnp.concatenate([w_out.reshape(d_o, dim), w_down, w_up.T], axis=0)
        rep = lax.axis_index('dp') * n_seq + sp
        n_tp, n_rep = mesh.shape['tp'], mesh.shape['dp'] * n_seq
        piece = dim // n_rep
        w_slice = lax.dynamic_slice_in_dim(shard, rep * piece, piece, axis=1)
        w_all = lax.all_gather(w_slice, ('dp', 'sp', 'tp'))
        w_all = w_all.reshape(n_rep, n_tp, d_o + 2 * d_f, piece)

        w_cat = jnp.concatenate([w_query.reshape(dim, -1) * jnp.asarray(0.125, BF16),
                                 w_key.reshape(dim, -1), w_value.reshape(dim, -1)], axis=1)
        qkv, picked, kmax = qkv_part(tokens, w_cat, local_idx)
        halo_l = lax.ppermute(qkv[n_rows - WIN:, QB:], 'sp', to_right)
        halo_r = lax.ppermute(qkv[:WIN, QB:], 'sp', to_left)

        half = n_glob // 2
        mine = lax.dynamic_slice_in_dim(picked, core * half, half)
        other = lax.ppermute(lax.dynamic_slice_in_dim(picked, (1 - core) * half, half), 'sp', core_swap)
        mine = mine + other
        mine, flag_pos = lax.optimization_barrier((mine, glob_pos))
        k_pos = first_row - WIN + jnp.arange(n_rows + 2 * WIN)
        k_off = jnp.any(flag_pos[:, None] == k_pos[None, :], axis=0) | (k_pos < 0) | (k_pos >= seq_len)
        bias = jnp.where(k_off, -jnp.inf, 0.0).astype(F32)[None, :]
        lane = jnp.arange(LANES) % HEAD
        extra = jnp.where(lane == 0, 1.0, jnp.where((lane == 1) & k_off[:, None], FLOOR, 0.0)).astype(BF16)
        got = lax.ppermute(mine, 'sp', chip_swap)
        win = window_part(qkv, halo_l, halo_r, extra, bias, kmax, 0, 3)
        got, win = lax.optimization_barrier((got, win))
        mine = mine + got
        other = lax.ppermute(mine, 'sp', core_swap)
        qkv_g = jnp.concatenate([jnp.where(core == 0, mine, other), jnp.where(core == 0, other, mine)], axis=0)

        part = global_queries_part(qkv_g, qkv, kmax)

        quarter = n_glob // 4
        got = lax.ppermute(lax.dynamic_slice_in_dim(part, (1 - core) * half, half, axis=1), 'sp', core_swap)
        joined = jnp.stack(combine(lax.dynamic_slice_in_dim(part, core * half, half, axis=1), got))
        joined, kmax = lax.optimization_barrier((joined, kmax))
        got = lax.ppermute(lax.dynamic_slice_in_dim(joined, (1 - chip) * quarter, quarter, axis=1), 'sp', chip_swap)
        win = window_part(qkv, halo_l, halo_r, extra, bias, kmax, 3, 4, win)
        o_pre = global_keys_part(qkv, qkv_g, kmax, win, n_rows // 4)
        got, win, o_pre = lax.optimization_barrier((got, win, o_pre))
        g_acc, _, g_l = combine(lax.dynamic_slice_in_dim(joined, chip * quarter, quarter, axis=1), got)
        mine = (g_acc / g_l).astype(BF16)
        other = lax.ppermute(mine, 'sp', chip_swap)
        mine = jnp.concatenate([jnp.where(chip == 0, mine, other), jnp.where(chip == 0, other, mine)], axis=0)
        other = lax.ppermute(mine, 'sp', core_swap)
        glob_out = jnp.concatenate([jnp.where(core == 0, mine, other), jnp.where(core == 0, other, mine)], axis=0)

        return streamed(exchange_mlp(tokens, w_all, qkv, qkv_g, win, o_pre, glob_out, local_idx, n_tp, d_o, d_f))

    row_spec = P(('dp', 'sp'), None)
    head_spec = P(None, 'tp', None)
    in_specs = (row_spec, P('dp'), head_spec, head_spec, head_spec, P('tp', None, None), P(None, 'tp'), P('tp', None))
    return jax.shard_map(device_layer, mesh=mesh, in_specs=in_specs, out_specs=row_spec, check_vma=False)
```

```python
import functools
import math

import jax
import jax.numpy as jnp
from jax import lax
from jax.experimental import pallas as pl
from jax.experimental.pallas import tpu as pltpu
from jax.sharding import PartitionSpec as P

WIN = 256
QB = 256
FLOOR = -3.0e38
F32 = jnp.float32
BF16 = jnp.bfloat16
LANES = 128
HEAD = 64
NT = (((1,), (1,)), ((), ()))


def dot_nt(a, b):
    return lax.dot_general(a, b, NT, preferred_element_type=F32)


def dot_nn(a, b):
    return jnp.dot(a, b, preferred_element_type=F32)


def params(n_axes, vmem_mib=48):
    return pltpu.CompilerParams(
        dimension_semantics=("arbitrary",) * n_axes, vmem_limit_bytes=vmem_mib << 20)


def cost(flops, bytes_accessed, exps=0):
    return pl.CostEstimate(flops=int(flops), bytes_accessed=int(bytes_accessed), transcendentals=int(exps))


def head_sums(rows):
    n = rows.shape[1]
    r = lax.broadcasted_iota(jnp.int32, (n, n), 0) // HEAD
    c = lax.broadcasted_iota(jnp.int32, (n, n), 1) // HEAD
    pick = jnp.where(r == (c + 1 - 2 * (c % 2)), 1.0, 0.0).astype(BF16)
    wide = rows.astype(F32)
    return dot_nn((wide * wide).astype(BF16), pick)


def qkv_kernel(pos_ref, idx_ref, x_ref, w_ref, qkv_ref, pick_ref, kmax_ref, acc_ref):
    step = pl.program_id(0)
    n_blk = x_ref.shape[0]
    lo = step * n_blk
    gb = LANES

    @pl.when(step == 0)
    def _():
        acc_ref[...] = jnp.zeros_like(acc_ref)
        kmax_ref[...] = jnp.zeros_like(kmax_ref)

    rows = dot_nn(x_ref[...], w_ref[...]).astype(BF16)
    qkv_ref[...] = rows
    kmax_ref[...] = jnp.maximum(kmax_ref[...], jnp.max(head_sums(rows[:, QB:512]), axis=0, keepdims=True))

    @pl.loop(0, idx_ref.shape[0] // gb)
    def _(b):
        g0 = pl.multiple_of(b * gb, gb)

        @pl.when((pos_ref[g0] < lo + n_blk) & (pos_ref[g0 + gb - 1] >= lo))
        def _():
            hit = idx_ref[pl.ds(g0, gb), :] == lo + lax.broadcasted_iota(jnp.int32, (gb, n_blk), 1)
            acc_ref[pl.ds(g0, gb), :] += dot_nn(hit.astype(F32).astype(BF16), qkv_ref[...])

    @pl.when(step == pl.num_programs(0) - 1)
    def _():
        pick_ref[...] = acc_ref[...].astype(pick_ref.dtype)


def qkv_part(tokens, w_cat, local_idx):
    n_rows, dim = tokens.shape
    n_glob = local_idx.shape[0]
    width = w_cat.shape[1]
    rb = 512
    return pl.pallas_call(
        qkv_kernel,
        grid_spec=pltpu.PrefetchScalarGridSpec(
            num_scalar_prefetch=1, grid=(n_rows // rb,),
            in_specs=[pl.BlockSpec((n_glob, 1), lambda i, p: (0, 0)), pl.BlockSpec((rb, dim), lambda i, p: (i, 0)),
                      pl.BlockSpec((dim, width), lambda i, p: (0, 0))],
            out_specs=[pl.BlockSpec((rb, width), lambda i, p: (i, 0)), pl.BlockSpec((n_glob, width), lambda i, p: (0, 0)),
                       pl.BlockSpec((1, QB), lambda i, p: (0, 0))],
            scratch_shapes=[pltpu.VMEM((n_glob, width), F32)]),
        out_shape=[jax.ShapeDtypeStruct((n_rows, width), BF16), jax.ShapeDtypeStruct((n_glob, width), BF16),
                   jax.ShapeDtypeStruct((1, QB), F32)],
        compiler_params=params(1), cost_estimate=cost(8e9, 24e6), name="qkv",
    )(local_idx, local_idx[:, None], tokens, w_cat)


def low_lanes(n):
    return lax.broadcasted_iota(jnp.int32, (n, LANES), 1) < HEAD


def shifts(q, kmax):
    return (-1.02 * jnp.sqrt(head_sums(q) * kmax)).astype(BF16)


def own_half(pair, other, half):
    low = low_lanes(pair.shape[0])
    return jnp.where(low, pair, other) if half == 0 else jnp.where(low, other, pair)


def query_rows(q, neg, half):
    lane = lax.broadcasted_iota(jnp.int32, q.shape, 1) % HEAD
    return own_half(q, jnp.where(lane == 0, neg, jnp.ones_like(neg)), half)


def key_extra(n):
    return jnp.where(lax.broadcasted_iota(jnp.int32, (n, LANES), 1) % HEAD == 0, 1.0, 0.0).astype(BF16)


def stream(q_rows, tiles):
    acc = total = None
    for keys, values in tiles:
        e = jnp.exp(dot_nt(q_rows, keys))
        part = e[:, :LANES] + e[:, LANES:]
        out = dot_nn(e.astype(BF16), values)
        acc = out if acc is None else acc + out
        total = part if total is None else total + part
    return acc, total


def row_sum(lanes):
    return jnp.sum(lanes, axis=1, keepdims=True)


def out_of_range(*totals):
    good = [jnp.logical_and(jnp.min(t) > 1e-25, jnp.max(t) < 1e30) for t in totals]
    return jnp.logical_not(functools.reduce(jnp.logical_and, good))


def exact_heads(q, n_keys, key_rows, acc_ref, m_ref, l_ref):
    @pl.loop(0, 2)
    def _(half):
        exact_head(q, half, n_keys, key_rows, acc_ref, m_ref, l_ref)


def exact_head(q, half, n_keys, key_rows, acc_ref, m_ref, l_ref):
    mine = lax.broadcasted_iota(jnp.int32, q.shape, 1) // HEAD == half
    q1 = jnp.where(mine, q, jnp.zeros_like(q))
    acc_ref[half] = jnp.zeros(q.shape, F32)
    l_ref[half] = jnp.zeros(q.shape, F32)
    m_ref[half] = jnp.full(q.shape, FLOOR, F32)

    @pl.loop(0, n_keys // QB)
    def _(c):
        keys, values, bias = key_rows(c)
        s = dot_nt(q1, keys)
        if bias is not None:
            s = s + bias
        m_old = m_ref[half]
        m_new = jnp.maximum(m_old, jnp.max(s, axis=1, keepdims=True))
        alpha = jnp.exp(m_old - m_new)
        e = jnp.exp(s - m_new[:, :1])
        l_ref[half] = alpha * l_ref[half] + row_sum(e)
        acc_ref[half] = alpha * acc_ref[half] + dot_nn(e.astype(BF16), values)
        m_ref[half] = m_new


def window_kernel(q_ref, kl_ref, kc_ref, kr_ref, vl_ref, vc_ref, vr_ref, hkl_ref, hkr_ref, hvl_ref, hvr_ref,
                  extra_ref, bias_ref, kmax_ref, *refs, first, n_blk):
    acc_ref, m_ref, l_ref, tri_ref, key_ref, val_ref, ea_ref, em_ref, el_ref = refs[-9:]
    i = first + pl.program_id(1)
    n = q_ref.shape[0]
    is_first = i == 0
    is_last = i == n_blk - 1

    @pl.when(pl.program_id(1) == 0)
    def _():
        r_i = lax.broadcasted_iota(jnp.int32, (QB, QB), 0)
        c_i = lax.broadcasted_iota(jnp.int32, (QB, QB), 1)
        tri_ref[:QB] = jnp.where(c_i <= r_i, 0.0, -jnp.inf)
        tri_ref[QB:2 * QB] = jnp.zeros((QB, QB), F32)
        tri_ref[2 * QB:] = jnp.where(c_i >= r_i, 0.0, -jnp.inf)

    key_ref[:QB] = jnp.where(is_first, hkl_ref[...], kl_ref[...])
    key_ref[QB:QB + n] = kc_ref[...]
    key_ref[QB + n:] = jnp.where(is_last, hkr_ref[...], kr_ref[...])
    val_ref[:QB] = jnp.where(is_first, hvl_ref[...], vl_ref[...])
    val_ref[QB:QB + n] = vc_ref[...]
    val_ref[QB + n:] = jnp.where(is_last, hvr_ref[...], vr_ref[...])

    q = q_ref[...]
    neg = shifts(q, kmax_ref[...])
    accs, sums = [], []
    for half in range(2):
        qx = query_rows(q, neg, half)
        acc, total = [None] * (n // QB), [None] * (n // QB)
        for t in range(n // QB + 2):
            b0, b1 = max(t - 2, 0), min(t + 1, n // QB)
            extra = extra_ref[pl.ds(pl.multiple_of(i * n + t * QB, QB), QB), :]
            s = dot_nt(qx[b0 * QB:b1 * QB], own_half(key_ref[t * QB:(t + 1) * QB], extra, half))
            e = jnp.exp(s + window_mask(tri_ref, t, b0, b1))
            part = e[:, :LANES] + e[:, LANES:]
            out = dot_nn(e.astype(BF16), val_ref[t * QB:(t + 1) * QB])
            for b in range(b0, b1):
                r = slice((b - b0) * QB, (b - b0 + 1) * QB)
                acc[b] = out[r] if acc[b] is None else acc[b] + out[r]
                total[b] = part[r] if total[b] is None else total[b] + part[r]
        accs.append(jnp.concatenate(acc, axis=0))
        sums.append(row_sum(jnp.concatenate(total, axis=0)))
    low = low_lanes(n)
    acc_ref[...] = jnp.where(low, accs[0], accs[1])
    l_ref[...] = jnp.where(low, sums[0], sums[1])
    m_ref[...] = -pltpu.roll(neg.astype(F32), HEAD, 1)

    @pl.when(out_of_range(*sums))
    def _():
        @pl.loop(0, n // QB)
        def _(b):
            rows = pl.ds(pl.multiple_of(b * QB, QB), QB)

            def key_rows(c):
                at = pl.ds(pl.multiple_of((b + c) * QB, QB), QB)
                bias = bias_ref[:, pl.ds(pl.multiple_of(i * n + (b + c) * QB, QB), QB)]
                return key_ref[at], val_ref[at], bias + tri_ref[pl.ds(pl.multiple_of((2 - c) * QB, QB), QB)]

            exact_heads(q_ref[rows], 3 * QB, key_rows, ea_ref, em_ref, el_ref)
            low = low_lanes(QB)
            for out, src in ((acc_ref, ea_ref), (m_ref, em_ref), (l_ref, el_ref)):
                out[rows] = jnp.where(low, src[0], src[1])


def window_mask(tri_ref, t, b0, b1):
    return tri_ref[(b0 - t + 2) * QB:(b1 - t + 2) * QB]


def window_part(qkv, halo_l, halo_r, extra, bias, kmax, first, last, win=()):
    n_rows = qkv.shape[0]
    rb = n_rows // 4
    per = rb // QB
    n_blk, n_small = n_rows // rb, n_rows // QB
    mid = lambda c: pl.BlockSpec((rb, LANES), lambda p, i: (first + i, 2 * c + p))
    left = lambda c: pl.BlockSpec((QB, LANES), lambda p, i: (jnp.maximum((first + i) * per - 1, 0), 2 * c + p))
    right = lambda c: pl.BlockSpec((QB, LANES), lambda p, i: (jnp.minimum((first + i) * per + per, n_small - 1), 2 * c + p))
    halo = lambda c: pl.BlockSpec((QB, LANES), lambda p, i: (0, 2 * c + p))
    whole = lambda a: pl.BlockSpec(a.shape, lambda p, i: (0,) * a.ndim)
    out = jax.ShapeDtypeStruct((n_rows, QB), F32)
    pair = pltpu.VMEM((2, QB, LANES), F32)
    part = (last - first) / n_blk
    return pl.pallas_call(
        functools.partial(window_kernel, first=first, n_blk=n_blk), grid=(2, last - first),
        in_specs=[mid(0), left(1), mid(1), right(1), left(2), mid(2), right(2), halo(0), halo(0), halo(1), halo(1),
                  whole(extra), whole(bias), pl.BlockSpec((1, LANES), lambda p, i: (0, p))]
        + [pl.BlockSpec(memory_space=pl.ANY)] * len(win),
        out_specs=[pl.BlockSpec((rb, LANES), lambda p, i: (first + i, p))] * 3,
        out_shape=[out, out, out], input_output_aliases={14 + n: n for n in range(len(win))},
        scratch_shapes=[pltpu.VMEM((3 * QB, QB), F32), pltpu.VMEM((rb + 2 * QB, LANES), BF16),
                        pltpu.VMEM((rb + 2 * QB, LANES), BF16), pair, pair, pair],
        compiler_params=params(2, 60), cost_estimate=cost(30e9 * part, 30e6 * part, 12e6 * part), name="window_part",
    )(qkv, qkv, qkv, qkv, qkv, qkv, qkv, halo_l, halo_r, halo_l, halo_r, extra, bias, kmax, *win)


def global_keys_kernel(q_ref, kg_ref, vg_ref, kmax_ref, acc_ref, m_ref, l_ref, out_ref,
                       k_ref, ea_ref, em_ref, el_ref):
    n = q_ref.shape[0]
    i = pl.program_id(1)

    @pl.when(i == 0)
    def _():
        extra = key_extra(kg_ref.shape[0])
        for half in range(2):
            k_ref[half] = own_half(kg_ref[...], extra, half)

    def finish(acc, m, total):
        m_all = jnp.maximum(m, m_ref[...])
        a, b = jnp.exp(m - m_all), jnp.exp(m_ref[...] - m_all)
        out_ref[...] = ((acc * a + acc_ref[...] * b) / (total * a + l_ref[...] * b)).astype(out_ref.dtype)

    q = q_ref[...]
    neg = shifts(q, kmax_ref[...])
    low = low_lanes(n)
    res = [stream(query_rows(q, neg, half), [(k_ref[half, t:t + QB], vg_ref[t:t + QB]) for t in range(0, vg_ref.shape[0], QB)])
           for half in range(2)]
    sums = [row_sum(r[1]) for r in res]
    finish(jnp.where(low, res[0][0], res[1][0]), -pltpu.roll(neg.astype(F32), HEAD, 1), jnp.where(low, sums[0], sums[1]))

    @pl.when(out_of_range(*sums))
    def _():
        def key_rows(c):
            at = pl.ds(pl.multiple_of(c * QB, QB), QB)
            return kg_ref[at], vg_ref[at], None

        exact_heads(q_ref[...], vg_ref.shape[0], key_rows, ea_ref, em_ref, el_ref)
        finish(*(jnp.where(low, r[0], r[1]) for r in (ea_ref, em_ref, el_ref)))


def global_keys_part(qkv, qkv_g, kmax, win, n_rows):
    n_glob = qkv_g.shape[0]
    rb = min(512, n_rows)
    row = pl.BlockSpec((rb, LANES), lambda p, i: (i, p))
    pair = pltpu.VMEM((2, rb, LANES), F32)
    return pl.pallas_call(
        global_keys_kernel, grid=(2, n_rows // rb),
        in_specs=[row, pl.BlockSpec((n_glob, LANES), lambda p, i: (0, 2 + p)), pl.BlockSpec((n_glob, LANES), lambda p, i: (0, 4 + p)),
                  pl.BlockSpec((1, LANES), lambda p, i: (0, p)), row, row, row],
        out_specs=row, out_shape=jax.ShapeDtypeStruct((n_rows, QB), BF16),
        scratch_shapes=[pltpu.VMEM((2, n_glob, LANES), BF16), pair, pair, pair],
        compiler_params=params(2), cost_estimate=cost(10e9, 8e6, 4e6), name="global_keys",
    )(qkv, qkv_g, qkv_g, kmax, *win)


def global_queries_kernel(q_ref, k_ref, v_ref, kmax_ref, out_ref, acc_ref, m_ref, l_ref, *, kb):
    j = pl.program_id(2)
    n = q_ref.shape[0]
    low = low_lanes(n)

    @pl.when(j == 0)
    def _():
        acc_ref[...] = jnp.zeros_like(acc_ref)
        l_ref[...] = jnp.zeros_like(l_ref)

    extra = key_extra(QB)
    q = q_ref[...]
    neg = shifts(q, kmax_ref[...])
    for half in range(2):
        rows = [pl.ds(pl.multiple_of(j * kb, kb) + t, QB) for t in range(0, kb, QB)]
        acc, total = stream(query_rows(q, neg, half), [(own_half(k_ref[r], extra, half), v_ref[r]) for r in rows])
        acc_ref[half] += acc
        l_ref[half] += total

    @pl.when(j == pl.num_programs(2) - 1)
    def _():
        sums = [row_sum(l_ref[half]) for half in range(2)]
        out_ref[0] = jnp.where(low, acc_ref[0], acc_ref[1])
        out_ref[1] = -pltpu.roll(neg.astype(F32), HEAD, 1)
        out_ref[2] = jnp.where(low, sums[0], sums[1])

        @pl.when(out_of_range(*sums))
        def _():
            def key_rows(c):
                at = pl.ds(pl.multiple_of(c * QB, QB), QB)
                return k_ref[at], v_ref[at], None

            exact_heads(q_ref[...], v_ref.shape[0], key_rows, acc_ref, m_ref, l_ref)
            for k, r in enumerate((acc_ref, m_ref, l_ref)):
                out_ref[k] = jnp.where(low, r[0], r[1])


def global_queries_part(qkv_g, qkv, kmax):
    n_glob = qkv_g.shape[0]
    n_rows = qkv.shape[0]
    rb = 512
    kb = min(1024, n_rows)
    return pl.pallas_call(
        functools.partial(global_queries_kernel, kb=kb), grid=(2, n_glob // rb, n_rows // kb),
        in_specs=[pl.BlockSpec((rb, LANES), lambda p, i, j: (i, p)), pl.BlockSpec((n_rows, LANES), lambda p, i, j: (0, 2 + p)),
                  pl.BlockSpec((n_rows, LANES), lambda p, i, j: (0, 4 + p)), pl.BlockSpec((1, LANES), lambda p, i, j: (0, p))],
        out_specs=pl.BlockSpec((3, rb, LANES), lambda p, i, j: (0, i, p)),
        out_shape=jax.ShapeDtypeStruct((3, n_glob, QB), F32),
        scratch_shapes=[pltpu.VMEM((2, rb, LANES), F32)] * 3,
        compiler_params=params(3), cost_estimate=cost(34e9, 20e6, 16e6), name="global_queries",
    )(qkv_g, qkv, qkv, kmax)


def exchange_mlp_kernel(x_hbm, w_hbm, qkv_hbm, qkvg_hbm, acc_hbm, m_hbm, l_hbm, glob_hbm, idx_ref, pre_ref, y_hbm,
                        x_ref, o_ref, wo_ref, w2_ref, w1_ref, q_ref, kg_ref, glob_ref, win_ref, load_sem, win_sem, y_sem,
                        up_send, up_recv, down_send, down_recv, *, n_tp, n_rep, d_o, d_f, rb):
    me = lax.axis_index('tp')
    n_blk = x_ref.shape[0] // rb
    width = n_tp * d_f
    qb = min(QB, rb)

    barrier = pltpu.get_barrier_semaphore()

    @pl.when(me > 0)
    def _():
        pl.semaphore_signal(barrier, inc=1, device_id={'tp': me - 1}, device_id_type=pl.DeviceIdType.MESH)

    @pl.when(me < n_tp - 1)
    def _():
        pl.semaphore_signal(barrier, inc=1, device_id={'tp': me + 1}, device_id_type=pl.DeviceIdType.MESH)

    early = [pltpu.make_async_copy(qkv_hbm.at[:, pl.ds(0, QB)], q_ref, load_sem.at[0]),
             pltpu.make_async_copy(qkvg_hbm.at[:, pl.ds(QB, 512)], kg_ref, load_sem.at[1]),
             pltpu.make_async_copy(glob_hbm, glob_ref, load_sem.at[2])]

    def rows_of(b):
        return pl.ds(pl.multiple_of(b * rb, rb), rb)

    def fetch(b):
        return [pltpu.make_async_copy(h.at[rows_of(b)], win_ref.at[b % 2, n], win_sem.at[b % 2, n])
                for n, h in enumerate((acc_hbm, m_hbm, l_hbm))]

    for c in early + fetch(2):
        c.start()
    copies = [pltpu.make_async_copy(x_hbm, x_ref, load_sem.at[3])]
    piece = wo_ref.shape[1] // n_rep
    for j in range(n_rep):
        for t in range(n_tp):
            lanes = pl.ds(j * piece, piece)
            for src, n, dst in ((0, d_o, wo_ref), (d_o, d_f, w2_ref), (d_o + d_f, d_f, w1_ref)):
                copies.append(pltpu.make_async_copy(w_hbm.at[j, t, pl.ds(src, n)], dst.at[pl.ds(t * n, n), lanes],
                                                    load_sem.at[3 + len(copies)]))
    for c in copies:
        c.start()

    ends = jnp.logical_or(me == 0, me == n_tp - 1)

    @pl.when(ends)
    def _():
        pl.semaphore_wait(barrier, 1)

    @pl.when(jnp.logical_not(ends))
    def _():
        pl.semaphore_wait(barrier, 2)

    for c in early:
        c.wait()

    def attend(b):
        @pl.when(b + 1 < n_blk)
        def _():
            for c in fetch(b + 1):
                c.start()

        for c in fetch(b):
            c.wait()

        @pl.loop(0, rb // qb)
        def _(r):
            at = pl.ds(pl.multiple_of(r * qb, qb), qb)
            rows = pl.ds(pl.multiple_of(b * rb + r * qb, qb), qb)
            low = low_lanes(qb)
            parts = []
            for pr in range(2):
                cols = slice(pr * LANES, pr * LANES + LANES)
                q = q_ref[rows, cols]
                zero = jnp.zeros_like(q)
                q2 = jnp.concatenate([jnp.where(low, q, zero), jnp.where(low, zero, q)], axis=0)
                sc = dot_nt(q2, kg_ref[:, cols])
                top = jnp.max(sc, axis=1, keepdims=True)
                e = jnp.exp(sc - top)
                total = row_sum(e)
                acc = dot_nn(e.astype(BF16), kg_ref[:, QB + pr * LANES:QB + pr * LANES + LANES])
                acc, m, total = (jnp.where(low, v[:qb], v[qb:]) for v in (acc, top, total))
                acc_w, m_w, l_w = (win_ref[b % 2, n, at, cols] for n in range(3))
                m_all = jnp.maximum(m, m_w)
                f, f_w = jnp.exp(m - m_all), jnp.exp(m_w - m_all)
                parts.append((acc * f + acc_w * f_w) / (total * f + l_w * f_w))
            place(rows, b * rb + r * qb, jnp.concatenate(parts, axis=1))

    def place(rows, row0, o):
        row = row0 + lax.broadcasted_iota(jnp.int32, (o.shape[0], 1), 0)
        hit = jnp.where(idx_ref[...] == row, 1.0, 0.0)
        placed = dot_nn(hit.astype(BF16), glob_ref[...])
        o_ref[me, rows] = jnp.where(row_sum(hit) > 0.5, placed, o).astype(BF16)

    def up(d, b):
        at = o_ref.at[me - d, rows_of(b)]
        return pltpu.make_async_remote_copy(at, at, up_send.at[d, b], up_recv.at[d, b], device_id={'tp': me + 1},
                                            device_id_type=pl.DeviceIdType.MESH)

    def down(d, b):
        at = o_ref.at[me + d, rows_of(b)]
        return pltpu.make_async_remote_copy(at, at, down_send.at[d, b], down_recv.at[d, b], device_id={'tp': me - 1},
                                            device_id_type=pl.DeviceIdType.MESH)

    def landed(recv, d, shard, b):
        at = o_ref.at[shard, rows_of(b)]
        pltpu.make_async_remote_copy(at, at, up_send.at[0, b], recv.at[d - 1, b], device_id={'tp': me},
                                     device_id_type=pl.DeviceIdType.MESH).wait_recv()

    def send_own(b):
        @pl.when(me < n_tp - 1)
        def _():
            up(0, b).start()

        @pl.when(me > 0)
        def _():
            down(0, b).start()

    for b in range(2):
        place(pl.ds(b * rb, rb), b * rb, pre_ref[b * rb:(b + 1) * rb, :].astype(F32))
    send_own(0)

    def step(s, carry):
        @pl.when(s + 1 < n_blk)
        def _():
            send_own(s + 1)

        for d in range(n_tp - 2, 0, -1):
            b = s - (d - 1)
            here = (b >= 0) & (b < n_blk)

            @pl.when(here & (me >= d) & (me < n_tp - 1))
            def _():
                landed(up_recv, d, me - d, b)
                up(d, b).start()

            @pl.when(here & (me + d <= n_tp - 1) & (me > 0))
            def _():
                landed(down_recv, d, me + d, b)
                down(d, b).start()

        @pl.when(s + 2 < n_blk)
        def _():
            attend(s + 2)

        @pl.when(s == n_tp - 2)
        def _():
            for c in copies:
                c.wait()

        @pl.when(s >= n_tp - 2)
        def _():
            b = s - (n_tp - 2)
            rows = rows_of(b)
            for d in range(1, n_tp):
                @pl.when(me == n_tp - 1)
                def _():
                    landed(up_recv, d, me - d, b)

                @pl.when(me == 0)
                def _():
                    landed(down_recv, d, me + d, b)

            mixed = dot_nn(o_ref[0, rows], wo_ref[:d_o, :])
            for t in range(1, n_tp):
                mixed += dot_nn(o_ref[t, rows], wo_ref[t * d_o:(t + 1) * d_o, :])
            h = (x_ref[rows].astype(F32) + mixed).astype(BF16)
            acc = h.astype(F32)
            for f0 in range(0, width, 512):
                f1 = min(f0 + 512, width)
                z = dot_nt(h, w1_ref[f0:f1, :])
                u = 0.5 * z * (1.0 + jnp.tanh(math.sqrt(2.0 / math.pi) * (z + 0.044715 * (z * z * z))))
                acc += dot_nn(u.astype(BF16), w2_ref[f0:f1, :])
            x_ref[rows] = acc.astype(BF16)
            pltpu.make_async_copy(x_ref.at[rows], y_hbm.at[rows], y_sem.at[b]).start()

        return carry

    lax.fori_loop(0, n_blk + n_tp - 2, step, 0)

    def finish(b, carry):
        rows = rows_of(b)
        pltpu.make_async_copy(x_ref.at[rows], y_hbm.at[rows], y_sem.at[b]).wait()
        for d in range(n_tp - 1):
            @pl.when((me < n_tp - 1) & (me >= d))
            def _():
                up(d, b).wait_send()

            @pl.when((me > 0) & (me + d <= n_tp - 1))
            def _():
                down(d, b).wait_send()

        return carry

    lax.fori_loop(0, n_blk, finish, 0)


def exchange_mlp(tokens, w_all, qkv, qkv_g, win, o_pre, glob_out, local_idx, n_tp, d_o, d_f):
    n_rows, dim = tokens.shape
    n_glob = local_idx.shape[0]
    n_rep = w_all.shape[0]
    rb = n_rows // 8
    n_blk = n_rows // rb
    anywhere = pl.BlockSpec(memory_space=pl.ANY)
    dma = pltpu.SemaphoreType.DMA
    return pl.pallas_call(
        functools.partial(exchange_mlp_kernel, n_tp=n_tp, n_rep=n_rep, d_o=d_o, d_f=d_f, rb=rb),
        in_specs=[anywhere] * 8 + [pl.BlockSpec(memory_space=pltpu.VMEM)] * 2, out_specs=anywhere,
        out_shape=jax.ShapeDtypeStruct(tokens.shape, BF16),
        scratch_shapes=[pltpu.VMEM((n_rows, dim), BF16), pltpu.VMEM((n_tp, n_rows, d_o), BF16),
                        pltpu.VMEM((n_tp * d_o, dim), BF16), pltpu.VMEM((n_tp * d_f, dim), BF16),
                        pltpu.VMEM((n_tp * d_f, dim), BF16), pltpu.VMEM((n_rows, d_o), BF16),
                        pltpu.VMEM((n_glob, 2 * d_o), BF16), pltpu.VMEM((n_glob, d_o), BF16),
                        pltpu.VMEM((2, 3, rb, d_o), F32), dma((4 + 3 * n_rep * n_tp,)), dma((2, 3)), dma((n_blk,)),
                        dma((n_tp - 1, n_blk)), dma((n_tp - 1, n_blk)), dma((n_tp - 1, n_blk)), dma((n_tp - 1, n_blk))],
        compiler_params=pltpu.CompilerParams(collective_id=1, has_side_effects=True, vmem_limit_bytes=60 << 20),
        cost_estimate=cost(2 * n_rows * dim * (dim + 2 * n_tp * d_f), 40e6), name="exchange_mlp",
    )(tokens, w_all, qkv, qkv_g, *win, glob_out, local_idx[None, :], o_pre)


def copy_kernel(a_hbm, b_hbm, buf_ref, in_sem, out_sem):
    n, rows = buf_ref.shape[:2]
    at = [pl.ds(i * rows, rows) for i in range(n)]
    loads = [pltpu.make_async_copy(a_hbm.at[r], buf_ref.at[i], in_sem.at[i]) for i, r in enumerate(at)]
    stores = [pltpu.make_async_copy(buf_ref.at[i], b_hbm.at[r], out_sem.at[i]) for i, r in enumerate(at)]
    for c in loads:
        c.start()
    for load, store in zip(loads, stores):
        load.wait()
        store.start()
    for c in stores:
        c.wait()


def streamed(a):
    n = 8
    anywhere = pl.BlockSpec(memory_space=pl.ANY)
    dma = pltpu.SemaphoreType.DMA
    return pl.pallas_call(copy_kernel, in_specs=[anywhere], out_specs=anywhere,
                          out_shape=jax.ShapeDtypeStruct(a.shape, a.dtype),
                          scratch_shapes=[pltpu.VMEM((n, a.shape[0] // n, a.shape[1]), a.dtype), dma((n,)), dma((n,))],
                          compiler_params=pltpu.CompilerParams(vmem_limit_bytes=params(0).vmem_limit_bytes), name="result")(a)


def combine(a, b):
    m = jnp.maximum(a[1], b[1])
    e_a, e_b = jnp.exp(a[1] - m), jnp.exp(b[1] - m)
    return a[0] * e_a + b[0] * e_b, m, a[2] * e_a + b[2] * e_b


def solution(mesh):
    n_seq = mesh.shape['sp']
    to_right = [(i, i + 1) for i in range(n_seq - 1)]
    to_left = [(i + 1, i) for i in range(n_seq - 1)]
    core_swap = [(i, i ^ 1) for i in range(n_seq)]
    chip_swap = [(i, i ^ 2) for i in range(n_seq)]

    def device_layer(tokens, glob_pos, w_query, w_key, w_value, w_out, w_up, w_down):
        n_rows, dim = tokens.shape
        n_glob = glob_pos.shape[0]
        sp = lax.axis_index('sp')
        core, chip = sp % 2, sp // 2
        first_row = sp * n_rows
        seq_len = n_rows * n_seq
        local_idx = glob_pos - first_row

        d_o, d_f = w_out.shape[0] * w_out.shape[1], w_down.shape[0]
        shard = jnp.concatenate([w_out.reshape(d_o, dim), w_down, w_up.T], axis=0)
        rep = lax.axis_index('dp') * n_seq + sp
        n_tp, n_rep = mesh.shape['tp'], mesh.shape['dp'] * n_seq
        piece = dim // n_rep
        w_slice = lax.dynamic_slice_in_dim(shard, rep * piece, piece, axis=1)
        w_all = lax.all_gather(w_slice, ('dp', 'sp', 'tp'))
        w_all = w_all.reshape(n_rep, n_tp, d_o + 2 * d_f, piece)

        w_cat = jnp.concatenate([w_query.reshape(dim, -1) * jnp.asarray(0.125, BF16),
                                 w_key.reshape(dim, -1), w_value.reshape(dim, -1)], axis=1)
        qkv, picked, kmax = qkv_part(tokens, w_cat, local_idx)
        halo_l = lax.ppermute(qkv[n_rows - WIN:, QB:], 'sp', to_right)
        halo_r = lax.ppermute(qkv[:WIN, QB:], 'sp', to_left)

        half = n_glob // 2
        mine = lax.dynamic_slice_in_dim(picked, core * half, half)
        other = lax.ppermute(lax.dynamic_slice_in_dim(picked, (1 - core) * half, half), 'sp', core_swap)
        mine = mine + other
        mine, flag_pos = lax.optimization_barrier((mine, glob_pos))
        k_pos = first_row - WIN + jnp.arange(n_rows + 2 * WIN)
        k_off = jnp.any(flag_pos[:, None] == k_pos[None, :], axis=0) | (k_pos < 0) | (k_pos >= seq_len)
        bias = jnp.where(k_off, -jnp.inf, 0.0).astype(F32)[None, :]
        lane = jnp.arange(LANES) % HEAD
        extra = jnp.where(lane == 0, 1.0, jnp.where((lane == 1) & k_off[:, None], FLOOR, 0.0)).astype(BF16)
        got = lax.ppermute(mine, 'sp', chip_swap)
        win = window_part(qkv, halo_l, halo_r, extra, bias, kmax, 0, 3)
        got, win = lax.optimization_barrier((got, win))
        mine = mine + got
        other = lax.ppermute(mine, 'sp', core_swap)
        qkv_g = jnp.concatenate([jnp.where(core == 0, mine, other), jnp.where(core == 0, other, mine)], axis=0)

        part = global_queries_part(qkv_g, qkv, kmax)

        quarter = n_glob // 4
        got = lax.ppermute(lax.dynamic_slice_in_dim(part, (1 - core) * half, half, axis=1), 'sp', core_swap)
        joined = jnp.stack(combine(lax.dynamic_slice_in_dim(part, core * half, half, axis=1), got))
        joined, kmax = lax.optimization_barrier((joined, kmax))
        got = lax.ppermute(lax.dynamic_slice_in_dim(joined, (1 - chip) * quarter, quarter, axis=1), 'sp', chip_swap)
        win = window_part(qkv, halo_l, halo_r, extra, bias, kmax, 3, 4, win)
        o_pre = global_keys_part(qkv, qkv_g, kmax, win, n_rows // 4)
        got, win, o_pre = lax.optimization_barrier((got, win, o_pre))
        g_acc, _, g_l = combine(lax.dynamic_slice_in_dim(joined, chip * quarter, quarter, axis=1), got)
        mine = (g_acc / g_l).astype(BF16)
        other = lax.ppermute(mine, 'sp', chip_swap)
        mine = jnp.concatenate([jnp.where(chip == 0, mine, other), jnp.where(chip == 0, other, mine)], axis=0)
        other = lax.ppermute(mine, 'sp', core_swap)
        glob_out = jnp.concatenate([jnp.where(core == 0, mine, other), jnp.where(core == 0, other, mine)], axis=0)

        return streamed(exchange_mlp(tokens, w_all, qkv, qkv_g, win, o_pre, glob_out, local_idx, n_tp, d_o, d_f))

    row_spec = P(('dp', 'sp'), None)
    head_spec = P(None, 'tp', None)
    in_specs = (row_spec, P('dp'), head_spec, head_spec, head_spec, P('tp', None, None), P(None, 'tp'), P('tp', None))
    return jax.shard_map(device_layer, mesh=mesh, in_specs=in_specs, out_specs=row_spec, check_vma=False)
```
